32 devices in a mesh: dp: 1 (over z), tp: 32 (over y, x, core).
Axes of the slice: x: 4, y: 4, z: 1, core: 2. Of those that a mesh axis runs over, the one named last changes fastest.
The devices are a block of a 4x4x8 slice.
Arguments:
- tokens: bfloat16 [1, 2048, 4096], P('dp', 'tp')
- doc_ids: int32 [1, 2048], P('dp', 'tp')
- norm1_gain: float32 [2, 4096], replicated
- norm1_shift: float32 [2, 4096], replicated
- qkv_weight: bfloat16 [2, 4096, 3, 32, 128], P(None, None, None, 'tp')
- out_weight: bfloat16 [2, 32, 128, 4096], P(None, 'tp')
- out_bias: float32 [2, 4096], replicated
- norm2_gain: float32 [2, 4096], replicated
- norm2_shift: float32 [2, 4096], replicated
- up_weight: bfloat16 [2, 4096, 16384], P(None, None, 'tp')
- up_bias: float32 [2, 16384], P(None, 'tp')
- down_weight: bfloat16 [2, 16384, 4096], P(None, 'tp')
- down_bias: float32 [2, 4096], replicated
Outputs:
- output: bfloat16 [1, 2048, 4096], P('dp', 'tp')
All inputs are finite; a program needn't handle non-finite values.
Results may differ from the reference program's by a relative error of at most 0.0120228.
Values are sent between devices in bfloat16 or wider.
A program may use at most 768 MiB of HBM per device.

```python
import jax
import jax.numpy as jnp
from jax import lax

BATCH = 1
SEQ_LEN = 2048
D_MODEL = 4096
N_HEADS = 32
HEAD_DIM = 128
FF_DIM = 16384
GROUPS = 32
LAYERS = 2
DOC_CUTS = 3
QUERY_BLOCK = 256


def setup_inputs(seed: int = 0, part: int = 0) -> dict:
    root_key = jax.random.key(seed)
    keys_all = jax.random.split(root_key, 12)
    part_key = jax.random.fold_in(keys_all[0], part)
    tok_key, scale_key, cut_key = jax.random.split(part_key, 3)
    base_tok = jax.random.normal(tok_key, (BATCH, SEQ_LEN, D_MODEL), jnp.float32)
    row_scale = jnp.exp(0.5 * jax.random.normal(scale_key, (BATCH, SEQ_LEN, 1), jnp.float32))
    tokens = (base_tok * row_scale).astype(jnp.bfloat16)
    cut_pos = jax.random.randint(cut_key, (BATCH, 1, DOC_CUTS), 1, SEQ_LEN, dtype=jnp.int32)
    positions = jnp.arange(SEQ_LEN, dtype=jnp.int32)[None, :, None]
    doc_ids = jnp.sum((positions >= cut_pos).astype(jnp.int32), axis=-1, dtype=jnp.int32)
    d_scale = D_MODEL ** -0.5
    f_scale = FF_DIM ** -0.5
    qkv_mult = jnp.array([1.4142135, 1.4142135, 1.0], jnp.float32)[None, None, :, None, None]
    vec_shape = (LAYERS, D_MODEL)
    qkv_weight = jax.random.normal(keys_all[1], (LAYERS, D_MODEL, 3, N_HEADS, HEAD_DIM), jnp.float32) * qkv_mult * d_scale
    out_weight = jax.random.normal(keys_all[2], (LAYERS, N_HEADS, HEAD_DIM, D_MODEL), jnp.float32) * (1.5 * d_scale)
    up_weight = jax.random.normal(keys_all[3], (LAYERS, D_MODEL, FF_DIM), jnp.float32) * d_scale
    down_weight = jax.random.normal(keys_all[4], (LAYERS, FF_DIM, D_MODEL), jnp.float32) * f_scale
    return {
        "tokens": tokens,
        "doc_ids": doc_ids,
        "norm1_gain": 1.0 + 0.2 * jax.random.normal(keys_all[5], vec_shape, jnp.float32),
        "norm1_shift": 0.2 * jax.random.normal(keys_all[6], vec_shape, jnp.float32),
        "qkv_weight": qkv_weight.astype(jnp.bfloat16),
        "out_weight": out_weight.astype(jnp.bfloat16),
        "out_bias": 0.3 * jax.random.normal(keys_all[7], vec_shape, jnp.float32),
        "norm2_gain": 1.0 + 0.2 * jax.random.normal(keys_all[8], vec_shape, jnp.float32),
        "norm2_shift": 0.2 * jax.random.normal(keys_all[9], vec_shape, jnp.float32),
        "up_weight": up_weight.astype(jnp.bfloat16),
        "up_bias": 0.5 * jax.random.normal(keys_all[10], (LAYERS, FF_DIM), jnp.float32),
        "down_weight": down_weight.astype(jnp.bfloat16),
        "down_bias": 0.3 * jax.random.normal(keys_all[11], vec_shape, jnp.float32),
    }


def layer_norm(residual, gain_vec, shift_vec):
    mean_val = jnp.mean(residual, axis=-1, keepdims=True)
    centered = residual - mean_val
    variance = jnp.mean(centered * centered, axis=-1, keepdims=True)
    return (centered * lax.rsqrt(variance + 1e-5) * gain_vec + shift_vec).astype(jnp.bfloat16)


def attend_sequence(qkv_seq, ids_seq):
    n_blocks = SEQ_LEN // QUERY_BLOCK
    keys32 = qkv_seq[:, 1].astype(jnp.float32)
    values32 = qkv_seq[:, 2].astype(jnp.float32)
    q_blocks = qkv_seq[:, 0].reshape(n_blocks, QUERY_BLOCK, N_HEADS, HEAD_DIM)
    id_blocks = ids_seq.reshape(n_blocks, QUERY_BLOCK)
    starts = jnp.arange(n_blocks, dtype=jnp.int32) * QUERY_BLOCK
    key_pos = jnp.arange(SEQ_LEN, dtype=jnp.int32)

    def one_block(block_in):
        q_blk, id_blk, start_row = block_in
        scores = jnp.einsum("qhe,khe->hqk", q_blk.astype(jnp.float32), keys32) * (HEAD_DIM ** -0.5)
        query_pos = start_row + jnp.arange(QUERY_BLOCK, dtype=jnp.int32)
        allowed = (key_pos[None, :] <= query_pos[:, None]) & (ids_seq[None, :] == id_blk[:, None])
        scores = jnp.where(allowed[None], scores, -1e30)
        probs_blk = jax.nn.softmax(scores, axis=-1).astype(jnp.bfloat16)
        return jnp.einsum("hqk,khe->qhe", probs_blk.astype(jnp.float32), values32).astype(jnp.bfloat16)

    return lax.map(one_block, (q_blocks, id_blocks, starts)).reshape(SEQ_LEN, N_HEADS, HEAD_DIM)


def grouped_sum(activations, weight):
    def add_group(running, group_in):
        act_g, weight_g = group_in
        part_out = jnp.dot(act_g, weight_g, preferred_element_type=jnp.float32).astype(jnp.bfloat16)
        return running + part_out.astype(jnp.float32), None
    zero_acc = jnp.zeros((activations.shape[1], weight.shape[2]), jnp.float32)
    total, unused = lax.scan(add_group, zero_acc, (activations, weight))
    return total


def run_sequence(tok_seq, ids_seq, layer_params):
    head_group = N_HEADS // GROUPS
    ff_group = FF_DIM // GROUPS

    def one_layer(residual, params):
        n1_gain, n1_shift, w_qkv, w_out, b_out, n2_gain, n2_shift, w_up, b_up, w_down, b_down = params
        normed = layer_norm(residual, n1_gain, n1_shift)
        qkv_seq = jnp.dot(normed, w_qkv.reshape(D_MODEL, 3 * N_HEADS * HEAD_DIM), preferred_element_type=jnp.float32).astype(jnp.bfloat16)
        attn_out = attend_sequence(qkv_seq.reshape(SEQ_LEN, 3, N_HEADS, HEAD_DIM), ids_seq)
        attn_groups = jnp.moveaxis(attn_out.reshape(SEQ_LEN, GROUPS, head_group * HEAD_DIM), 1, 0)
        attn_sum = grouped_sum(attn_groups, w_out.reshape(GROUPS, head_group * HEAD_DIM, D_MODEL))
        residual = residual + (attn_sum + b_out)
        normed2 = layer_norm(residual, n2_gain, n2_shift)
        pre_act = jnp.dot(normed2, w_up, preferred_element_type=jnp.float32) + b_up
        hidden = jax.nn.gelu(pre_act, approximate=True).astype(jnp.bfloat16)
        hid_groups = jnp.moveaxis(hidden.reshape(SEQ_LEN, GROUPS, ff_group), 1, 0)
        mlp_sum = grouped_sum(hid_groups, w_down.reshape(GROUPS, ff_group, D_MODEL))
        residual = residual + (mlp_sum + b_down)
        return residual, None

    resid_end, unused = lax.scan(one_layer, tok_seq.astype(jnp.float32), layer_params)
    return resid_end.astype(jnp.bfloat16)


def reference(tokens, doc_ids, norm1_gain, norm1_shift, qkv_weight, out_weight, out_bias, norm2_gain, norm2_shift, up_weight, up_bias, down_weight, down_bias):
    layer_params = (norm1_gain, norm1_shift, qkv_weight, out_weight, out_bias, norm2_gain, norm2_shift, up_weight, up_bias, down_weight, down_bias)
    return lax.map(lambda seq_in: run_sequence(seq_in[0], seq_in[1], layer_params), (tokens, doc_ids))
```

```python
import functools
import math

import jax
import jax.numpy as jnp
from jax import lax
from jax.experimental import pallas as pl
from jax.experimental.pallas import tpu as pltpu
from jax.sharding import PartitionSpec as P

QUERY_ROWS = 512
COLS = 512
MESH = pl.DeviceIdType.MESH
VMEM_LIMIT = 66 * 1000 * 1000

FAR_FIRST = (2, 1, -1, 0)


class Place:
    def __init__(self, side):
        self.side = side
        self.me = lax.axis_index("tp")
        self.core = self.me % 2
        chip = self.me // 2
        self.x = chip % side
        self.y = chip // side
        self.partner = chip * 2 + 1 - self.core
        self.first = {1: self.dev(1, 0), -1: self.dev(-1, 0)}
        self.second = {1: self.dev(0, 1), -1: self.dev(0, -1)}

    def dev(self, i, j, core=None):
        core = self.core if core is None else core
        dx = i * (1 - core) + j * core
        dy = j * (1 - core) + i * core
        return (((self.y + dy + self.side) % self.side) * self.side + (self.x + dx + self.side) % self.side) * 2 + core

    def barrier(self):
        sem = pltpu.get_barrier_semaphore()
        others = [self.first[1], self.first[-1], self.second[1], self.second[-1], self.partner]
        for other in others:
            pl.semaphore_signal(sem, inc=1, device_id={"tp": other}, device_id_type=MESH)
        pl.semaphore_wait(sem, len(others))


def by_cols(width, fn):
    step = min(COLS, width)

    def body(n, carry):
        fn(pl.ds(pl.multiple_of(n * step, step), step))
        return carry

    lax.fori_loop(0, width // step, body, 0)


def scatter_kernel(side, layer, act_ref, w_hbm, res_ref, bias_ref, out_ref, w_ref, own, snd, prt, stg, mid, fin, stg2, mid2, fin2, w_sem, pair_send, pair_recv, send_sem, recv_sem):
    load_w = pltpu.make_async_copy(w_hbm.at[layer, 0] if len(w_hbm.shape) == 4 else w_hbm.at[layer], w_ref, w_sem)
    load_w.start()
    place = Place(side)
    rows, width = res_ref.shape
    half = rows // 2
    place.barrier()
    load_w.wait()

    def remote(src, dst, slot, device):
        return pltpu.make_async_remote_copy(src_ref=src, dst_ref=dst, send_sem=send_sem.at[slot], recv_sem=recv_sem.at[slot], device_id={"tp": device}, device_id_type=MESH)

    def pair_copy(g, jj):
        return pltpu.make_async_remote_copy(src_ref=snd.at[g % 2, jj], dst_ref=prt.at[g, jj], send_sem=pair_send.at[g, jj], recv_sem=pair_recv.at[g, jj], device_id={"tp": place.partner}, device_id_type=MESH)

    def product(core, g, dst):
        starts = [pl.multiple_of(place.dev(FAR_FIRST[g], j, core) * rows, rows) for j in FAR_FIRST]

        def piece(cols):
            lhs = jnp.concatenate([act_ref[pl.ds(s, rows), :] for s in starts], axis=0)
            part = jnp.dot(lhs, w_ref[:, cols], preferred_element_type=jnp.float32).astype(jnp.bfloat16)
            for jj in range(side):
                dst[jj, :, cols] = part[jj * rows:(jj + 1) * rows]

        by_cols(width, piece)

    def pair_sum(g, jj, h, cols):
        at = pl.ds(h * half, half)
        return own[g, jj, at, cols].astype(jnp.float32) + prt[g, jj, at, cols].astype(jnp.float32)

    far, plus, minus, here = range(side)
    sent = []

    def send(src, dst, slot, device):
        copy = remote(src, dst, slot, device)
        copy.start()
        sent.append(copy)

    def arrived(dst, slot):
        remote(dst, dst, slot, place.me).wait_recv()

    def open_group(g):
        for jj in range(side):
            if g >= 2:
                pair_copy(g - 2, jj).wait_send()
        product(1 - place.core, g, snd.at[g % 2])
        for jj in range(side):
            pair_copy(g, jj).start()
        product(place.core, g, own.at[g])
        for jj in range(side):
            pair_copy(g, jj).wait_recv()
        for k, (jj, h) in enumerate(((far, 0), (far, 1), (plus, 1), (minus, 0))):
            def stage(cols, k=k, jj=jj, h=h):
                stg[g, k, :, cols] = pair_sum(g, jj, h, cols)
            by_cols(width, stage)
            dst = mid.at[g, k] if k < 2 else fin.at[g, k]
            slot = 6 * g + (4 + k if k < 2 else k)
            send(stg.at[g, k], dst, slot, place.second[1 if k % 2 == 0 else -1])

    def relay(g):
        for k, (jj, h) in enumerate(((plus, 0), (minus, 1))):
            arrived(mid.at[g, k], 6 * g + 4 + k)
            def add(cols, k=k, jj=jj, h=h):
                mid[g, k, :, cols] += pair_sum(g, jj, h, cols)
            by_cols(width, add)
            send(mid.at[g, k], fin.at[g, k], 6 * g + k, place.second[1 if k == 0 else -1])

    base = 6 * side

    def close_group(g):
        for k in range(4):
            arrived(fin.at[g, k], 6 * g + k)

        def total(h, cols):
            return pair_sum(g, here, h, cols) + fin[g, 0 if h == 0 else 1, :, cols] + fin[g, 3 if h == 0 else 2, :, cols]

        def keep(k, h):
            def fn(cols):
                stg2[k, :, cols] = total(h, cols)
            by_cols(width, fn)

        def join(k):
            arrived(mid2.at[k], base + 4 + k)
            def fn(cols):
                mid2[k, :, cols] += total(k, cols)
            by_cols(width, fn)
            send(mid2.at[k], fin2.at[k], base + k, place.first[1 if k == 0 else -1])

        if g == far:
            keep(0, 0)
            send(stg2.at[0], mid2.at[0], base + 4, place.first[1])
            keep(1, 1)
            send(stg2.at[1], mid2.at[1], base + 5, place.first[-1])
        elif g == plus:
            keep(2, 1)
            send(stg2.at[2], fin2.at[2], base + 2, place.first[1])
            join(0)
        elif g == minus:
            keep(3, 0)
            send(stg2.at[3], fin2.at[3], base + 3, place.first[-1])
            join(1)
        else:
            for k in range(4):
                arrived(fin2.at[k], base + k)
            for h in range(2):
                def fn(cols, h=h):
                    at = pl.ds(h * half, half)
                    summed = total(h, cols) + fin2[0 if h == 0 else 1, :, cols] + fin2[3 if h == 0 else 2, :, cols]
                    out_ref[at, cols] = res_ref[at, cols] + (summed + bias_ref[layer:layer + 1, cols])
                by_cols(width, fn)

    open_group(0)
    open_group(1)
    relay(0)
    open_group(2)
    relay(1)
    close_group(0)
    open_group(3)
    relay(2)
    close_group(1)
    relay(3)
    close_group(2)
    close_group(3)
    for g in (side - 2, side - 1):
        for jj in range(side):
            pair_copy(g, jj).wait_send()
    for copy in sent:
        copy.wait_send()


def project_and_scatter(side, call_id, layer, act, weight, residual, bias):
    rows, width = residual.shape
    depth = act.shape[1]
    half = rows // 2
    quad = (side, side, rows, width)
    part = (side, 2, half, width)
    vmem = pl.BlockSpec(memory_space=pltpu.VMEM)
    return pl.pallas_call(
        functools.partial(scatter_kernel, side, layer),
        out_shape=jax.ShapeDtypeStruct((rows, width), jnp.float32),
        in_specs=[vmem, pl.BlockSpec(memory_space=pl.ANY), vmem, vmem],
        out_specs=vmem,
        scratch_shapes=[
            pltpu.VMEM((depth, width), jnp.bfloat16),
            pltpu.VMEM(quad, jnp.bfloat16),
            pltpu.VMEM((2,) + quad[1:], jnp.bfloat16),
            pltpu.VMEM(quad, jnp.bfloat16),
            pltpu.VMEM((side, 4, half, width), jnp.float32),
            pltpu.VMEM(part, jnp.float32),
            pltpu.VMEM((side, 4, half, width), jnp.float32),
            pltpu.VMEM((4, half, width), jnp.float32),
            pltpu.VMEM((2, half, width), jnp.float32),
            pltpu.VMEM((4, half, width), jnp.float32),
            pltpu.SemaphoreType.DMA,
            pltpu.SemaphoreType.DMA((side, side)),
            pltpu.SemaphoreType.DMA((side, side)),
            pltpu.SemaphoreType.DMA((6 * side + 6,)),
            pltpu.SemaphoreType.DMA((6 * side + 6,)),
        ],
        compiler_params=pltpu.CompilerParams(collective_id=call_id, has_side_effects=True, vmem_limit_bytes=VMEM_LIMIT),
        name=f"scatter_{call_id}",
    )(act, weight, residual, bias)


GATHER_ORDER = ((0, 0), (-1, 0), (1, 0), (0, -1), (0, 1), (2, 0), (-1, -1), (-1, 1), (1, -1), (1, 1), (0, 2), (2, -1), (2, 1), (-1, 2), (1, 2), (2, 2))


def gather_kernel(side, layer, gelu, n_out, tail, res_ref, gain_ref, shift_ref, w_hbm, b_ref, *refs):
    tails, refs = (refs[0], refs[1:]) if tail else (None, refs)
    outs, refs = refs[:n_out], refs[n_out:]
    tails_out, refs = (refs[0], refs[1:]) if tail else (None, refs)
    (w_ref, buf, w_sem, send_sem, recv_sem, pair_send, pair_recv) = refs
    load_w = pltpu.make_async_copy(w_hbm.at[layer], w_ref, w_sem)
    load_w.start()
    place = Place(side)
    rows, width = res_ref.shape
    half = rows // 2
    for at in (pl.ds(0, half), pl.ds(half, half)):
        residual = res_ref[at, :]
        centered = residual - jnp.mean(residual, axis=-1, keepdims=True)
        variance = jnp.mean(centered * centered, axis=-1, keepdims=True)
        normed = centered * lax.rsqrt(variance + 1e-5) * gain_ref[layer:layer + 1, :] + shift_ref[layer:layer + 1, :]
        buf[place.me, at, pl.ds(0, width)] = normed.astype(jnp.bfloat16)
    if tail:
        buf[place.me, :, pl.ds(width, tail)] = tails[...]
    place.barrier()

    def view(i, j, h, core=None):
        return buf.at[place.dev(i, j, core), pl.ds(h * half, half)]

    def wrap(k):
        return (k + 1) % side - 1

    def slot(i, j, h):
        return ((i % side) * side + j % side) * 2 + h

    sent = []

    def send(i, j, h, axis, step):
        there = (wrap(i - step), j) if axis == 0 else (i, wrap(j - step))
        device = (place.first, place.second)[axis][step]
        index = slot(i, j, h)
        copy = pltpu.make_async_remote_copy(src_ref=view(i, j, h), dst_ref=view(i, j, h), send_sem=send_sem.at[axis * 2 + (step > 0), index], recv_sem=recv_sem.at[slot(*there, h)], device_id={"tp": device}, device_id_type=MESH)
        copy.start()
        sent.append(copy)

    def pair(i, j, h, core=None):
        index = slot(i, j, h)
        ref = view(i, j, h, core)
        return pltpu.make_async_remote_copy(src_ref=ref, dst_ref=ref, send_sem=pair_send.at[index], recv_sem=pair_recv.at[index], device_id={"tp": place.partner}, device_id_type=MESH)

    def share(i, j, h):
        copy = pair(i, j, h)
        copy.start()
        sent.append(copy)

    def arrived(i, j, h):
        ref = view(i, j, h)
        pltpu.make_async_remote_copy(src_ref=ref, dst_ref=ref, send_sem=send_sem.at[0, 0], recv_sem=recv_sem.at[slot(i, j, h)], device_id={"tp": place.me}, device_id_type=MESH).wait_recv()

    def multiply(shards, core):
        devs = [place.dev(i, j, core) for i, j in shards]
        step = 128 if w_ref.shape[1] % 256 else 256

        def piece(cols, outs, out_cols):
            lhs = jnp.concatenate([buf[d, :, pl.ds(0, width)] for d in devs], axis=0)
            part = jnp.dot(lhs, w_ref[:, cols], preferred_element_type=jnp.float32)
            if gelu:
                part = jax.nn.gelu(part + b_ref[layer:layer + 1, cols], approximate=True)
            part = part.astype(jnp.bfloat16)
            for k, d in enumerate(devs):
                outs[pl.ds(pl.multiple_of(d * rows, rows), rows), out_cols] = part[k * rows:(k + 1) * rows]

        if n_out == 1:
            def body(n, carry):
                cols = pl.ds(pl.multiple_of(n * step, step), step)
                piece(cols, outs[0], cols)
                return carry
            lax.fori_loop(0, w_ref.shape[1] // step, body, 0)
        else:
            if tail:
                for d in devs:
                    tails_out[pl.ds(pl.multiple_of(d * rows, rows), rows), :] = buf[d, :, pl.ds(width, tail)]
            each = w_ref.shape[1] // n_out
            for k in range(n_out):
                piece(pl.ds(k * each, each), outs[k], pl.ds(0, each))

    def forward(i, j, h):
        if j == 0:
            if i == 0:
                send(i, j, h, 0, 1)
                send(i, j, h, 0, -1)
            elif i == -1 and h == 0:
                send(i, j, h, 0, 1)
            elif i == 1 and h == 1:
                send(i, j, h, 0, -1)
            send(i, j, h, 1, 1)
            send(i, j, h, 1, -1)
        elif j == -1 and h == 0:
            send(i, j, h, 1, 1)
        elif j == 1 and h == 1:
            send(i, j, h, 1, -1)
        share(i, j, h)

    for h in range(2):
        forward(0, 0, h)
    load_w.wait()
    count = len(GATHER_ORDER) // 4
    for g in range(count):
        shards = GATHER_ORDER[g * 4:g * 4 + 4]
        lead = [(i, j, 1 if 1 in (i, j) and -1 not in (i, j) else 0) for i, j in shards if (i, j) != (0, 0)]
        for i, j, h in lead + [(i, j, 1 - h) for i, j, h in lead]:
            arrived(i, j, h)
            forward(i, j, h)
        multiply(shards, place.core)
        for i, j in shards:
            for h in range(2):
                pair(i, j, h, 1 - place.core).wait_recv()
        multiply(shards, 1 - place.core)
    for copy in sent:
        copy.wait_send()


def gather_and_project(side, call_id, layer, residual, gain, shift, weight, bias, gelu, n_out, tails=None):
    rows, width = residual.shape
    tail = 0 if tails is None else tails.shape[1]
    extra = [] if tails is None else [tails]
    groups = 2 * side * side
    wide = weight.shape[2]
    vmem = pl.BlockSpec(memory_space=pltpu.VMEM)
    outs = pl.pallas_call(
        functools.partial(gather_kernel, side, layer, gelu, n_out, tail),
        out_shape=[jax.ShapeDtypeStruct((groups * rows, wide // n_out), jnp.bfloat16)] * n_out + [jax.ShapeDtypeStruct((groups * rows, tail), jnp.bfloat16) for _ in extra],
        in_specs=[vmem, vmem, vmem, pl.BlockSpec(memory_space=pl.ANY), vmem] + [vmem for _ in extra],
        out_specs=[vmem] * (n_out + len(extra)),
        scratch_shapes=[
            pltpu.VMEM((width, wide), jnp.bfloat16),
            pltpu.VMEM((groups, rows, width + tail), jnp.bfloat16),
            pltpu.SemaphoreType.DMA,
            pltpu.SemaphoreType.DMA((4, groups)),
            pltpu.SemaphoreType.DMA((groups,)),
            pltpu.SemaphoreType.DMA((groups,)),
            pltpu.SemaphoreType.DMA((groups,)),
        ],
        compiler_params=pltpu.CompilerParams(collective_id=call_id, has_side_effects=True, vmem_limit_bytes=VMEM_LIMIT),
        name=f"gather_{call_id}",
    )(residual, gain, shift, weight, bias, *extra)
    return outs if len(outs) > 1 else outs[0]


def doc_causal_attention(queries, keys_in, values_in, all_ids):
    seq_len = queries.shape[0]
    score_scale = queries.shape[1] ** -0.5
    block_rows = min(QUERY_ROWS, seq_len)
    pieces = []
    for start_row in range(0, seq_len, block_rows):
        stop_row = start_row + block_rows
        scores = jnp.einsum("qe,ke->qk", queries[start_row:stop_row], keys_in[:stop_row], preferred_element_type=jnp.float32) * score_scale
        query_pos = start_row + jnp.arange(block_rows)
        key_pos = jnp.arange(stop_row)
        allowed = (key_pos[None, :] <= query_pos[:, None]) & (all_ids[start_row:stop_row, None] == all_ids[None, :stop_row])
        scores = jnp.where(allowed, scores, -1e30)
        probs_blk = jax.nn.softmax(scores, axis=-1).astype(jnp.bfloat16)
        pieces.append(jnp.einsum("qk,ke->qe", probs_blk, values_in[:stop_row], preferred_element_type=jnp.float32).astype(jnp.bfloat16))
    return jnp.concatenate(pieces, axis=0)


def solution(mesh):
    groups = mesh.shape["tp"]
    side = math.isqrt(groups // 2)
    assert 2 * side * side == groups and side == 4
    row_spec = P("dp", "tp", None)
    vec_spec = P(None, None)
    in_specs = (row_spec, P("dp", "tp"), vec_spec, vec_spec, P(None, None, None, "tp", None), P(None, "tp", None, None), vec_spec, vec_spec, vec_spec, P(None, None, "tp"), P(None, "tp"), P(None, "tp", None), vec_spec)

    def device_fn(tokens, doc_ids, norm1_gain, norm1_shift, qkv_weight, out_weight, out_bias, norm2_gain, norm2_shift, up_weight, up_bias, down_weight, down_bias):
        layers, width = norm1_gain.shape
        id_cols = jnp.broadcast_to(doc_ids[0].astype(jnp.bfloat16)[:, None], (doc_ids.shape[1], 128))
        qkv_flat = qkv_weight.reshape(layers, width, -1)
        residual = tokens[0].astype(jnp.float32)
        for layer in range(layers):
            ids = [4 * layer + k for k in range(4)]
            tails = id_cols if layer == 0 else None
            q, k, v, *gathered = gather_and_project(side, ids[0], layer, residual, norm1_gain, norm1_shift, qkv_flat, norm1_gain, False, 3, tails)
            if layer == 0:
                all_ids = gathered[0][:, 0]
            attn_out = doc_causal_attention(q, k, v, all_ids)
            residual = project_and_scatter(side, ids[1], layer, attn_out, out_weight, residual, out_bias)
            hidden = gather_and_project(side, ids[2], layer, residual, norm2_gain, norm2_shift, up_weight, up_bias, True, 1)
            residual = project_and_scatter(side, ids[3], layer, hidden, down_weight, residual, down_bias)
        return residual.astype(jnp.bfloat16)[None]

    return jax.shard_map(device_fn, mesh=mesh, in_specs=in_specs, out_specs=row_spec, check_vma=False)
```

```python
import functools
import math

import jax
import jax.numpy as jnp
from jax import lax
from jax.experimental import pallas as pl
from jax.experimental.pallas import tpu as pltpu
from jax.sharding import PartitionSpec as P

COLS = 512
MESH = pl.DeviceIdType.MESH
VMEM_LIMIT = 66 * 1000 * 1000

STEPS = (2, 1, -1, 0)


class Place:
    def __init__(self, side):
        self.side = side
        self.me = lax.axis_index("tp")
        self.core = self.me % 2
        chip = self.me // 2
        self.x = chip % side
        self.y = chip // side
        self.partner = chip * 2 + 1 - self.core
        self.first = {1: self.dev(1, 0), -1: self.dev(-1, 0)}
        self.second = {1: self.dev(0, 1), -1: self.dev(0, -1)}

    def dev(self, i, j, core=None):
        core = self.core if core is None else core
        dx = i * (1 - core) + j * core
        dy = j * (1 - core) + i * core
        return (((self.y + dy + self.side) % self.side) * self.side + (self.x + dx + self.side) % self.side) * 2 + core

    def barrier(self):
        sem = pltpu.get_barrier_semaphore()
        others = [self.first[1], self.first[-1], self.second[1], self.second[-1], self.partner]
        for other in others:
            pl.semaphore_signal(sem, inc=1, device_id={"tp": other}, device_id_type=MESH)
        pl.semaphore_wait(sem, len(others))


def by_cols(width, fn):
    step = min(COLS, width)

    def body(n, carry):
        fn(pl.ds(pl.multiple_of(n * step, step), step))
        return carry

    lax.fori_loop(0, width // step, body, 0)


def scatter_kernel(side, layer, act_ref, w_hbm, res_ref, bias_ref, out_ref, w_ref, own, snd, prt, stg, mid, fin, stg2, mid2, fin2, w_sem, pair_send, pair_recv, send_sem, recv_sem):
    load_w = pltpu.make_async_copy(w_hbm.at[layer, 0] if len(w_hbm.shape) == 4 else w_hbm.at[layer], w_ref, w_sem)
    load_w.start()
    place = Place(side)
    rows, width = res_ref.shape
    half = rows // 2
    place.barrier()
    load_w.wait()

    def remote(src, dst, slot, device):
        return pltpu.make_async_remote_copy(src_ref=src, dst_ref=dst, send_sem=send_sem.at[slot], recv_sem=recv_sem.at[slot], device_id={"tp": device}, device_id_type=MESH)

    def pair_copy(g, jj):
        return pltpu.make_async_remote_copy(src_ref=snd.at[g % 2, jj], dst_ref=prt.at[g, jj], send_sem=pair_send.at[g, jj], recv_sem=pair_recv.at[g, jj], device_id={"tp": place.partner}, device_id_type=MESH)

    def product(core, g, dst):
        starts = [pl.multiple_of(place.dev(STEPS[g], j, core) * rows, rows) for j in STEPS]

        def piece(cols):
            lhs = jnp.concatenate([act_ref[pl.ds(s, rows), :] for s in starts], axis=0)
            part = jnp.dot(lhs, w_ref[:, cols], preferred_element_type=jnp.float32).astype(jnp.bfloat16)
            for jj in range(side):
                dst[jj, :, cols] = part[jj * rows:(jj + 1) * rows]

        by_cols(width, piece)

    def pair_sum(g, jj, h, cols):
        at = pl.ds(h * half, half)
        return own[g, jj, at, cols].astype(jnp.float32) + prt[g, jj, at, cols].astype(jnp.float32)

    far, plus, minus, here = range(side)
    sent = []

    def send(src, dst, slot, device):
        copy = remote(src, dst, slot, device)
        copy.start()
        sent.append(copy)

    def arrived(dst, slot):
        remote(dst, dst, slot, place.me).wait_recv()

    def open_group(g):
        for jj in range(side):
            if g >= 2:
                pair_copy(g - 2, jj).wait_send()
        product(1 - place.core, g, snd.at[g % 2])
        for jj in range(side):
            pair_copy(g, jj).start()
        product(place.core, g, own.at[g])
        for jj in range(side):
            pair_copy(g, jj).wait_recv()
        for k, (jj, h) in enumerate(((far, 0), (far, 1), (plus, 1), (minus, 0))):
            def stage(cols, k=k, jj=jj, h=h):
                stg[g, k, :, cols] = pair_sum(g, jj, h, cols)
            by_cols(width, stage)
            dst = mid.at[g, k] if k < 2 else fin.at[g, k]
            slot = 6 * g + (4 + k if k < 2 else k)
            send(stg.at[g, k], dst, slot, place.second[1 if k % 2 == 0 else -1])

    def relay(g):
        for k, (jj, h) in enumerate(((plus, 0), (minus, 1))):
            arrived(mid.at[g, k], 6 * g + 4 + k)
            def add(cols, k=k, jj=jj, h=h):
                mid[g, k, :, cols] += pair_sum(g, jj, h, cols)
            by_cols(width, add)
            send(mid.at[g, k], fin.at[g, k], 6 * g + k, place.second[1 if k == 0 else -1])

    base = 6 * side

    def close_group(g):
        for k in range(4):
            arrived(fin.at[g, k], 6 * g + k)

        def total(h, cols):
            return pair_sum(g, here, h, cols) + fin[g, 0 if h == 0 else 1, :, cols] + fin[g, 3 if h == 0 else 2, :, cols]

        def keep(k, h):
            def fn(cols):
                stg2[k, :, cols] = total(h, cols)
            by_cols(width, fn)

        def join(k):
            arrived(mid2.at[k], base + 4 + k)
            def fn(cols):
                mid2[k, :, cols] += total(k, cols)
            by_cols(width, fn)
            send(mid2.at[k], fin2.at[k], base + k, place.first[1 if k == 0 else -1])

        if g == far:
            keep(0, 0)
            send(stg2.at[0], mid2.at[0], base + 4, place.first[1])
            keep(1, 1)
            send(stg2.at[1], mid2.at[1], base + 5, place.first[-1])
        elif g == plus:
            keep(2, 1)
            send(stg2.at[2], fin2.at[2], base + 2, place.first[1])
            join(0)
        elif g == minus:
            keep(3, 0)
            send(stg2.at[3], fin2.at[3], base + 3, place.first[-1])
            join(1)
        else:
            for k in range(4):
                arrived(fin2.at[k], base + k)
            for h in range(2):
                def fn(cols, h=h):
                    at = pl.ds(h * half, half)
                    summed = total(h, cols) + fin2[0 if h == 0 else 1, :, cols] + fin2[3 if h == 0 else 2, :, cols]
                    out_ref[at, cols] = res_ref[at, cols] + (summed + bias_ref[layer:layer + 1, cols])
                by_cols(width, fn)

    open_group(0)
    open_group(1)
    relay(0)
    open_group(2)
    relay(1)
    close_group(0)
    open_group(3)
    relay(2)
    close_group(1)
    relay(3)
    close_group(2)
    close_group(3)
    for g in (side - 2, side - 1):
        for jj in range(side):
            pair_copy(g, jj).wait_send()
    for copy in sent:
        copy.wait_send()


def project_and_scatter(side, call_id, layer, act, weight, residual, bias):
    rows, width = residual.shape
    depth = act.shape[1]
    half = rows // 2
    quad = (side, side, rows, width)
    part = (side, 2, half, width)
    vmem = pl.BlockSpec(memory_space=pltpu.VMEM)
    return pl.pallas_call(
        functools.partial(scatter_kernel, side, layer),
        out_shape=jax.ShapeDtypeStruct((rows, width), jnp.float32),
        in_specs=[vmem, pl.BlockSpec(memory_space=pl.ANY), vmem, vmem],
        out_specs=vmem,
        scratch_shapes=[
            pltpu.VMEM((depth, width), jnp.bfloat16),
            pltpu.VMEM(quad, jnp.bfloat16),
            pltpu.VMEM((2,) + quad[1:], jnp.bfloat16),
            pltpu.VMEM(quad, jnp.bfloat16),
            pltpu.VMEM((side, 4, half, width), jnp.float32),
            pltpu.VMEM(part, jnp.float32),
            pltpu.VMEM((side, 4, half, width), jnp.float32),
            pltpu.VMEM((4, half, width), jnp.float32),
            pltpu.VMEM((2, half, width), jnp.float32),
            pltpu.VMEM((4, half, width), jnp.float32),
            pltpu.SemaphoreType.DMA,
            pltpu.SemaphoreType.DMA((side, side)),
            pltpu.SemaphoreType.DMA((side, side)),
            pltpu.SemaphoreType.DMA((6 * side + 6,)),
            pltpu.SemaphoreType.DMA((6 * side + 6,)),
        ],
        compiler_params=pltpu.CompilerParams(collective_id=call_id, has_side_effects=True, vmem_limit_bytes=VMEM_LIMIT),
        name=f"scatter_{call_id}",
    )(act, weight, residual, bias)


GATHER_ORDER = sorted(((i, j) for i in STEPS for j in STEPS), key=lambda at: (2 * abs(at[0]) + 3 * abs(at[1]), at))


def gather_kernel(side, layer, gelu, tail, res_ref, gain_ref, shift_ref, w_hbm, b_ref, *refs):
    tails, refs = (refs[0], refs[1:]) if tail else (None, refs)
    out, refs = refs[0], refs[1:]
    tails_out, refs = (refs[0], refs[1:]) if tail else (None, refs)
    (w_ref, buf, w_sem, send_sem, recv_sem, pair_send, pair_recv) = refs
    if len(w_hbm.shape) == 3:
        loads = [pltpu.make_async_copy(w_hbm.at[layer], w_ref, w_sem.at[0])]
    else:
        each = w_hbm.shape[4]
        loads = [pltpu.make_async_copy(w_hbm.at[layer, k, 0], w_ref.at[:, pl.ds(k * each, each)], w_sem.at[k]) for k in range(w_hbm.shape[1])]
    for load in loads:
        load.start()
    place = Place(side)
    rows, width = res_ref.shape
    half = rows // 2
    for at in (pl.ds(0, half), pl.ds(half, half)):
        residual = res_ref[at, :]
        centered = residual - jnp.mean(residual, axis=-1, keepdims=True)
        variance = jnp.mean(centered * centered, axis=-1, keepdims=True)
        normed = centered * lax.rsqrt(variance + 1e-5) * gain_ref[layer:layer + 1, :] + shift_ref[layer:layer + 1, :]
        buf[place.me, at, pl.ds(0, width)] = normed.astype(jnp.bfloat16)
    if tail:
        buf[place.me, :, pl.ds(width, tail)] = tails[...]
    place.barrier()

    def view(i, j, h, core=None):
        return buf.at[place.dev(i, j, core), pl.ds(h * half, half)]

    def wrap(k):
        return (k + 1) % side - 1

    def slot(i, j, h):
        return ((i % side) * side + j % side) * 2 + h

    sent = []

    def send(i, j, h, axis, step):
        there = (wrap(i - step), j) if axis == 0 else (i, wrap(j - step))
        device = (place.first, place.second)[axis][step]
        index = slot(i, j, h)
        copy = pltpu.make_async_remote_copy(src_ref=view(i, j, h), dst_ref=view(i, j, h), send_sem=send_sem.at[axis * 2 + (step > 0), index], recv_sem=recv_sem.at[slot(*there, h)], device_id={"tp": device}, device_id_type=MESH)
        copy.start()
        sent.append(copy)

    def pair(i, j, h, core=None):
        index = slot(i, j, h)
        ref = view(i, j, h, core)
        return pltpu.make_async_remote_copy(src_ref=ref, dst_ref=ref, send_sem=pair_send.at[index], recv_sem=pair_recv.at[index], device_id={"tp": place.partner}, device_id_type=MESH)

    def share(i, j, h):
        copy = pair(i, j, h)
        copy.start()
        sent.append(copy)

    def arrived(i, j, h):
        ref = view(i, j, h)
        pltpu.make_async_remote_copy(src_ref=ref, dst_ref=ref, send_sem=send_sem.at[0, 0], recv_sem=recv_sem.at[slot(i, j, h)], device_id={"tp": place.me}, device_id_type=MESH).wait_recv()

    def multiply(shards, core):
        devs = [place.dev(i, j, core) for i, j in shards]
        wide = w_ref.shape[1]
        step = wide if wide % 256 else 256
        at = [pl.ds(pl.multiple_of(d * rows, rows), rows) for d in devs]
        if tail:
            for d, where in zip(devs, at):
                tails_out[where, :] = buf[d, :, pl.ds(width, tail)]

        def piece(cols):
            lhs = jnp.concatenate([buf[d, :, pl.ds(0, width)] for d in devs], axis=0)
            part = jnp.dot(lhs, w_ref[:, cols], preferred_element_type=jnp.float32)
            if gelu:
                part = jax.nn.gelu(part + b_ref[layer:layer + 1, cols], approximate=True)
            part = part.astype(jnp.bfloat16)
            for k, where in enumerate(at):
                out[where, cols] = part[k * rows:(k + 1) * rows]

        if step == wide:
            piece(pl.ds(0, wide))
        else:
            def body(n, carry):
                piece(pl.ds(pl.multiple_of(n * step, step), step))
                return carry
            lax.fori_loop(0, wide // step, body, 0)

    def forward(i, j, h):
        if j == 0:
            if i == 0:
                send(i, j, h, 0, 1)
                send(i, j, h, 0, -1)
            elif i == -1 and h == 0:
                send(i, j, h, 0, 1)
            elif i == 1 and h == 1:
                send(i, j, h, 0, -1)
            send(i, j, h, 1, 1)
            send(i, j, h, 1, -1)
        elif j == -1 and h == 0:
            send(i, j, h, 1, 1)
        elif j == 1 and h == 1:
            send(i, j, h, 1, -1)
        share(i, j, h)

    for h in range(2):
        forward(0, 0, h)
    for load in loads:
        load.wait()
    count = len(GATHER_ORDER) // 4
    for g in range(count):
        shards = GATHER_ORDER[g * 4:g * 4 + 4]
        lead = [(i, j, 1 if 1 in (i, j) and -1 not in (i, j) else 0) for i, j in shards if (i, j) != (0, 0)]
        for i, j, h in lead + [(i, j, 1 - h) for i, j, h in lead]:
            arrived(i, j, h)
            forward(i, j, h)
        for i, j in shards:
            for h in range(2):
                pair(i, j, h, 1 - place.core).wait_recv()

        def both(k, carry):
            multiply(shards, (place.core + k) % 2)
            return carry

        lax.fori_loop(0, 2, both, 0)
    for copy in sent:
        copy.wait_send()


def gather_and_project(side, call_id, layer, residual, gain, shift, weight, bias, gelu, tails=None):
    rows, width = residual.shape
    tail = 0 if tails is None else tails.shape[1]
    extra = [] if tails is None else [tails]
    groups = 2 * side * side
    wide = weight.shape[2] if weight.ndim == 3 else weight.shape[1] * weight.shape[4]
    vmem = pl.BlockSpec(memory_space=pltpu.VMEM)
    outs = pl.pallas_call(
        functools.partial(gather_kernel, side, layer, gelu, tail),
        out_shape=[jax.ShapeDtypeStruct((groups * rows, wide), jnp.bfloat16)] + [jax.ShapeDtypeStruct((groups * rows, tail), jnp.bfloat16) for _ in extra],
        in_specs=[vmem, vmem, vmem, pl.BlockSpec(memory_space=pl.ANY), vmem] + [vmem for _ in extra],
        out_specs=[vmem] * (1 + len(extra)),
        scratch_shapes=[
            pltpu.VMEM((width, wide), jnp.bfloat16),
            pltpu.VMEM((groups, rows, width + tail), jnp.bfloat16),
            pltpu.SemaphoreType.DMA((3,)),
            pltpu.SemaphoreType.DMA((4, groups)),
            pltpu.SemaphoreType.DMA((groups,)),
            pltpu.SemaphoreType.DMA((groups,)),
            pltpu.SemaphoreType.DMA((groups,)),
        ],
        compiler_params=pltpu.CompilerParams(collective_id=call_id, has_side_effects=True, vmem_limit_bytes=VMEM_LIMIT),
        name=f"gather_{call_id}",
    )(residual, gain, shift, weight, bias, *extra)
    return outs if len(outs) > 1 else outs[0]


QUERY_BLOCK = 256
RING = ((-1, 0), (1, 1), (-1, 1), (1, 0), (2, 0), (2, 1))


def attend_kernel(side, layer, qkv_ref, ids_ref, row_ids_ref, w_hbm, res_ref, bias_ref, out_ref, w_own, wbuf, obuf, o_own, scores, acc, rbuf, load_sem, ws_send, ws_recv, wg_send, wg_recv, os_send, os_recv, og_send, og_recv, op_send, op_recv, back_send, back_recv):
    load_w = pltpu.make_async_copy(w_hbm.at[layer, 0], w_own, load_sem)
    load_w.start()
    me = lax.axis_index("tp")
    core = me % 2
    x = me // 2 % side
    y = me // 2 // side
    rows, width = res_ref.shape
    dim = w_own.shape[0]
    share = width // (2 * side)
    parts, _, _, cols = wbuf.shape
    line = rows * 2 * side
    steps = STEPS

    def at(dx, dy, dc):
        return (((y + dy + side) % side) * side + (x + dx + side) % side) * 2 + (core + dc) % 2

    peers = [at(dx, 0, dc) for dx in steps for dc in (1, 0) if (dx, dc) != (0, 0)]
    columns = [at(0, dy, 0) for dy in steps[:3]]
    barrier = pltpu.get_barrier_semaphore()
    for peer in peers + columns:
        pl.semaphore_signal(barrier, inc=1, device_id={"tp": peer}, device_id_type=MESH)
    pl.semaphore_wait(barrier, len(peers) + len(columns))
    load_w.wait()

    sent = []

    def send(src, dst, send_sem, recv_sem, device):
        if device is None:
            copy = pltpu.make_async_copy(src, dst, recv_sem)
        else:
            copy = pltpu.make_async_remote_copy(src_ref=src, dst_ref=dst, send_sem=send_sem, recv_sem=recv_sem, device_id={"tp": device}, device_id_type=MESH)
            sent.append(copy)
        copy.start()

    def arrived(dst, recv_sem):
        pltpu.make_async_copy(dst, dst, recv_sem).wait()

    def target(dx, dy, dc):
        return None if (dx, dy, dc) == (0, 0, 0) else at(dx, dy, dc)

    def first_col(device, part):
        return pl.multiple_of(device % (2 * side) * share + part * cols, 128)

    for part in range(parts):
        for k, dx in enumerate(steps):
            for dc in range(2):
                src = w_own.at[:, pl.ds(first_col(at(dx, 0, dc), part), cols)]
                send(src, wbuf.at[part, me], ws_send.at[part, k, dc], ws_recv.at[part, k, dc], target(dx, 0, dc))

    def w_slots(part, j, h):
        return wbuf.at[part, pl.ds(((y + j + side) % side) * 2 * side + h * side, side)]

    def w_ring(part, j, h):
        index = RING.index((j, h))
        return wg_send.at[part, index], wg_recv.at[part, index]

    def w_first(part):
        for k, dx in enumerate(steps):
            for dc in range(2):
                arrived(wbuf.at[part, at(-dx, 0, dc)], ws_recv.at[part, k, dc])
        for h in range(2):
            send(w_slots(part, 0, h), w_slots(part, 0, h), *w_ring(part, -1, h), at(0, 1, 0))
            send(w_slots(part, 0, 1 - h), w_slots(part, 0, 1 - h), *w_ring(part, 1, 1 - h), at(0, -1, 0))

    def w_arrived(part, j, h):
        arrived(w_slots(part, j, h), w_ring(part, j, h)[1])

    def w_relay(part):
        w_arrived(part, -1, 0)
        send(w_slots(part, -1, 0), w_slots(part, -1, 0), *w_ring(part, 2, 0), at(0, 1, 0))
        w_arrived(part, 1, 1)
        send(w_slots(part, 1, 1), w_slots(part, 1, 1), *w_ring(part, 2, 1), at(0, -1, 0))

    block = scores.shape[0]
    half = block // 2

    def attend(b):
        q_rows = pl.ds(pl.multiple_of(b * block, block), block)
        q = qkv_ref[q_rows, pl.ds(0, dim)]
        q_ids = ids_ref[q_rows, 0:1].astype(jnp.float32)
        q_pos = b * block + lax.broadcasted_iota(jnp.int32, (block, block), 0)

        def chunk(c):
            return pl.ds(pl.multiple_of(c * block, block), block)

        def score(c, top):
            s = lax.dot_general(q, qkv_ref[chunk(c), pl.ds(dim, dim)], (((1,), (1,)), ((), ())), preferred_element_type=jnp.float32) * dim ** -0.5
            k_pos = c * block + lax.broadcasted_iota(jnp.int32, (block, block), 1)
            allowed = (k_pos <= q_pos) & (row_ids_ref[0:1, chunk(c)] == q_ids)
            s = jnp.where(allowed, s, -1e30)
            scores[:, chunk(c)] = s
            return jnp.maximum(top, jnp.maximum(s[:, :half], s[:, half:]))

        top = jnp.max(lax.fori_loop(0, b + 1, score, jnp.full((block, half), -1e30, jnp.float32)), axis=-1, keepdims=True)

        def power(c, total):
            e = jnp.exp(scores[:, chunk(c)] - top)
            scores[:, chunk(c)] = e
            return total + (e[:, :half] + e[:, half:])

        total = jnp.sum(lax.fori_loop(0, b + 1, power, jnp.zeros((block, half), jnp.float32)), axis=-1, keepdims=True)
        inverse = 1.0 / total

        def mix(c, mixed):
            probs = (scores[:, chunk(c)] * inverse).astype(jnp.bfloat16)
            return mixed + jnp.dot(probs, qkv_ref[chunk(c), pl.ds(2 * dim, dim)], preferred_element_type=jnp.float32)

        o_own[q_rows, :] = lax.fori_loop(0, b + 1, mix, jnp.zeros((block, dim), jnp.float32)).astype(jnp.bfloat16)

    def o_slot(c, xx, yy):
        return (c * side + xx) * side + yy

    def attend_line(k):
        n = (y + steps[k] + side) % side

        def body(b, carry):
            attend(n * (line // block) + b)
            return carry

        lax.fori_loop(0, line // block, body, 0)
        src = o_own.at[pl.ds(pl.multiple_of(n * line, line), line)]
        send(src, obuf.at[o_slot(core, x, y)], os_send.at[k], os_recv.at[k], target(0, steps[k], 0))

    def o_slots(i, h, dc=0):
        return obuf.at[pl.ds(o_slot((core + dc) % 2, (x + i + side) % side, h * (side // 2)), side // 2)]

    def o_send(i, h, step, index):
        send(o_slots(i, h), o_slots(i, h), og_send.at[index], og_recv.at[index], at(step, 0, 0))

    def o_share(k, i, h):
        send(o_slots(i, h), o_slots(i, h), op_send.at[k], op_recv.at[k], at(0, 0, 1))

    attend_line(0)
    attend_line(1)
    w_first(0)
    attend_line(2)
    attend_line(3)
    w_relay(0)
    for k, dy in enumerate(steps):
        arrived(obuf.at[o_slot(core, x, (y - dy + side) % side)], os_recv.at[k])
    for h in range(2):
        o_send(0, h, 1, RING.index((-1, h)))
        o_send(0, 1 - h, -1, RING.index((1, 1 - h)))
    for part in range(1, parts):
        w_first(part)
    for h in range(2):
        o_share(h, 0, h)
    for k, (i, h) in enumerate(RING):
        arrived(o_slots(i, h), og_recv.at[k])
        if (i, h) == (-1, 0):
            o_send(i, h, 1, RING.index((2, 0)))
        if (i, h) == (1, 1):
            o_send(i, h, -1, RING.index((2, 1)))
        o_share(2 + k, i, h)
        if k == 3:
            for part in range(1, parts):
                w_relay(part)
    for k, (i, h) in enumerate(((0, 0), (0, 1)) + RING):
        arrived(o_slots(i, h, 1), op_recv.at[k])

    strip = min(128, line)

    def project(part, j):
        yy = (y + j + side) % side

        def body(n, carry):
            at_rows = pl.ds(pl.multiple_of(n * strip, strip), strip)
            total = None if j == 0 else acc[part, at_rows, :]
            for xx in range(side):
                for c in range(2):
                    head = jnp.dot(obuf[o_slot(c, xx, yy), at_rows, :], wbuf[part, (yy * side + xx) * 2 + c], preferred_element_type=jnp.float32)
                    head = head.astype(jnp.bfloat16).astype(jnp.float32)
                    total = head if total is None else total + head
            acc[part, at_rows, :] = total
            return carry

        lax.fori_loop(0, line // strip, body, 0)

    def back_rows(device):
        return pl.ds(pl.multiple_of(device % (2 * side) * rows, rows), rows)

    for part in range(parts):
        project(part, 0)
        for j in (-1, 1, 2):
            for h in range(2):
                if (j, h) not in ((-1, 0), (1, 1)):
                    w_arrived(part, j, h)
            project(part, j)
        for k, dx in enumerate(steps):
            for dc in range(2):
                src = acc.at[part, back_rows(at(dx, 0, dc))]
                dst = rbuf.at[:, pl.ds(first_col(me, part), cols)]
                send(src, dst, back_send.at[part, k, dc], back_recv.at[part, k, dc], target(dx, 0, dc))
    for part in range(parts):
        for k, dx in enumerate(steps):
            for dc in range(2):
                arrived(rbuf.at[:, pl.ds(first_col(at(-dx, 0, dc), part), cols)], back_recv.at[part, k, dc])

    def finish(at_cols):
        out_ref[:, at_cols] = res_ref[:, at_cols] + (rbuf[:, at_cols] + bias_ref[layer:layer + 1, at_cols])

    by_cols(width, finish)
    for copy in sent:
        copy.wait_send()


def attend_and_project(side, call_id, layer, qkv, ids, row_ids, weight, residual, bias):
    rows, width = residual.shape
    seq, dim = qkv.shape[0], weight.shape[2]
    groups = 2 * side * side
    parts = 2
    cols = width // (2 * side) // parts
    block = min(QUERY_BLOCK, rows * 2 * side)
    vmem = pl.BlockSpec(memory_space=pltpu.VMEM)
    dma = pltpu.SemaphoreType.DMA
    return pl.pallas_call(
        functools.partial(attend_kernel, side, layer),
        out_shape=jax.ShapeDtypeStruct((rows, width), jnp.float32),
        in_specs=[vmem, vmem, vmem, pl.BlockSpec(memory_space=pl.ANY), vmem, vmem],
        out_specs=vmem,
        scratch_shapes=[
            pltpu.VMEM((dim, width), jnp.bfloat16),
            pltpu.VMEM((parts, groups, dim, cols), jnp.bfloat16),
            pltpu.VMEM((groups, rows * 2 * side, dim), jnp.bfloat16),
            pltpu.VMEM((seq, dim), jnp.bfloat16),
            pltpu.VMEM((block, seq), jnp.float32),
            pltpu.VMEM((parts, rows * 2 * side, cols), jnp.float32),
            pltpu.VMEM((rows, width), jnp.float32),
            dma,
            dma((parts, side, 2)), dma((parts, side, 2)),
            dma((parts, 6)), dma((parts, 6)),
            dma((side,)), dma((side,)),
            dma((6,)), dma((6,)),
            dma((8,)), dma((8,)),
            dma((parts, side, 2)), dma((parts, side, 2)),
        ],
        compiler_params=pltpu.CompilerParams(collective_id=call_id, has_side_effects=True, vmem_limit_bytes=VMEM_LIMIT),
        name=f"attend_{call_id}",
    )(qkv, ids, row_ids, weight, residual, bias)


def solution(mesh):
    groups = mesh.shape["tp"]
    side = math.isqrt(groups // 2)
    assert 2 * side * side == groups and side == 4
    row_spec = P("dp", "tp", None)
    vec_spec = P()
    second = P(None, "tp")
    in_specs = (row_spec, P("dp", "tp"), vec_spec, vec_spec, P(None, None, None, "tp"), second, vec_spec, vec_spec, vec_spec, P(None, None, "tp"), second, second, vec_spec)

    def device_fn(tokens, doc_ids, norm1_gain, norm1_shift, qkv_weight, out_weight, out_bias, norm2_gain, norm2_shift, up_weight, up_bias, down_weight, down_bias):
        layers = norm1_gain.shape[0]
        id_cols = jnp.broadcast_to(doc_ids[0].astype(jnp.bfloat16)[:, None], (doc_ids.shape[1], 128))
        qkv_thirds = jnp.transpose(qkv_weight, (0, 2, 3, 1, 4))
        residual = tokens[0].astype(jnp.float32)
        for layer in range(layers):
            ids = [4 * layer + k for k in range(4)]
            tails = id_cols if layer == 0 else None
            qkv = gather_and_project(side, ids[0], layer, residual, norm1_gain, norm1_shift, qkv_thirds, norm1_gain, False, tails)
            if layer == 0:
                qkv, all_ids = qkv
                row_ids = all_ids[:, 0].astype(jnp.float32)[None]
            residual = attend_and_project(side, ids[1], layer, qkv, all_ids, row_ids, out_weight, residual, out_bias)
            hidden = gather_and_project(side, ids[2], layer, residual, norm2_gain, norm2_shift, up_weight, up_bias, True)
            residual = project_and_scatter(side, ids[3], layer, hidden, down_weight, residual, down_bias)
        return residual.astype(jnp.bfloat16)[None]

    return jax.shard_map(device_fn, mesh=mesh, in_specs=in_specs, out_specs=row_spec, check_vma=False)
```

```python
import functools
import math

import jax
import jax.numpy as jnp
from jax import lax
from jax.experimental import pallas as pl
from jax.experimental.pallas import tpu as pltpu
from jax.sharding import PartitionSpec as P

COLS = 512
MESH = pl.DeviceIdType.MESH
VMEM_LIMIT = 66 * 1000 * 1000

STEPS = (2, 1, -1, 0)
OTHER_SIDE = (2, -1, 1, 0)


class Place:
    def __init__(self, side):
        self.side = side
        self.me = lax.axis_index("tp")
        self.core = self.me % 2
        chip = self.me // 2
        self.x = chip % side
        self.y = chip // side
        self.partner = chip * 2 + 1 - self.core
        self.first = {1: self.dev(1, 0), -1: self.dev(-1, 0)}
        self.second = {1: self.dev(0, 1), -1: self.dev(0, -1)}

    def dev(self, i, j, core=None):
        core = self.core if core is None else core
        dx = i * (1 - core) + j * core
        dy = j * (1 - core) + i * core
        return (((self.y + dy + self.side) % self.side) * self.side + (self.x + dx + self.side) % self.side) * 2 + core

    def barrier(self):
        sem = pltpu.get_barrier_semaphore()
        others = [self.first[1], self.first[-1], self.second[1], self.second[-1], self.partner]
        for other in others:
            pl.semaphore_signal(sem, inc=1, device_id={"tp": other}, device_id_type=MESH)
        pl.semaphore_wait(sem, len(others))


def by_cols(width, fn):
    step = min(COLS, width)

    def body(n, carry):
        fn(pl.ds(pl.multiple_of(n * step, step), step))
        return carry

    lax.fori_loop(0, width // step, body, 0)


def scatter_kernel(side, layer, act_ref, w_hbm, res_ref, bias_ref, out_ref, w_ref, own, snd, prt, stg, mid, fin, stg2, mid2, fin2, w_sem, pair_send, pair_recv, send_sem, recv_sem):
    load_w = pltpu.make_async_copy(w_hbm.at[layer, 0] if len(w_hbm.shape) == 4 else w_hbm.at[layer], w_ref, w_sem)
    load_w.start()
    place = Place(side)
    rows, width = res_ref.shape
    half = rows // 2
    place.barrier()
    load_w.wait()

    def remote(src, dst, slot, device):
        return pltpu.make_async_remote_copy(src_ref=src, dst_ref=dst, send_sem=send_sem.at[slot], recv_sem=recv_sem.at[slot], device_id={"tp": device}, device_id_type=MESH)

    def pair_copy(g, jj):
        return pltpu.make_async_remote_copy(src_ref=snd.at[g % 2, jj], dst_ref=prt.at[g, jj], send_sem=pair_send.at[g, jj], recv_sem=pair_recv.at[g, jj], device_id={"tp": place.partner}, device_id_type=MESH)

    def product(core, g, dst):
        starts = [pl.multiple_of(place.dev(i, j, core) * rows + h * half, half) for j in STEPS for h, i in enumerate((STEPS[g], OTHER_SIDE[g]))]

        def piece(cols):
            lhs = jnp.concatenate([act_ref[pl.ds(s, half), :] for s in starts], axis=0)
            part = jnp.dot(lhs, w_ref[:, cols], preferred_element_type=jnp.float32).astype(jnp.bfloat16)
            for jj in range(side):
                dst[jj, :, cols] = part[jj * rows:(jj + 1) * rows]

        by_cols(width, piece)

    def pair_sum(g, jj, h, cols):
        at = pl.ds(h * half, half)
        return own[g, jj, at, cols].astype(jnp.float32) + prt[g, jj, at, cols].astype(jnp.float32)

    far, plus, minus, here = range(side)
    sent = []

    def send(src, dst, slot, device):
        copy = remote(src, dst, slot, device)
        copy.start()
        sent.append(copy)

    def arrived(dst, slot):
        remote(dst, dst, slot, place.me).wait_recv()

    def open_group(g):
        for jj in range(side):
            if g >= 2:
                pair_copy(g - 2, jj).wait_send()
        product(1 - place.core, g, snd.at[g % 2])
        for jj in range(side):
            pair_copy(g, jj).start()
        product(place.core, g, own.at[g])
        shared = set()
        for k, (jj, h) in enumerate(((far, 0), (far, 1), (plus, 1), (minus, 0))):
            if jj not in shared:
                shared.add(jj)
                pair_copy(g, jj).wait_recv()
            def stage(cols, k=k, jj=jj, h=h):
                stg[g, k, :, cols] = pair_sum(g, jj, h, cols)
            by_cols(width, stage)
            dst = mid.at[g, k] if k < 2 else fin.at[g, k]
            slot = 6 * g + (4 + k if k < 2 else k)
            send(stg.at[g, k], dst, slot, place.second[1 if k % 2 == 0 else -1])

    def relay(g):
        for k, (jj, h) in enumerate(((plus, 0), (minus, 1))):
            arrived(mid.at[g, k], 6 * g + 4 + k)
            def add(cols, k=k, jj=jj, h=h):
                mid[g, k, :, cols] += pair_sum(g, jj, h, cols)
            by_cols(width, add)
            send(mid.at[g, k], fin.at[g, k], 6 * g + k, place.second[1 if k == 0 else -1])

    base = 6 * side

    def close_group(g):
        pair_copy(g, here).wait_recv()
        for k in range(4):
            arrived(fin.at[g, k], 6 * g + k)

        def total(h, cols):
            return pair_sum(g, here, h, cols) + fin[g, 0 if h == 0 else 1, :, cols] + fin[g, 3 if h == 0 else 2, :, cols]

        def keep(k, h):
            def fn(cols):
                stg2[k, :, cols] = total(h, cols)
            by_cols(width, fn)

        def join(k):
            arrived(mid2.at[k], base + 4 + k)
            def fn(cols):
                mid2[k, :, cols] += total(k, cols)
            by_cols(width, fn)
            send(mid2.at[k], fin2.at[k], base + k, place.first[1 if k == 0 else -1])

        if g == far:
            keep(0, 0)
            send(stg2.at[0], mid2.at[0], base + 4, place.first[1])
            keep(1, 1)
            send(stg2.at[1], mid2.at[1], base + 5, place.first[-1])
        elif g == plus:
            join(0)
            join(1)
        elif g == minus:
            keep(2, 1)
            send(stg2.at[2], fin2.at[2], base + 2, place.first[1])
            keep(3, 0)
            send(stg2.at[3], fin2.at[3], base + 3, place.first[-1])
        else:
            for k in range(4):
                arrived(fin2.at[k], base + k)
            for h in range(2):
                def fn(cols, h=h):
                    at = pl.ds(h * half, half)
                    summed = total(h, cols) + fin2[0 if h == 0 else 1, :, cols] + fin2[3 if h == 0 else 2, :, cols]
                    out_ref[at, cols] = res_ref[at, cols] + (summed + bias_ref[layer:layer + 1, cols])
                by_cols(width, fn)

    open_group(0)
    open_group(1)
    open_group(2)
    relay(0)
    open_group(3)
    relay(1)
    close_group(0)
    relay(2)
    close_group(1)
    relay(3)
    close_group(2)
    close_group(3)
    for g in (side - 2, side - 1):
        for jj in range(side):
            pair_copy(g, jj).wait_send()
    for copy in sent:
        copy.wait_send()


def project_and_scatter(side, call_id, layer, act, weight, residual, bias):
    rows, width = residual.shape
    depth = act.shape[1]
    half = rows // 2
    quad = (side, side, rows, width)
    part = (side, 2, half, width)
    vmem = pl.BlockSpec(memory_space=pltpu.VMEM)
    return pl.pallas_call(
        functools.partial(scatter_kernel, side, layer),
        out_shape=jax.ShapeDtypeStruct((rows, width), jnp.float32),
        in_specs=[vmem, pl.BlockSpec(memory_space=pl.ANY), vmem, vmem],
        out_specs=vmem,
        scratch_shapes=[
            pltpu.VMEM((depth, width), jnp.bfloat16),
            pltpu.VMEM(quad, jnp.bfloat16),
            pltpu.VMEM((2,) + quad[1:], jnp.bfloat16),
            pltpu.VMEM(quad, jnp.bfloat16),
            pltpu.VMEM((side, 4, half, width), jnp.float32),
            pltpu.VMEM(part, jnp.float32),
            pltpu.VMEM((side, 4, half, width), jnp.float32),
            pltpu.VMEM((4, half, width), jnp.float32),
            pltpu.VMEM((2, half, width), jnp.float32),
            pltpu.VMEM((4, half, width), jnp.float32),
            pltpu.SemaphoreType.DMA,
            pltpu.SemaphoreType.DMA((side, side)),
            pltpu.SemaphoreType.DMA((side, side)),
            pltpu.SemaphoreType.DMA((6 * side + 6,)),
            pltpu.SemaphoreType.DMA((6 * side + 6,)),
        ],
        compiler_params=pltpu.CompilerParams(collective_id=call_id, has_side_effects=True, vmem_limit_bytes=VMEM_LIMIT),
        name=f"scatter_{call_id}",
    )(act, weight, residual, bias)


GATHER_ORDER = sorted(((i, j) for i in STEPS for j in STEPS), key=lambda at: (2 * abs(at[0]) + 3 * abs(at[1]), at))


def gather_kernel(side, layer, gelu, tail, res_ref, gain_ref, shift_ref, w_hbm, b_ref, *refs):
    tails, refs = (refs[0], refs[1:]) if tail else (None, refs)
    out, refs = refs[0], refs[1:]
    tails_out, refs = (refs[0], refs[1:]) if tail else (None, refs)
    (w_ref, buf, w_sem, send_sem, recv_sem, pair_send, pair_recv) = refs
    if len(w_hbm.shape) == 3:
        loads = [pltpu.make_async_copy(w_hbm.at[layer], w_ref, w_sem.at[0])]
    else:
        each = w_hbm.shape[4]
        loads = [pltpu.make_async_copy(w_hbm.at[layer, k, 0], w_ref.at[:, pl.ds(k * each, each)], w_sem.at[k]) for k in range(w_hbm.shape[1])]
    for load in loads:
        load.start()
    place = Place(side)
    rows, width = res_ref.shape
    half = rows // 2
    for at in (pl.ds(0, half), pl.ds(half, half)):
        residual = res_ref[at, :]
        centered = residual - jnp.mean(residual, axis=-1, keepdims=True)
        variance = jnp.mean(centered * centered, axis=-1, keepdims=True)
        normed = centered * lax.rsqrt(variance + 1e-5) * gain_ref[layer:layer + 1, :] + shift_ref[layer:layer + 1, :]
        buf[place.me, at, pl.ds(0, width)] = normed.astype(jnp.bfloat16)
    if tail:
        buf[place.me, :, pl.ds(width, tail)] = tails[...]
    place.barrier()

    def view(i, j, h, core=None):
        return buf.at[place.dev(i, j, core), pl.ds(h * half, half)]

    def wrap(k):
        return (k + 1) % side - 1

    def slot(i, j, h):
        return ((i % side) * side + j % side) * 2 + h

    sent = []

    def send(i, j, h, axis, step):
        there = (wrap(i - step), j) if axis == 0 else (i, wrap(j - step))
        device = (place.first, place.second)[axis][step]
        index = slot(i, j, h)
        copy = pltpu.make_async_remote_copy(src_ref=view(i, j, h), dst_ref=view(i, j, h), send_sem=send_sem.at[axis * 2 + (step > 0), index], recv_sem=recv_sem.at[slot(*there, h)], device_id={"tp": device}, device_id_type=MESH)
        copy.start()
        sent.append(copy)

    def pair(i, j, h, core=None):
        index = slot(i, j, h)
        ref = view(i, j, h, core)
        return pltpu.make_async_remote_copy(src_ref=ref, dst_ref=ref, send_sem=pair_send.at[index], recv_sem=pair_recv.at[index], device_id={"tp": place.partner}, device_id_type=MESH)

    def share(i, j, h):
        copy = pair(i, j, h)
        copy.start()
        sent.append(copy)

    def arrived(i, j, h):
        ref = view(i, j, h)
        pltpu.make_async_remote_copy(src_ref=ref, dst_ref=ref, send_sem=send_sem.at[0, 0], recv_sem=recv_sem.at[slot(i, j, h)], device_id={"tp": place.me}, device_id_type=MESH).wait_recv()

    def multiply(shards, core):
        devs = [place.dev(i, j, core) for i, j in shards]
        wide = w_ref.shape[1]
        step = wide if wide % 256 else 256
        at = [pl.ds(pl.multiple_of(d * rows, rows), rows) for d in devs]
        if tail:
            for d, where in zip(devs, at):
                tails_out[where, :] = buf[d, :, pl.ds(width, tail)]

        def piece(cols):
            lhs = jnp.concatenate([buf[d, :, pl.ds(0, width)] for d in devs], axis=0)
            part = jnp.dot(lhs, w_ref[:, cols], preferred_element_type=jnp.float32)
            if gelu:
                part = jax.nn.gelu(part + b_ref[layer:layer + 1, cols], approximate=True)
            part = part.astype(jnp.bfloat16)
            for k, where in enumerate(at):
                out[where, cols] = part[k * rows:(k + 1) * rows]

        if step == wide:
            piece(pl.ds(0, wide))
        else:
            def body(n, carry):
                piece(pl.ds(pl.multiple_of(n * step, step), step))
                return carry
            lax.fori_loop(0, wide // step, body, 0)

    def forward(i, j, h):
        if j == 0:
            if i == 0:
                send(i, j, h, 0, 1)
                send(i, j, h, 0, -1)
            elif i == -1 and h == 0:
                send(i, j, h, 0, 1)
            elif i == 1 and h == 1:
                send(i, j, h, 0, -1)
            send(i, j, h, 1, 1)
            send(i, j, h, 1, -1)
        elif j == -1 and h == 0:
            send(i, j, h, 1, 1)
        elif j == 1 and h == 1:
            send(i, j, h, 1, -1)
        share(i, j, h)

    for h in range(2):
        forward(0, 0, h)
    for load in loads:
        load.wait()
    cuts = (0, 4, 8, 12, 14, 16)
    for start, stop in zip(cuts, cuts[1:]):
        shards = GATHER_ORDER[start:stop]
        lead = [(i, j, 1 if 1 in (i, j) and -1 not in (i, j) else 0) for i, j in shards if (i, j) != (0, 0)]
        for i, j, h in lead + [(i, j, 1 - h) for i, j, h in lead]:
            arrived(i, j, h)
            forward(i, j, h)
        for i, j in shards:
            for h in range(2):
                pair(i, j, h, 1 - place.core).wait_recv()

        def both(k, carry):
            multiply(shards, (place.core + k) % 2)
            return carry

        lax.fori_loop(0, 2, both, 0)
    for copy in sent:
        copy.wait_send()


def gather_and_project(side, call_id, layer, residual, gain, shift, weight, bias, gelu, tails=None):
    rows, width = residual.shape
    tail = 0 if tails is None else tails.shape[1]
    extra = [] if tails is None else [tails]
    groups = 2 * side * side
    wide = weight.shape[2] if weight.ndim == 3 else weight.shape[1] * weight.shape[4]
    vmem = pl.BlockSpec(memory_space=pltpu.VMEM)
    outs = pl.pallas_call(
        functools.partial(gather_kernel, side, layer, gelu, tail),
        out_shape=[jax.ShapeDtypeStruct((groups * rows, wide), jnp.bfloat16)] + [jax.ShapeDtypeStruct((groups * rows, tail), jnp.bfloat16) for _ in extra],
        in_specs=[vmem, vmem, vmem, pl.BlockSpec(memory_space=pl.ANY), vmem] + [vmem for _ in extra],
        out_specs=[vmem] * (1 + len(extra)),
        scratch_shapes=[
            pltpu.VMEM((width, wide), jnp.bfloat16),
            pltpu.VMEM((groups, rows, width + tail), jnp.bfloat16),
            pltpu.SemaphoreType.DMA((3,)),
            pltpu.SemaphoreType.DMA((4, groups)),
            pltpu.SemaphoreType.DMA((groups,)),
            pltpu.SemaphoreType.DMA((groups,)),
            pltpu.SemaphoreType.DMA((groups,)),
        ],
        compiler_params=pltpu.CompilerParams(collective_id=call_id, has_side_effects=True, vmem_limit_bytes=VMEM_LIMIT),
        name=f"gather_{call_id}",
    )(residual, gain, shift, weight, bias, *extra)
    return outs if len(outs) > 1 else outs[0]


QUERY_BLOCK = 256
RING = ((-1, 0), (1, 1), (-1, 1), (1, 0), (2, 0), (2, 1))


def attend_kernel(side, layer, qkv_ref, ids_ref, row_ids_ref, w_hbm, res_ref, bias_ref, out_ref, w_own, wbuf, obuf, o_own, scores, acc, rbuf, load_sem, ws_send, ws_recv, wg_send, wg_recv, os_send, os_recv, og_send, og_recv, op_send, op_recv, back_send, back_recv):
    load_w = pltpu.make_async_copy(w_hbm.at[layer, 0], w_own, load_sem)
    load_w.start()
    me = lax.axis_index("tp")
    core = me % 2
    x = me // 2 % side
    y = me // 2 // side
    rows, width = res_ref.shape
    dim = w_own.shape[0]
    share = width // (2 * side)
    parts, _, _, cols = wbuf.shape
    line = rows * 2 * side
    steps = STEPS

    def at(dx, dy, dc):
        return (((y + dy + side) % side) * side + (x + dx + side) % side) * 2 + (core + dc) % 2

    peers = [at(dx, 0, dc) for dx in steps for dc in (1, 0) if (dx, dc) != (0, 0)]
    columns = [at(0, dy, 0) for dy in steps[:3]]
    barrier = pltpu.get_barrier_semaphore()
    for peer in peers + columns:
        pl.semaphore_signal(barrier, inc=1, device_id={"tp": peer}, device_id_type=MESH)
    pl.semaphore_wait(barrier, len(peers) + len(columns))
    load_w.wait()

    sent = []

    def send(src, dst, send_sem, recv_sem, device):
        if device is None:
            copy = pltpu.make_async_copy(src, dst, recv_sem)
        else:
            copy = pltpu.make_async_remote_copy(src_ref=src, dst_ref=dst, send_sem=send_sem, recv_sem=recv_sem, device_id={"tp": device}, device_id_type=MESH)
            sent.append(copy)
        copy.start()

    def arrived(dst, recv_sem):
        pltpu.make_async_copy(dst, dst, recv_sem).wait()

    def target(dx, dy, dc):
        return None if (dx, dy, dc) == (0, 0, 0) else at(dx, dy, dc)

    def first_col(device, part):
        return pl.multiple_of(device % (2 * side) * share + part * cols, 128)

    for part in range(parts):
        for k, dx in enumerate(steps):
            for dc in range(2):
                src = w_own.at[:, pl.ds(first_col(at(dx, 0, dc), part), cols)]
                send(src, wbuf.at[part, me], ws_send.at[part, k, dc], ws_recv.at[part, k, dc], target(dx, 0, dc))

    def w_slots(part, j, h):
        return wbuf.at[part, pl.ds(((y + j + side) % side) * 2 * side + h * side, side)]

    def w_ring(part, j, h):
        index = RING.index((j, h))
        return wg_send.at[part, index], wg_recv.at[part, index]

    def w_first(part):
        for k, dx in enumerate(steps):
            for dc in range(2):
                arrived(wbuf.at[part, at(-dx, 0, dc)], ws_recv.at[part, k, dc])
        for h in range(2):
            send(w_slots(part, 0, h), w_slots(part, 0, h), *w_ring(part, -1, h), at(0, 1, 0))
            send(w_slots(part, 0, 1 - h), w_slots(part, 0, 1 - h), *w_ring(part, 1, 1 - h), at(0, -1, 0))

    def w_arrived(part, j, h):
        arrived(w_slots(part, j, h), w_ring(part, j, h)[1])

    def w_relay(part):
        w_arrived(part, -1, 0)
        send(w_slots(part, -1, 0), w_slots(part, -1, 0), *w_ring(part, 2, 0), at(0, 1, 0))
        w_arrived(part, 1, 1)
        send(w_slots(part, 1, 1), w_slots(part, 1, 1), *w_ring(part, 2, 1), at(0, -1, 0))

    block = scores.shape[0]
    half = block // 2

    def attend(b):
        q_rows = pl.ds(pl.multiple_of(b * block, block), block)
        q = qkv_ref[q_rows, pl.ds(0, dim)]
        q_ids = ids_ref[q_rows, 0:1].astype(jnp.float32)
        q_pos = b * block + lax.broadcasted_iota(jnp.int32, (block, block), 0)

        def chunk(c):
            return pl.ds(pl.multiple_of(c * block, block), block)

        def score(c, top):
            s = lax.dot_general(q, qkv_ref[chunk(c), pl.ds(dim, dim)], (((1,), (1,)), ((), ())), preferred_element_type=jnp.float32) * dim ** -0.5
            k_pos = c * block + lax.broadcasted_iota(jnp.int32, (block, block), 1)
            allowed = (k_pos <= q_pos) & (row_ids_ref[0:1, chunk(c)] == q_ids)
            s = jnp.where(allowed, s, -1e30)
            scores[:, chunk(c)] = s
            return jnp.maximum(top, jnp.maximum(s[:, :half], s[:, half:]))

        top = jnp.max(lax.fori_loop(0, b + 1, score, jnp.full((block, half), -1e30, jnp.float32)), axis=-1, keepdims=True)

        def power(c, total):
            e = jnp.exp(scores[:, chunk(c)] - top)
            scores[:, chunk(c)] = e
            return total + (e[:, :half] + e[:, half:])

        total = jnp.sum(lax.fori_loop(0, b + 1, power, jnp.zeros((block, half), jnp.float32)), axis=-1, keepdims=True)
        inverse = 1.0 / total

        def mix(c, mixed):
            probs = (scores[:, chunk(c)] * inverse).astype(jnp.bfloat16)
            return mixed + jnp.dot(probs, qkv_ref[chunk(c), pl.ds(2 * dim, dim)], preferred_element_type=jnp.float32)

        o_own[q_rows, :] = lax.fori_loop(0, b + 1, mix, jnp.zeros((block, dim), jnp.float32)).astype(jnp.bfloat16)

    def o_slot(c, xx, yy):
        return (c * side + xx) * side + yy

    def attend_line(k):
        n = (y + steps[k] + side) % side

        def body(b, carry):
            attend(n * (line // block) + b)
            return carry

        lax.fori_loop(0, line // block, body, 0)
        src = o_own.at[pl.ds(pl.multiple_of(n * line, line), line)]
        send(src, obuf.at[o_slot(core, x, y)], os_send.at[k], os_recv.at[k], target(0, steps[k], 0))

    def o_slots(i, h, dc=0):
        return obuf.at[pl.ds(o_slot((core + dc) % 2, (x + i + side) % side, h * (side // 2)), side // 2)]

    def o_send(i, h, step, index):
        send(o_slots(i, h), o_slots(i, h), og_send.at[index], og_recv.at[index], at(step, 0, 0))

    def o_share(k, i, h):
        send(o_slots(i, h), o_slots(i, h), op_send.at[k], op_recv.at[k], at(0, 0, 1))

    attend_line(0)
    attend_line(1)
    w_first(0)
    attend_line(2)
    w_first(1)
    attend_line(3)
    w_relay(0)
    for k, dy in enumerate(steps):
        arrived(obuf.at[o_slot(core, x, (y - dy + side) % side)], os_recv.at[k])
    for h in range(2):
        o_send(0, h, 1, RING.index((-1, h)))
        o_send(0, 1 - h, -1, RING.index((1, 1 - h)))
    w_first(2)
    for h in range(2):
        o_share(h, 0, h)
    w_relay(1)
    w_first(3)
    for k, (i, h) in enumerate(RING):
        arrived(o_slots(i, h), og_recv.at[k])
        if (i, h) == (-1, 0):
            o_send(i, h, 1, RING.index((2, 0)))
        if (i, h) == (1, 1):
            o_send(i, h, -1, RING.index((2, 1)))
        o_share(2 + k, i, h)
        if k == 3:
            w_relay(2)
    for k, (i, h) in enumerate(((0, 0), (0, 1)) + RING):
        arrived(o_slots(i, h, 1), op_recv.at[k])

    strip = min(block, line)

    def project(part, j):
        yy = (y + j + side) % side

        def body(n, carry):
            at_rows = pl.ds(pl.multiple_of(n * strip, strip), strip)
            total = None if j == 0 else acc[part, at_rows, :]
            for xx in range(side):
                for c in range(2):
                    head = jnp.dot(obuf[o_slot(c, xx, yy), at_rows, :], wbuf[part, (yy * side + xx) * 2 + c], preferred_element_type=jnp.float32)
                    head = head.astype(jnp.bfloat16).astype(jnp.float32)
                    total = head if total is None else total + head
            acc[part, at_rows, :] = total
            return carry

        lax.fori_loop(0, line // strip, body, 0)

    def back_rows(device):
        return pl.ds(pl.multiple_of(device % (2 * side) * rows, rows), rows)

    for part in range(parts):
        project(part, 0)
        for j in (-1, 1, 2):
            for h in range(2):
                if (j, h) not in ((-1, 0), (1, 1)):
                    w_arrived(part, j, h)
            project(part, j)
        for k, dx in enumerate(steps):
            for dc in range(2):
                src = acc.at[part, back_rows(at(dx, 0, dc))]
                dst = rbuf.at[:, pl.ds(first_col(me, part), cols)]
                send(src, dst, back_send.at[part, k, dc], back_recv.at[part, k, dc], target(dx, 0, dc))
        if part == 0:
            w_relay(3)
    for part in range(parts):
        for k, dx in enumerate(steps):
            for dc in range(2):
                arrived(rbuf.at[:, pl.ds(first_col(at(-dx, 0, dc), part), cols)], back_recv.at[part, k, dc])

    def finish(at_cols):
        out_ref[:, at_cols] = res_ref[:, at_cols] + (rbuf[:, at_cols] + bias_ref[layer:layer + 1, at_cols])

    by_cols(width, finish)
    for copy in sent:
        copy.wait_send()


def attend_and_project(side, call_id, layer, qkv, ids, row_ids, weight, residual, bias):
    rows, width = residual.shape
    seq, dim = qkv.shape[0], weight.shape[2]
    groups = 2 * side * side
    parts = 4
    cols = width // (2 * side) // parts
    block = min(QUERY_BLOCK, rows * 2 * side)
    vmem = pl.BlockSpec(memory_space=pltpu.VMEM)
    dma = pltpu.SemaphoreType.DMA
    return pl.pallas_call(
        functools.partial(attend_kernel, side, layer),
        out_shape=jax.ShapeDtypeStruct((rows, width), jnp.float32),
        in_specs=[vmem, vmem, vmem, pl.BlockSpec(memory_space=pl.ANY), vmem, vmem],
        out_specs=vmem,
        scratch_shapes=[
            pltpu.VMEM((dim, width), jnp.bfloat16),
            pltpu.VMEM((parts, groups, dim, cols), jnp.bfloat16),
            pltpu.VMEM((groups, rows * 2 * side, dim), jnp.bfloat16),
            pltpu.VMEM((seq, dim), jnp.bfloat16),
            pltpu.VMEM((block, seq), jnp.float32),
            pltpu.VMEM((parts, rows * 2 * side, cols), jnp.float32),
            pltpu.VMEM((rows, width), jnp.float32),
            dma,
            dma((parts, side, 2)), dma((parts, side, 2)),
            dma((parts, 6)), dma((parts, 6)),
            dma((side,)), dma((side,)),
            dma((6,)), dma((6,)),
            dma((8,)), dma((8,)),
            dma((parts, side, 2)), dma((parts, side, 2)),
        ],
        compiler_params=pltpu.CompilerParams(collective_id=call_id, has_side_effects=True, vmem_limit_bytes=VMEM_LIMIT),
        name=f"attend_{call_id}",
    )(qkv, ids, row_ids, weight, residual, bias)


def solution(mesh):
    groups = mesh.shape["tp"]
    side = math.isqrt(groups // 2)
    assert 2 * side * side == groups and side == 4
    row_spec = P("dp", "tp", None)
    vec_spec = P()
    second = P(None, "tp")
    in_specs = (row_spec, P("dp", "tp"), vec_spec, vec_spec, P(None, None, None, "tp"), second, vec_spec, vec_spec, vec_spec, P(None, None, "tp"), second, second, vec_spec)

    def device_fn(tokens, doc_ids, norm1_gain, norm1_shift, qkv_weight, out_weight, out_bias, norm2_gain, norm2_shift, up_weight, up_bias, down_weight, down_bias):
        layers = norm1_gain.shape[0]
        id_cols = jnp.broadcast_to(doc_ids[0].astype(jnp.bfloat16)[:, None], (doc_ids.shape[1], 128))
        qkv_thirds = jnp.transpose(qkv_weight, (0, 2, 3, 1, 4))
        residual = tokens[0].astype(jnp.float32)
        for layer in range(layers):
            ids = [4 * layer + k for k in range(4)]
            tails = id_cols if layer == 0 else None
            qkv = gather_and_project(side, ids[0], layer, residual, norm1_gain, norm1_shift, qkv_thirds, norm1_gain, False, tails)
            if layer == 0:
                qkv, all_ids = qkv
                row_ids = all_ids[:, 0].astype(jnp.float32)[None]
            residual = attend_and_project(side, ids[1], layer, qkv, all_ids, row_ids, out_weight, residual, out_bias)
            hidden = gather_and_project(side, ids[2], layer, residual, norm2_gain, norm2_shift, up_weight, up_bias, True)
            residual = project_and_scatter(side, ids[3], layer, hidden, down_weight, residual, down_bias)
        return residual.astype(jnp.bfloat16)[None]

    return jax.shard_map(device_fn, mesh=mesh, in_specs=in_specs, out_specs=row_spec, check_vma=False)
```

```python
import functools
import math

import jax
import jax.numpy as jnp
from jax import lax
from jax.experimental import pallas as pl
from jax.experimental.pallas import tpu as pltpu
from jax.sharding import PartitionSpec as P

COLS = 512
MESH = pl.DeviceIdType.MESH
VMEM_LIMIT = 66 * 1000 * 1000

STEPS = (2, 1, -1, 0)
OTHER_SIDE = (2, -1, 1, 0)


class Place:
    def __init__(self, side):
        self.side = side
        self.me = lax.axis_index("tp")
        self.core = self.me % 2
        chip = self.me // 2
        self.x = chip % side
        self.y = chip // side
        self.partner = chip * 2 + 1 - self.core
        self.first = {1: self.dev(1, 0), -1: self.dev(-1, 0)}
        self.second = {1: self.dev(0, 1), -1: self.dev(0, -1)}

    def dev(self, i, j, core=None):
        core = self.core if core is None else core
        dx = i * (1 - core) + j * core
        dy = j * (1 - core) + i * core
        return (((self.y + dy + self.side) % self.side) * self.side + (self.x + dx + self.side) % self.side) * 2 + core

    def barrier(self):
        sem = pltpu.get_barrier_semaphore()
        others = [self.first[1], self.first[-1], self.second[1], self.second[-1], self.partner]
        for other in others:
            pl.semaphore_signal(sem, inc=1, device_id={"tp": other}, device_id_type=MESH)
        pl.semaphore_wait(sem, len(others))


def by_cols(width, fn):
    step = min(COLS, width)

    def body(n, carry):
        fn(pl.ds(pl.multiple_of(n * step, step), step))
        return carry

    lax.fori_loop(0, width // step, body, 0)


def scatter_kernel(side, layer, act_ref, w_hbm, res_ref, bias_ref, out_ref, w_ref, own, snd, prt, stg, mid, fin, stg2, mid2, fin2, w_sem, pair_send, pair_recv, send_sem, recv_sem):
    load_w = pltpu.make_async_copy(w_hbm.at[layer, 0] if len(w_hbm.shape) == 4 else w_hbm.at[layer], w_ref, w_sem)
    load_w.start()
    place = Place(side)
    rows, width = res_ref.shape
    half = rows // 2
    place.barrier()
    load_w.wait()

    def remote(src, dst, slot, device):
        return pltpu.make_async_remote_copy(src_ref=src, dst_ref=dst, send_sem=send_sem.at[slot], recv_sem=recv_sem.at[slot], device_id={"tp": device}, device_id_type=MESH)

    def pair_copy(g, jj):
        return pltpu.make_async_remote_copy(src_ref=snd.at[g % 2, jj], dst_ref=prt.at[g, jj], send_sem=pair_send.at[g, jj], recv_sem=pair_recv.at[g, jj], device_id={"tp": place.partner}, device_id_type=MESH)

    def product(core, g, dst):
        starts = [pl.multiple_of(place.dev(i, j, core) * rows + h * half, half) for j in STEPS for h, i in enumerate((STEPS[g], OTHER_SIDE[g]))]

        def piece(cols):
            lhs = jnp.concatenate([act_ref[pl.ds(s, half), :] for s in starts], axis=0)
            part = jnp.dot(lhs, w_ref[:, cols], preferred_element_type=jnp.float32).astype(jnp.bfloat16)
            for jj in range(side):
                dst[jj, :, cols] = part[jj * rows:(jj + 1) * rows]

        by_cols(width, piece)

    def pair_sum(g, jj, h, cols):
        at = pl.ds(h * half, half)
        return own[g, jj, at, cols].astype(jnp.float32) + prt[g, jj, at, cols].astype(jnp.float32)

    far, plus, minus, here = range(side)
    sent = []

    def send(src, dst, slot, device):
        copy = remote(src, dst, slot, device)
        copy.start()
        sent.append(copy)

    def arrived(dst, slot):
        remote(dst, dst, slot, place.me).wait_recv()

    def open_group(g):
        for jj in range(side):
            if g >= 2:
                pair_copy(g - 2, jj).wait_send()
        product(1 - place.core, g, snd.at[g % 2])
        for jj in range(side):
            pair_copy(g, jj).start()
        product(place.core, g, own.at[g])
        shared = set()
        for k, (jj, h) in enumerate(((far, 0), (far, 1), (plus, 1), (minus, 0))):
            if jj not in shared:
                shared.add(jj)
                pair_copy(g, jj).wait_recv()
            def stage(cols, k=k, jj=jj, h=h):
                stg[g, k, :, cols] = pair_sum(g, jj, h, cols)
            by_cols(width, stage)
            dst = mid.at[g, k] if k < 2 else fin.at[g, k]
            slot = 6 * g + (4 + k if k < 2 else k)
            send(stg.at[g, k], dst, slot, place.second[1 if k % 2 == 0 else -1])

    def relay(g):
        for k, (jj, h) in enumerate(((plus, 0), (minus, 1))):
            arrived(mid.at[g, k], 6 * g + 4 + k)
            def add(cols, k=k, jj=jj, h=h):
                mid[g, k, :, cols] += pair_sum(g, jj, h, cols)
            by_cols(width, add)
            send(mid.at[g, k], fin.at[g, k], 6 * g + k, place.second[1 if k == 0 else -1])

    base = 6 * side

    def close_group(g):
        pair_copy(g, here).wait_recv()
        for k in range(4):
            arrived(fin.at[g, k], 6 * g + k)

        def total(h, cols):
            return pair_sum(g, here, h, cols) + fin[g, 0 if h == 0 else 1, :, cols] + fin[g, 3 if h == 0 else 2, :, cols]

        def keep(k, h):
            def fn(cols):
                stg2[k, :, cols] = total(h, cols)
            by_cols(width, fn)

        def join(k):
            arrived(mid2.at[k], base + 4 + k)
            def fn(cols):
                mid2[k, :, cols] += total(k, cols)
            by_cols(width, fn)
            send(mid2.at[k], fin2.at[k], base + k, place.first[1 if k == 0 else -1])

        if g == far:
            keep(0, 0)
            send(stg2.at[0], mid2.at[0], base + 4, place.first[1])
            keep(1, 1)
            send(stg2.at[1], mid2.at[1], base + 5, place.first[-1])
        elif g == plus:
            join(0)
            join(1)
        elif g == minus:
            keep(2, 1)
            send(stg2.at[2], fin2.at[2], base + 2, place.first[1])
            keep(3, 0)
            send(stg2.at[3], fin2.at[3], base + 3, place.first[-1])
        else:
            for k in range(4):
                arrived(fin2.at[k], base + k)
            for h in range(2):
                def fn(cols, h=h):
                    at = pl.ds(h * half, half)
                    summed = total(h, cols) + fin2[0 if h == 0 else 1, :, cols] + fin2[3 if h == 0 else 2, :, cols]
                    out_ref[at, cols] = res_ref[at, cols] + (summed + bias_ref[layer:layer + 1, cols])
                by_cols(width, fn)

    open_group(0)
    open_group(1)
    open_group(2)
    relay(0)
    open_group(3)
    relay(1)
    close_group(0)
    relay(2)
    close_group(1)
    relay(3)
    close_group(2)
    close_group(3)
    for g in (side - 2, side - 1):
        for jj in range(side):
            pair_copy(g, jj).wait_send()
    for copy in sent:
        copy.wait_send()


def project_and_scatter(side, call_id, layer, act, weight, residual, bias):
    rows, width = residual.shape
    depth = act.shape[1]
    half = rows // 2
    quad = (side, side, rows, width)
    part = (side, 2, half, width)
    vmem = pl.BlockSpec(memory_space=pltpu.VMEM)
    return pl.pallas_call(
        functools.partial(scatter_kernel, side, layer),
        out_shape=jax.ShapeDtypeStruct((rows, width), jnp.float32),
        in_specs=[vmem, pl.BlockSpec(memory_space=pl.ANY), vmem, vmem],
        out_specs=vmem,
        scratch_shapes=[
            pltpu.VMEM((depth, width), jnp.bfloat16),
            pltpu.VMEM(quad, jnp.bfloat16),
            pltpu.VMEM((2,) + quad[1:], jnp.bfloat16),
            pltpu.VMEM(quad, jnp.bfloat16),
            pltpu.VMEM((side, 4, half, width), jnp.float32),
            pltpu.VMEM(part, jnp.float32),
            pltpu.VMEM((side, 4, half, width), jnp.float32),
            pltpu.VMEM((4, half, width), jnp.float32),
            pltpu.VMEM((2, half, width), jnp.float32),
            pltpu.VMEM((4, half, width), jnp.float32),
            pltpu.SemaphoreType.DMA,
            pltpu.SemaphoreType.DMA((side, side)),
            pltpu.SemaphoreType.DMA((side, side)),
            pltpu.SemaphoreType.DMA((6 * side + 6,)),
            pltpu.SemaphoreType.DMA((6 * side + 6,)),
        ],
        compiler_params=pltpu.CompilerParams(collective_id=call_id, has_side_effects=True, vmem_limit_bytes=VMEM_LIMIT),
        name=f"scatter_{call_id}",
    )(act, weight, residual, bias)


GATHER_ORDER = sorted(((i, j) for i in STEPS for j in STEPS), key=lambda at: (2 * abs(at[0]) + 3 * abs(at[1]), at))


def gather_kernel(side, layer, gelu, tail, res_ref, gain_ref, shift_ref, w_hbm, b_ref, *refs):
    tails, refs = (refs[0], refs[1:]) if tail else (None, refs)
    out, refs = refs[0], refs[1:]
    tails_out, refs = (refs[0], refs[1:]) if tail else (None, refs)
    (w_ref, buf, w_sem, send_sem, recv_sem, pair_send, pair_recv) = refs
    if len(w_hbm.shape) == 3:
        loads = [pltpu.make_async_copy(w_hbm.at[layer], w_ref, w_sem.at[0])]
    else:
        each = w_hbm.shape[4]
        loads = [pltpu.make_async_copy(w_hbm.at[layer, k, 0], w_ref.at[:, pl.ds(k * each, each)], w_sem.at[k]) for k in range(w_hbm.shape[1])]
    for load in loads:
        load.start()
    place = Place(side)
    rows, width = res_ref.shape
    half = rows // 2
    for at in (pl.ds(0, half), pl.ds(half, half)):
        residual = res_ref[at, :]
        centered = residual - jnp.mean(residual, axis=-1, keepdims=True)
        variance = jnp.mean(centered * centered, axis=-1, keepdims=True)
        normed = centered * lax.rsqrt(variance + 1e-5) * gain_ref[layer:layer + 1, :] + shift_ref[layer:layer + 1, :]
        buf[place.me, at, pl.ds(0, width)] = normed.astype(jnp.bfloat16)
    if tail:
        buf[place.me, :, pl.ds(width, tail)] = tails[...]
    place.barrier()

    def pick(n, values):
        value = values[0]
        for k, other in enumerate(values):
            value = jnp.where(n == k, other, value)
        return value

    def view(i, j, h, core=None):
        return buf.at[place.dev(i, j, core), pl.ds(pl.multiple_of(h * half, half), half)]

    def wrap(k):
        return (k + side + 1) % side - 1

    def slot(i, j, h):
        return ((i + side) % side * side + (j + side) % side) * 2 + h

    def ring_copies(i, j, h):
        own = (j == 0) & (i == 0)
        begins = (h == 0, h == 1)
        for axis, ahead in enumerate(((j == 0, i), (True, j))):
            whole = own if axis == 0 else j == 0
            for side_of, step in enumerate((1, -1)):
                there = (wrap(i - step), j) if axis == 0 else (i, wrap(j - step))
                device = (place.first, place.second)[axis][step]
                condition = whole | (ahead[0] & (ahead[1] == -step) & begins[side_of])
                yield condition, pltpu.make_async_remote_copy(src_ref=view(i, j, h), dst_ref=view(i, j, h), send_sem=send_sem.at[axis * 2 + side_of, slot(i, j, h)], recv_sem=recv_sem.at[slot(*there, h)], device_id={"tp": device}, device_id_type=MESH)

    def pair(i, j, h, core=None):
        index = slot(i, j, h)
        ref = view(i, j, h, core)
        return pltpu.make_async_remote_copy(src_ref=ref, dst_ref=ref, send_sem=pair_send.at[index], recv_sem=pair_recv.at[index], device_id={"tp": place.partner}, device_id_type=MESH)

    def arrived(i, j, h):
        ref = view(i, j, h)
        pltpu.make_async_remote_copy(src_ref=ref, dst_ref=ref, send_sem=send_sem.at[0, 0], recv_sem=recv_sem.at[slot(i, j, h)], device_id={"tp": place.me}, device_id_type=MESH).wait_recv()

    def multiply(i, j):
        devs = [place.dev(i, j), place.dev(i, j, 1 - place.core)]
        at = [pl.ds(pl.multiple_of(d * rows, rows), rows) for d in devs]
        if tail:
            for d, where in zip(devs, at):
                tails_out[where, :] = buf[d, :, pl.ds(width, tail)]
        lhs = jnp.concatenate([buf[d, :, pl.ds(0, width)] for d in devs], axis=0)
        part = jnp.dot(lhs, w_ref[...], preferred_element_type=jnp.float32)
        if gelu:
            part = jax.nn.gelu(part + b_ref[layer:layer + 1, :], approximate=True)
        part = part.astype(jnp.bfloat16)
        for k, where in enumerate(at):
            out[where, :] = part[k * rows:(k + 1) * rows]

    firsts = [at[0] for at in GATHER_ORDER]
    seconds = [at[1] for at in GATHER_ORDER]
    leads = [int(1 in at and -1 not in at) for at in GATHER_ORDER]

    def take(n, carry):
        i, j, lead = pick(n, firsts), pick(n, seconds), pick(n, leads)
        for k in range(2):
            h = (lead + k) % 2

            @pl.when(n > 0)
            def _():
                arrived(i, j, h)

            for condition, copy in ring_copies(i, j, h):
                pl.when(condition)(copy.start)
            pair(i, j, h).start()

        @pl.when(n == 0)
        def _():
            for load in loads:
                load.wait()

        for h in range(2):
            pair(i, j, h, 1 - place.core).wait_recv()
        multiply(i, j)
        return carry

    def drain(n, carry):
        i, j = pick(n, firsts), pick(n, seconds)
        for h in range(2):
            for condition, copy in ring_copies(i, j, h):
                pl.when(condition)(copy.wait_send)
            pair(i, j, h).wait_send()
        return carry

    lax.fori_loop(0, len(GATHER_ORDER), take, 0)
    lax.fori_loop(0, len(GATHER_ORDER), drain, 0)


def gather_and_project(side, call_id, layer, residual, gain, shift, weight, bias, gelu, tails=None):
    rows, width = residual.shape
    tail = 0 if tails is None else tails.shape[1]
    extra = [] if tails is None else [tails]
    groups = 2 * side * side
    wide = weight.shape[2] if weight.ndim == 3 else weight.shape[1] * weight.shape[4]
    vmem = pl.BlockSpec(memory_space=pltpu.VMEM)
    outs = pl.pallas_call(
        functools.partial(gather_kernel, side, layer, gelu, tail),
        out_shape=[jax.ShapeDtypeStruct((groups * rows, wide), jnp.bfloat16)] + [jax.ShapeDtypeStruct((groups * rows, tail), jnp.bfloat16) for _ in extra],
        in_specs=[vmem, vmem, vmem, pl.BlockSpec(memory_space=pl.ANY), vmem] + [vmem for _ in extra],
        out_specs=[vmem] * (1 + len(extra)),
        scratch_shapes=[
            pltpu.VMEM((width, wide), jnp.bfloat16),
            pltpu.VMEM((groups, rows, width + tail), jnp.bfloat16),
            pltpu.SemaphoreType.DMA((3,)),
            pltpu.SemaphoreType.DMA((4, groups)),
            pltpu.SemaphoreType.DMA((groups,)),
            pltpu.SemaphoreType.DMA((groups,)),
            pltpu.SemaphoreType.DMA((groups,)),
        ],
        compiler_params=pltpu.CompilerParams(collective_id=call_id, has_side_effects=True, vmem_limit_bytes=VMEM_LIMIT),
        name=f"gather_{call_id}",
    )(residual, gain, shift, weight, bias, *extra)
    return outs if len(outs) > 1 else outs[0]


QUERY_BLOCK = 256
RING = ((-1, 0), (1, 1), (-1, 1), (1, 0), (2, 0), (2, 1))


def attend_kernel(side, layer, qkv_ref, ids_ref, row_ids_ref, w_hbm, res_ref, bias_ref, out_ref, w_own, wbuf, obuf, o_own, scores, acc, rbuf, load_sem, ws_send, ws_recv, wg_send, wg_recv, os_send, os_recv, og_send, og_recv, op_send, op_recv, back_send, back_recv):
    load_w = pltpu.make_async_copy(w_hbm.at[layer, 0], w_own, load_sem)
    load_w.start()
    me = lax.axis_index("tp")
    core = me % 2
    x = me // 2 % side
    y = me // 2 // side
    rows, width = res_ref.shape
    dim = w_own.shape[0]
    share = width // (2 * side)
    parts, _, _, cols = wbuf.shape
    line = rows * 2 * side
    steps = STEPS

    def at(dx, dy, dc):
        return (((y + dy + side) % side) * side + (x + dx + side) % side) * 2 + (core + dc) % 2

    peers = [at(dx, 0, dc) for dx in steps for dc in (1, 0) if (dx, dc) != (0, 0)]
    columns = [at(0, dy, 0) for dy in steps[:3]]
    barrier = pltpu.get_barrier_semaphore()
    for peer in peers + columns:
        pl.semaphore_signal(barrier, inc=1, device_id={"tp": peer}, device_id_type=MESH)
    pl.semaphore_wait(barrier, len(peers) + len(columns))
    load_w.wait()

    sent = []

    def send(src, dst, send_sem, recv_sem, device):
        if device is None:
            copy = pltpu.make_async_copy(src, dst, recv_sem)
        else:
            copy = pltpu.make_async_remote_copy(src_ref=src, dst_ref=dst, send_sem=send_sem, recv_sem=recv_sem, device_id={"tp": device}, device_id_type=MESH)
            sent.append(copy)
        copy.start()

    def arrived(dst, recv_sem):
        pltpu.make_async_copy(dst, dst, recv_sem).wait()

    def target(dx, dy, dc):
        return None if (dx, dy, dc) == (0, 0, 0) else at(dx, dy, dc)

    def first_col(device, part):
        return pl.multiple_of(device % (2 * side) * share + part * cols, 128)

    for part in range(parts):
        for k, dx in enumerate(steps):
            for dc in range(2):
                src = w_own.at[:, pl.ds(first_col(at(dx, 0, dc), part), cols)]
                send(src, wbuf.at[part, me], ws_send.at[part, k, dc], ws_recv.at[part, k, dc], target(dx, 0, dc))

    def w_slots(part, j, h):
        return wbuf.at[part, pl.ds(((y + j + side) % side) * 2 * side + h * side, side)]

    def w_ring(part, j, h):
        index = RING.index((j, h))
        return wg_send.at[part, index], wg_recv.at[part, index]

    def w_first(part):
        for k, dx in enumerate(steps):
            for dc in range(2):
                arrived(wbuf.at[part, at(-dx, 0, dc)], ws_recv.at[part, k, dc])
        for h in range(2):
            send(w_slots(part, 0, h), w_slots(part, 0, h), *w_ring(part, -1, h), at(0, 1, 0))
            send(w_slots(part, 0, 1 - h), w_slots(part, 0, 1 - h), *w_ring(part, 1, 1 - h), at(0, -1, 0))

    def w_arrived(part, j, h):
        arrived(w_slots(part, j, h), w_ring(part, j, h)[1])

    def w_relay(part):
        w_arrived(part, -1, 0)
        send(w_slots(part, -1, 0), w_slots(part, -1, 0), *w_ring(part, 2, 0), at(0, 1, 0))
        w_arrived(part, 1, 1)
        send(w_slots(part, 1, 1), w_slots(part, 1, 1), *w_ring(part, 2, 1), at(0, -1, 0))

    block = scores.shape[0]
    half = block // 2

    def attend(b):
        q_rows = pl.ds(pl.multiple_of(b * block, block), block)
        q = qkv_ref[q_rows, pl.ds(0, dim)]
        q_ids = ids_ref[q_rows, 0:1].astype(jnp.float32)
        q_pos = b * block + lax.broadcasted_iota(jnp.int32, (block, block), 0)

        def chunk(c):
            return pl.ds(pl.multiple_of(c * block, block), block)

        def score(c, top):
            s = lax.dot_general(q, qkv_ref[chunk(c), pl.ds(dim, dim)], (((1,), (1,)), ((), ())), preferred_element_type=jnp.float32) * dim ** -0.5
            k_pos = c * block + lax.broadcasted_iota(jnp.int32, (block, block), 1)
            allowed = (k_pos <= q_pos) & (row_ids_ref[0:1, chunk(c)] == q_ids)
            s = jnp.where(allowed, s, -1e30)
            scores[:, chunk(c)] = s
            return jnp.maximum(top, jnp.maximum(s[:, :half], s[:, half:]))

        top = jnp.max(lax.fori_loop(0, b + 1, score, jnp.full((block, half), -1e30, jnp.float32)), axis=-1, keepdims=True)

        def power(c, total):
            e = jnp.exp(scores[:, chunk(c)] - top)
            scores[:, chunk(c)] = e
            return total + (e[:, :half] + e[:, half:])

        total = jnp.sum(lax.fori_loop(0, b + 1, power, jnp.zeros((block, half), jnp.float32)), axis=-1, keepdims=True)
        inverse = 1.0 / total

        def mix(c, mixed):
            probs = (scores[:, chunk(c)] * inverse).astype(jnp.bfloat16)
            return mixed + jnp.dot(probs, qkv_ref[chunk(c), pl.ds(2 * dim, dim)], preferred_element_type=jnp.float32)

        o_own[q_rows, :] = lax.fori_loop(0, b + 1, mix, jnp.zeros((block, dim), jnp.float32)).astype(jnp.bfloat16)

    def o_slot(c, xx, yy):
        return (c * side + xx) * side + yy

    def attend_line(k):
        n = (y + steps[k] + side) % side

        def body(b, carry):
            attend(n * (line // block) + b)
            return carry

        lax.fori_loop(0, line // block, body, 0)
        src = o_own.at[pl.ds(pl.multiple_of(n * line, line), line)]
        send(src, obuf.at[o_slot(core, x, y)], os_send.at[k], os_recv.at[k], target(0, steps[k], 0))

    def o_slots(i, h, dc=0):
        return obuf.at[pl.ds(o_slot((core + dc) % 2, (x + i + side) % side, h * (side // 2)), side // 2)]

    def o_send(i, h, step, index):
        send(o_slots(i, h), o_slots(i, h), og_send.at[index], og_recv.at[index], at(step, 0, 0))

    def o_share(k, i, h):
        send(o_slots(i, h), o_slots(i, h), op_send.at[k], op_recv.at[k], at(0, 0, 1))

    attend_line(0)
    attend_line(1)
    w_first(0)
    attend_line(2)
    w_first(1)
    attend_line(3)
    w_relay(0)
    for k, dy in enumerate(steps):
        arrived(obuf.at[o_slot(core, x, (y - dy + side) % side)], os_recv.at[k])
    for h in range(2):
        o_send(0, h, 1, RING.index((-1, h)))
        o_send(0, 1 - h, -1, RING.index((1, 1 - h)))
    w_first(2)
    for h in range(2):
        o_share(h, 0, h)
    w_relay(1)
    w_first(3)
    for k, (i, h) in enumerate(RING):
        arrived(o_slots(i, h), og_recv.at[k])
        if (i, h) == (-1, 0):
            o_send(i, h, 1, RING.index((2, 0)))
        if (i, h) == (1, 1):
            o_send(i, h, -1, RING.index((2, 1)))
        o_share(2 + k, i, h)
        if k == 3:
            w_relay(2)
    for k, (i, h) in enumerate(((0, 0), (0, 1)) + RING):
        arrived(o_slots(i, h, 1), op_recv.at[k])

    strip = min(block, line)

    def heads_of(part, at_rows, j, total):
        yy = (y + j + side) % side
        for xx in range(side):
            for c in range(2):
                head = jnp.dot(obuf[o_slot(c, xx, yy), at_rows, :], wbuf[part, (yy * side + xx) * 2 + c], preferred_element_type=jnp.float32)
                total = total + head.astype(jnp.bfloat16).astype(jnp.float32)
        return total

    def project(part, last):
        def body(n, carry):
            at_rows = pl.ds(pl.multiple_of(n * strip, strip), strip)
            if last:
                total = heads_of(part, at_rows, 2, acc[part, at_rows, :])
            else:
                total = lax.fori_loop(0, 3, lambda k, t: heads_of(part, at_rows, (k + 1) % 3 - 1, t), jnp.zeros((strip, cols), jnp.float32))
            acc[part, at_rows, :] = total
            return carry

        lax.fori_loop(0, line // strip, body, 0)

    def back_rows(device):
        return pl.ds(pl.multiple_of(device % (2 * side) * rows, rows), rows)

    for part in range(parts):
        w_arrived(part, -1, 1)
        w_arrived(part, 1, 0)
        project(part, False)
        for h in range(2):
            w_arrived(part, 2, h)
        project(part, True)
        for k, dx in enumerate(steps):
            for dc in range(2):
                src = acc.at[part, back_rows(at(dx, 0, dc))]
                dst = rbuf.at[:, pl.ds(first_col(me, part), cols)]
                send(src, dst, back_send.at[part, k, dc], back_recv.at[part, k, dc], target(dx, 0, dc))
        if part == 0:
            w_relay(3)
    for part in range(parts):
        for k, dx in enumerate(steps):
            for dc in range(2):
                arrived(rbuf.at[:, pl.ds(first_col(at(-dx, 0, dc), part), cols)], back_recv.at[part, k, dc])

    def finish(at_cols):
        out_ref[:, at_cols] = res_ref[:, at_cols] + (rbuf[:, at_cols] + bias_ref[layer:layer + 1, at_cols])

    by_cols(width, finish)
    for copy in sent:
        copy.wait_send()


def attend_and_project(side, call_id, layer, qkv, ids, row_ids, weight, residual, bias):
    rows, width = residual.shape
    seq, dim = qkv.shape[0], weight.shape[2]
    groups = 2 * side * side
    parts = 4
    cols = width // (2 * side) // parts
    block = min(QUERY_BLOCK, rows * 2 * side)
    vmem = pl.BlockSpec(memory_space=pltpu.VMEM)
    dma = pltpu.SemaphoreType.DMA
    return pl.pallas_call(
        functools.partial(attend_kernel, side, layer),
        out_shape=jax.ShapeDtypeStruct((rows, width), jnp.float32),
        in_specs=[vmem, vmem, vmem, pl.BlockSpec(memory_space=pl.ANY), vmem, vmem],
        out_specs=vmem,
        scratch_shapes=[
            pltpu.VMEM((dim, width), jnp.bfloat16),
            pltpu.VMEM((parts, groups, dim, cols), jnp.bfloat16),
            pltpu.VMEM((groups, rows * 2 * side, dim), jnp.bfloat16),
            pltpu.VMEM((seq, dim), jnp.bfloat16),
            pltpu.VMEM((block, seq), jnp.float32),
            pltpu.VMEM((parts, rows * 2 * side, cols), jnp.float32),
            pltpu.VMEM((rows, width), jnp.float32),
            dma,
            dma((parts, side, 2)), dma((parts, side, 2)),
            dma((parts, 6)), dma((parts, 6)),
            dma((side,)), dma((side,)),
            dma((6,)), dma((6,)),
            dma((8,)), dma((8,)),
            dma((parts, side, 2)), dma((parts, side, 2)),
        ],
        compiler_params=pltpu.CompilerParams(collective_id=call_id, has_side_effects=True, vmem_limit_bytes=VMEM_LIMIT),
        name=f"attend_{call_id}",
    )(qkv, ids, row_ids, weight, residual, bias)


def solution(mesh):
    groups = mesh.shape["tp"]
    side = math.isqrt(groups // 2)
    assert 2 * side * side == groups and side == 4
    row_spec = P("dp", "tp", None)
    vec_spec = P()
    second = P(None, "tp")
    in_specs = (row_spec, P("dp", "tp"), vec_spec, vec_spec, P(None, None, None, "tp"), second, vec_spec, vec_spec, vec_spec, P(None, None, "tp"), second, second, vec_spec)

    def device_fn(tokens, doc_ids, norm1_gain, norm1_shift, qkv_weight, out_weight, out_bias, norm2_gain, norm2_shift, up_weight, up_bias, down_weight, down_bias):
        layers = norm1_gain.shape[0]
        id_cols = jnp.broadcast_to(doc_ids[0].astype(jnp.bfloat16)[:, None], (doc_ids.shape[1], 128))
        qkv_thirds = jnp.transpose(qkv_weight, (0, 2, 3, 1, 4))
        residual = tokens[0].astype(jnp.float32)
        for layer in range(layers):
            ids = [4 * layer + k for k in range(4)]
            tails = id_cols if layer == 0 else None
            qkv = gather_and_project(side, ids[0], layer, residual, norm1_gain, norm1_shift, qkv_thirds, norm1_gain, False, tails)
            if layer == 0:
                qkv, all_ids = qkv
                row_ids = all_ids[:, 0].astype(jnp.float32)[None]
            residual = attend_and_project(side, ids[1], layer, qkv, all_ids, row_ids, out_weight, residual, out_bias)
            hidden = gather_and_project(side, ids[2], layer, residual, norm2_gain, norm2_shift, up_weight, up_bias, True)
            residual = project_and_scatter(side, ids[3], layer, hidden, down_weight, residual, down_bias)
        return residual.astype(jnp.bfloat16)[None]

    return jax.shard_map(device_fn, mesh=mesh, in_specs=in_specs, out_specs=row_spec, check_vma=False)
```

```python
import functools
import math

import jax
import jax.numpy as jnp
from jax import lax
from jax.experimental import pallas as pl
from jax.experimental.pallas import tpu as pltpu
from jax.sharding import PartitionSpec as P

COLS = 512
MESH = pl.DeviceIdType.MESH
VMEM_LIMIT = 66 * 1000 * 1000

STEPS = (2, 1, -1, 0)
OTHER_SIDE = (2, -1, 1, 0)


class Place:
    def __init__(self, side):
        self.side = side
        self.me = lax.axis_index("tp")
        self.core = self.me % 2
        chip = self.me // 2
        self.x = chip % side
        self.y = chip // side
        self.partner = chip * 2 + 1 - self.core
        self.first = {1: self.dev(1, 0), -1: self.dev(-1, 0)}
        self.second = {1: self.dev(0, 1), -1: self.dev(0, -1)}

    def dev(self, i, j, core=None):
        core = self.core if core is None else core
        dx = i * (1 - core) + j * core
        dy = j * (1 - core) + i * core
        return (((self.y + dy + self.side) % self.side) * self.side + (self.x + dx + self.side) % self.side) * 2 + core

    def neighbours(self):
        return [self.first[1], self.first[-1], self.second[1], self.second[-1], self.partner]


def announce(others):
    for other in others:
        pl.semaphore_signal(pltpu.get_barrier_semaphore(), inc=1, device_id={"tp": other}, device_id_type=MESH)


def meet(others):
    pl.semaphore_wait(pltpu.get_barrier_semaphore(), len(others))


def by_cols(width, fn):
    step = min(COLS, width)

    def body(n, carry):
        fn(pl.ds(pl.multiple_of(n * step, step), step))
        return carry

    lax.fori_loop(0, width // step, body, 0)


def scatter_kernel(side, layer, act_ref, w_hbm, res_ref, bias_ref, out_ref, w_ref, own, snd, prt, stg, mid, fin, stg2, mid2, fin2, w_sem, pair_send, pair_recv, send_sem, recv_sem):
    load_w = pltpu.make_async_copy(w_hbm.at[layer, 0] if len(w_hbm.shape) == 4 else w_hbm.at[layer], w_ref, w_sem)
    load_w.start()
    place = Place(side)
    rows, width = res_ref.shape
    half = rows // 2
    announce(place.neighbours())
    load_w.wait()

    def remote(src, dst, slot, device):
        return pltpu.make_async_remote_copy(src_ref=src, dst_ref=dst, send_sem=send_sem.at[slot], recv_sem=recv_sem.at[slot], device_id={"tp": device}, device_id_type=MESH)

    def pair_copy(g, jj):
        return pltpu.make_async_remote_copy(src_ref=snd.at[g % 2, jj], dst_ref=prt.at[g, jj], send_sem=pair_send.at[g, jj], recv_sem=pair_recv.at[g, jj], device_id={"tp": place.partner}, device_id_type=MESH)

    def product(core, g, dst):
        starts = [pl.multiple_of(place.dev(i, j, core) * rows + h * half, half) for j in STEPS for h, i in enumerate((STEPS[g], OTHER_SIDE[g]))]

        def piece(cols):
            lhs = jnp.concatenate([act_ref[pl.ds(s, half), :] for s in starts], axis=0)
            part = jnp.dot(lhs, w_ref[:, cols], preferred_element_type=jnp.float32).astype(jnp.bfloat16)
            for jj in range(side):
                dst[jj, :, cols] = part[jj * rows:(jj + 1) * rows]

        by_cols(width, piece)

    def pair_sum(g, jj, h, cols):
        at = pl.ds(h * half, half)
        return own[g, jj, at, cols].astype(jnp.float32) + prt[g, jj, at, cols].astype(jnp.float32)

    far, plus, minus, here = range(side)
    sent = []

    def send(src, dst, slot, device):
        copy = remote(src, dst, slot, device)
        copy.start()
        sent.append(copy)

    def arrived(dst, slot):
        remote(dst, dst, slot, place.me).wait_recv()

    def open_group(g):
        for jj in range(side):
            if g >= 2:
                pair_copy(g - 2, jj).wait_send()
        product(1 - place.core, g, snd.at[g % 2])
        if g == 0:
            meet(place.neighbours())
        for jj in range(side):
            pair_copy(g, jj).start()
        product(place.core, g, own.at[g])
        shared = set()
        for k, (jj, h) in enumerate(((far, 0), (far, 1), (plus, 1), (minus, 0))):
            if jj not in shared:
                shared.add(jj)
                pair_copy(g, jj).wait_recv()
            def stage(cols, k=k, jj=jj, h=h):
                stg[g, k, :, cols] = pair_sum(g, jj, h, cols)
            by_cols(width, stage)
            dst = mid.at[g, k] if k < 2 else fin.at[g, k]
            slot = 6 * g + (4 + k if k < 2 else k)
            send(stg.at[g, k], dst, slot, place.second[1 if k % 2 == 0 else -1])

    def relay(g):
        for k, (jj, h) in enumerate(((plus, 0), (minus, 1))):
            arrived(mid.at[g, k], 6 * g + 4 + k)
            def add(cols, k=k, jj=jj, h=h):
                mid[g, k, :, cols] += pair_sum(g, jj, h, cols)
            by_cols(width, add)
            send(mid.at[g, k], fin.at[g, k], 6 * g + k, place.second[1 if k == 0 else -1])

    base = 6 * side

    def close_group(g):
        pair_copy(g, here).wait_recv()
        for k in range(4):
            arrived(fin.at[g, k], 6 * g + k)

        def total(h, cols):
            return pair_sum(g, here, h, cols) + fin[g, 0 if h == 0 else 1, :, cols] + fin[g, 3 if h == 0 else 2, :, cols]

        def keep(k, h):
            def fn(cols):
                stg2[k, :, cols] = total(h, cols)
            by_cols(width, fn)

        def join(k):
            arrived(mid2.at[k], base + 4 + k)
            def fn(cols):
                mid2[k, :, cols] += total(k, cols)
            by_cols(width, fn)
            send(mid2.at[k], fin2.at[k], base + k, place.first[1 if k == 0 else -1])

        if g == far:
            keep(0, 0)
            send(stg2.at[0], mid2.at[0], base + 4, place.first[1])
            keep(1, 1)
            send(stg2.at[1], mid2.at[1], base + 5, place.first[-1])
        elif g == plus:
            join(0)
            join(1)
        elif g == minus:
            keep(2, 1)
            send(stg2.at[2], fin2.at[2], base + 2, place.first[1])
            keep(3, 0)
            send(stg2.at[3], fin2.at[3], base + 3, place.first[-1])
        else:
            for k in range(4):
                arrived(fin2.at[k], base + k)
            for h in range(2):
                def fn(cols, h=h):
                    at = pl.ds(h * half, half)
                    summed = total(h, cols) + fin2[0 if h == 0 else 1, :, cols] + fin2[3 if h == 0 else 2, :, cols]
                    out_ref[at, cols] = res_ref[at, cols] + (summed + bias_ref[layer:layer + 1, cols])
                by_cols(width, fn)

    open_group(0)
    open_group(1)
    open_group(2)
    relay(0)
    open_group(3)
    relay(1)
    close_group(0)
    relay(2)
    close_group(1)
    relay(3)
    close_group(2)
    close_group(3)
    for g in (side - 2, side - 1):
        for jj in range(side):
            pair_copy(g, jj).wait_send()
    for copy in sent:
        copy.wait_send()


def project_and_scatter(side, call_id, layer, act, weight, residual, bias):
    rows, width = residual.shape
    depth = act.shape[1]
    half = rows // 2
    quad = (side, side, rows, width)
    part = (side, 2, half, width)
    vmem = pl.BlockSpec(memory_space=pltpu.VMEM)
    return pl.pallas_call(
        functools.partial(scatter_kernel, side, layer),
        out_shape=jax.ShapeDtypeStruct((rows, width), jnp.float32),
        in_specs=[vmem, pl.BlockSpec(memory_space=pl.ANY), vmem, vmem],
        out_specs=vmem,
        scratch_shapes=[
            pltpu.VMEM((depth, width), jnp.bfloat16),
            pltpu.VMEM(quad, jnp.bfloat16),
            pltpu.VMEM((2,) + quad[1:], jnp.bfloat16),
            pltpu.VMEM(quad, jnp.bfloat16),
            pltpu.VMEM((side, 4, half, width), jnp.float32),
            pltpu.VMEM(part, jnp.float32),
            pltpu.VMEM((side, 4, half, width), jnp.float32),
            pltpu.VMEM((4, half, width), jnp.float32),
            pltpu.VMEM((2, half, width), jnp.float32),
            pltpu.VMEM((4, half, width), jnp.float32),
            pltpu.SemaphoreType.DMA,
            pltpu.SemaphoreType.DMA((side, side)),
            pltpu.SemaphoreType.DMA((side, side)),
            pltpu.SemaphoreType.DMA((6 * side + 6,)),
            pltpu.SemaphoreType.DMA((6 * side + 6,)),
        ],
        compiler_params=pltpu.CompilerParams(collective_id=call_id, has_side_effects=True, vmem_limit_bytes=VMEM_LIMIT),
        name=f"scatter_{call_id}",
    )(act, weight, residual, bias)


GATHER_ORDER = sorted(((i, j) for i in STEPS for j in STEPS), key=lambda at: (2 * abs(at[0]) + 3 * abs(at[1]), at))


def gather_body(place, layer, gelu, res_ref, gain_ref, shift_ref, w_ref, loads, b_ref, out, buf, sems, tails=None, tails_out=None, ready=None, hook=None):
    send_sem, recv_sem, pair_send, pair_recv = sems
    side = place.side
    rows, width = res_ref.shape
    tail = 0 if tails is None else tails.shape[1]
    half = rows // 2
    for at in (pl.ds(0, half), pl.ds(half, half)):
        residual = res_ref[at, :].astype(jnp.float32)
        centered = residual - jnp.mean(residual, axis=-1, keepdims=True)
        variance = jnp.mean(centered * centered, axis=-1, keepdims=True)
        normed = centered * lax.rsqrt(variance + 1e-5) * gain_ref[layer:layer + 1, :] + shift_ref[layer:layer + 1, :]
        buf[place.me, at, pl.ds(0, width)] = normed.astype(jnp.bfloat16)
    if tail:
        buf[place.me, :, pl.ds(width, tail)] = tails[...]
    if ready is not None:
        ready()

    def pick(n, values):
        value = values[0]
        for k, other in enumerate(values):
            value = jnp.where(n == k, other, value)
        return value

    def view(i, j, h, core=None):
        return buf.at[place.dev(i, j, core), pl.ds(pl.multiple_of(h * half, half), half)]

    def wrap(k):
        return (k + side + 1) % side - 1

    def slot(i, j, h):
        return ((i + side) % side * side + (j + side) % side) * 2 + h

    def ring_copies(i, j, h):
        own = (j == 0) & (i == 0)
        begins = (h == 0, h == 1)
        for axis, ahead in enumerate(((j == 0, i), (True, j))):
            whole = own if axis == 0 else j == 0
            for side_of, step in enumerate((1, -1)):
                there = (wrap(i - step), j) if axis == 0 else (i, wrap(j - step))
                device = (place.first, place.second)[axis][step]
                condition = whole | (ahead[0] & (ahead[1] == -step) & begins[side_of])
                yield condition, pltpu.make_async_remote_copy(src_ref=view(i, j, h), dst_ref=view(i, j, h), send_sem=send_sem.at[axis * 2 + side_of, slot(i, j, h)], recv_sem=recv_sem.at[slot(*there, h)], device_id={"tp": device}, device_id_type=MESH)

    def pair(i, j, h, core=None):
        index = slot(i, j, h)
        ref = view(i, j, h, core)
        return pltpu.make_async_remote_copy(src_ref=ref, dst_ref=ref, send_sem=pair_send.at[index], recv_sem=pair_recv.at[index], device_id={"tp": place.partner}, device_id_type=MESH)

    def arrived(i, j, h):
        ref = view(i, j, h)
        pltpu.make_async_remote_copy(src_ref=ref, dst_ref=ref, send_sem=send_sem.at[0, 0], recv_sem=recv_sem.at[slot(i, j, h)], device_id={"tp": place.me}, device_id_type=MESH).wait_recv()

    def multiply(i, j):
        devs = [place.dev(i, j), place.dev(i, j, 1 - place.core)]
        at = [pl.ds(pl.multiple_of(d * rows, rows), rows) for d in devs]
        if tail:
            for d, where in zip(devs, at):
                tails_out[where, :] = buf[d, :, pl.ds(width, tail)]
        lhs = jnp.concatenate([buf[d, :, pl.ds(0, width)] for d in devs], axis=0)
        part = jnp.dot(lhs, w_ref[...], preferred_element_type=jnp.float32)
        if gelu:
            part = jax.nn.gelu(part + b_ref[layer:layer + 1, :], approximate=True)
        part = part.astype(jnp.bfloat16)
        for k, where in enumerate(at):
            out[where, :] = part[k * rows:(k + 1) * rows]

    firsts = [at[0] for at in GATHER_ORDER]
    seconds = [at[1] for at in GATHER_ORDER]
    leads = [int(1 in at and -1 not in at) for at in GATHER_ORDER]

    def take(n, carry):
        i, j, lead = pick(n, firsts), pick(n, seconds), pick(n, leads)
        for k in range(2):
            h = (lead + k) % 2

            @pl.when(n > 0)
            def _():
                arrived(i, j, h)

            for condition, copy in ring_copies(i, j, h):
                pl.when(condition)(copy.start)
            pair(i, j, h).start()

        @pl.when(n == 0)
        def _():
            for load in loads:
                load.wait()

        for h in range(2):
            pair(i, j, h, 1 - place.core).wait_recv()
        multiply(i, j)
        return carry

    def drain(n, carry):
        i, j = pick(n, firsts), pick(n, seconds)
        for h in range(2):
            for condition, copy in ring_copies(i, j, h):
                pl.when(condition)(copy.wait_send)
            pair(i, j, h).wait_send()
        return carry

    last = max(n for n, at in enumerate(GATHER_ORDER) if at[1] != 2) + 1
    lax.fori_loop(0, last, take, 0)
    if hook is not None:
        hook()
    lax.fori_loop(last, len(GATHER_ORDER), take, 0)
    return lambda: lax.fori_loop(0, len(GATHER_ORDER), drain, 0)


QUERY_BLOCK = 256
RING = ((-1, 0), (1, 1), (-1, 1), (1, 0), (2, 0), (2, 1))


def attend_body(place, layer, qkv_ref, ids_ref, row_ids_ref, load_w, res_ref, bias_ref, out_ref, bufs, sems):
    w_own, wbuf, obuf, o_own, scores, acc, rbuf = bufs
    ws_send, ws_recv, wg_send, wg_recv, os_send, os_recv, og_send, og_recv, op_send, op_recv, back_send, back_recv = sems
    side, me, core, x, y = place.side, place.me, place.core, place.x, place.y
    rows, width = res_ref.shape
    dim = w_own.shape[0]
    share = width // (2 * side)
    parts, _, _, cols = wbuf.shape
    line = rows * 2 * side
    steps = STEPS

    def at(dx, dy, dc):
        return (((y + dy + side) % side) * side + (x + dx + side) % side) * 2 + (core + dc) % 2

    peers = [at(dx, 0, dc) for dx in steps for dc in (1, 0) if (dx, dc) != (0, 0)]
    columns = [at(0, dy, 0) for dy in steps[:3]]
    sent = []

    def send(src, dst, send_sem, recv_sem, device):
        if device is None:
            copy = pltpu.make_async_copy(src, dst, recv_sem)
        else:
            copy = pltpu.make_async_remote_copy(src_ref=src, dst_ref=dst, send_sem=send_sem, recv_sem=recv_sem, device_id={"tp": device}, device_id_type=MESH)
            sent.append(copy)
        copy.start()

    def arrived(dst, recv_sem):
        pltpu.make_async_copy(dst, dst, recv_sem).wait()

    def target(dx, dy, dc):
        return None if (dx, dy, dc) == (0, 0, 0) else at(dx, dy, dc)

    def first_col(device, part):
        return pl.multiple_of(device % (2 * side) * share + part * cols, 128)

    def begin():
        load_w.wait()
        for part in range(parts):
            for k, dx in enumerate(steps):
                for dc in range(2):
                    src = w_own.at[:, pl.ds(first_col(at(dx, 0, dc), part), cols)]
                    send(src, wbuf.at[part, me], ws_send.at[part, k, dc], ws_recv.at[part, k, dc], target(dx, 0, dc))

    def w_slots(part, j, h):
        return wbuf.at[part, pl.ds(((y + j + side) % side) * 2 * side + h * side, side)]

    def w_ring(part, j, h):
        index = RING.index((j, h))
        return wg_send.at[part, index], wg_recv.at[part, index]

    def w_first(part):
        for k, dx in enumerate(steps):
            for dc in range(2):
                arrived(wbuf.at[part, at(-dx, 0, dc)], ws_recv.at[part, k, dc])
        for h in range(2):
            send(w_slots(part, 0, h), w_slots(part, 0, h), *w_ring(part, -1, h), at(0, 1, 0))
            send(w_slots(part, 0, 1 - h), w_slots(part, 0, 1 - h), *w_ring(part, 1, 1 - h), at(0, -1, 0))

    def w_arrived(part, j, h):
        arrived(w_slots(part, j, h), w_ring(part, j, h)[1])

    def w_relay(part):
        w_arrived(part, -1, 0)
        send(w_slots(part, -1, 0), w_slots(part, -1, 0), *w_ring(part, 2, 0), at(0, 1, 0))
        w_arrived(part, 1, 1)
        send(w_slots(part, 1, 1), w_slots(part, 1, 1), *w_ring(part, 2, 1), at(0, -1, 0))

    block = scores.shape[0]
    half = block // 2

    def attend(b):
        q_rows = pl.ds(pl.multiple_of(b * block, block), block)
        q = qkv_ref[q_rows, pl.ds(0, dim)]
        q_ids = ids_ref[q_rows, 0:1].astype(jnp.float32)
        q_pos = b * block + lax.broadcasted_iota(jnp.int32, (block, block), 0)

        def chunk(c):
            return pl.ds(pl.multiple_of(c * block, block), block)

        def score(c, top):
            s = lax.dot_general(q, qkv_ref[chunk(c), pl.ds(dim, dim)], (((1,), (1,)), ((), ())), preferred_element_type=jnp.float32) * dim ** -0.5
            k_pos = c * block + lax.broadcasted_iota(jnp.int32, (block, block), 1)
            allowed = (k_pos <= q_pos) & (row_ids_ref[0:1, chunk(c)] == q_ids)
            s = jnp.where(allowed, s, -1e30)
            scores[:, chunk(c)] = s
            return jnp.maximum(top, jnp.maximum(s[:, :half], s[:, half:]))

        top = jnp.max(lax.fori_loop(0, b + 1, score, jnp.full((block, half), -1e30, jnp.float32)), axis=-1, keepdims=True)

        def power(c, total):
            e = jnp.exp(scores[:, chunk(c)] - top)
            scores[:, chunk(c)] = e
            return total + (e[:, :half] + e[:, half:])

        total = jnp.sum(lax.fori_loop(0, b + 1, power, jnp.zeros((block, half), jnp.float32)), axis=-1, keepdims=True)
        inverse = 1.0 / total

        def mix(c, mixed):
            probs = (scores[:, chunk(c)] * inverse).astype(jnp.bfloat16)
            return mixed + jnp.dot(probs, qkv_ref[chunk(c), pl.ds(2 * dim, dim)], preferred_element_type=jnp.float32)

        o_own[q_rows, :] = lax.fori_loop(0, b + 1, mix, jnp.zeros((block, dim), jnp.float32)).astype(jnp.bfloat16)

    def o_slot(c, xx, yy):
        return (c * side + xx) * side + yy

    def attend_line(k):
        n = (y + steps[k] + side) % side

        def body(b, carry):
            attend(n * (line // block) + b)
            return carry

        lax.fori_loop(0, line // block, body, 0)
        src = o_own.at[pl.ds(pl.multiple_of(n * line, line), line)]
        send(src, obuf.at[o_slot(core, x, y)], os_send.at[k], os_recv.at[k], target(0, steps[k], 0))

    def o_slots(i, h, dc=0):
        return obuf.at[pl.ds(o_slot((core + dc) % 2, (x + i + side) % side, h * (side // 2)), side // 2)]

    def o_send(i, h, step, index):
        send(o_slots(i, h), o_slots(i, h), og_send.at[index], og_recv.at[index], at(step, 0, 0))

    def o_share(k, i, h):
        send(o_slots(i, h), o_slots(i, h), op_send.at[k], op_recv.at[k], at(0, 0, 1))

    strip = min(block, line)

    def heads_of(part, at_rows, j, total):
        yy = (y + j + side) % side
        for xx in range(side):
            for c in range(2):
                head = jnp.dot(obuf[o_slot(c, xx, yy), at_rows, :], wbuf[part, (yy * side + xx) * 2 + c], preferred_element_type=jnp.float32)
                total = total + head.astype(jnp.bfloat16).astype(jnp.float32)
        return total

    def project(part, last):
        def body(n, carry):
            at_rows = pl.ds(pl.multiple_of(n * strip, strip), strip)
            if last:
                total = heads_of(part, at_rows, 2, acc[part, at_rows, :])
            else:
                total = lax.fori_loop(0, 3, lambda k, t: heads_of(part, at_rows, (k + 1) % 3 - 1, t), jnp.zeros((strip, cols), jnp.float32))
            acc[part, at_rows, :] = total
            return carry

        lax.fori_loop(0, line // strip, body, 0)

    def back_rows(device):
        return pl.ds(pl.multiple_of(device % (2 * side) * rows, rows), rows)

    def finish(at_cols):
        out_ref[:, at_cols] = res_ref[:, at_cols].astype(jnp.float32) + (rbuf[:, at_cols] + bias_ref[layer:layer + 1, at_cols])

    def proceed():
        attend_line(0)
        attend_line(1)
        w_first(0)
        attend_line(2)
        w_first(1)
        attend_line(3)
        w_relay(0)
        for k, dy in enumerate(steps):
            arrived(obuf.at[o_slot(core, x, (y - dy + side) % side)], os_recv.at[k])
        for h in range(2):
            o_send(0, h, 1, RING.index((-1, h)))
            o_send(0, 1 - h, -1, RING.index((1, 1 - h)))
        w_first(2)
        for h in range(2):
            o_share(h, 0, h)
        w_relay(1)
        w_first(3)
        for k, (i, h) in enumerate(RING):
            arrived(o_slots(i, h), og_recv.at[k])
            if (i, h) == (-1, 0):
                o_send(i, h, 1, RING.index((2, 0)))
            if (i, h) == (1, 1):
                o_send(i, h, -1, RING.index((2, 1)))
            o_share(2 + k, i, h)
            if k == 3:
                w_relay(2)
        for k, (i, h) in enumerate(((0, 0), (0, 1)) + RING):
            arrived(o_slots(i, h, 1), op_recv.at[k])

        for part in range(parts):
            w_arrived(part, -1, 1)
            w_arrived(part, 1, 0)
            project(part, False)
            for h in range(2):
                w_arrived(part, 2, h)
            project(part, True)
            for k, dx in enumerate(steps):
                for dc in range(2):
                    src = acc.at[part, back_rows(at(dx, 0, dc))]
                    dst = rbuf.at[:, pl.ds(first_col(me, part), cols)]
                    send(src, dst, back_send.at[part, k, dc], back_recv.at[part, k, dc], target(dx, 0, dc))
            if part == 0:
                w_relay(3)
        for part in range(parts):
            for k, dx in enumerate(steps):
                for dc in range(2):
                    arrived(rbuf.at[:, pl.ds(first_col(at(-dx, 0, dc), part), cols)], back_recv.at[part, k, dc])
        by_cols(width, finish)

    def drain():
        for copy in sent:
            copy.wait_send()

    return peers + columns, begin, proceed, drain


def front_kernel(side, layer, first, res_ref, ids_in, row_ids_in, gain1_ref, shift1_ref, w_qkv, w_out, bias_ref, gain2_ref, shift2_ref, w_up, b_ref, *refs):
    out_ref, hidden_ref, refs = refs[0], refs[1], refs[2:]
    ids_ref, row_ids_ref = ids_in, row_ids_in
    if first:
        ids_ref, row_ids_ref, refs = refs[0], refs[1], refs[2:]
    w_qkv_ref, w_up_ref, qkv_ref, buf1, buf2, refs = *refs[:5], refs[5:]
    bufs, w_sem, refs = refs[:7], refs[7], refs[8:]
    sems1, sems2, sems = refs[:4], refs[4:8], refs[8:]
    thirds = w_qkv.shape[1]
    each = w_qkv.shape[4]
    loads = [pltpu.make_async_copy(w_qkv.at[layer, k, 0], w_qkv_ref.at[:, pl.ds(k * each, each)], w_sem.at[k]) for k in range(thirds)]
    load_out = pltpu.make_async_copy(w_out.at[layer, 0], bufs[0], w_sem.at[thirds])
    load_up = pltpu.make_async_copy(w_up.at[layer], w_up_ref, w_sem.at[thirds + 1])
    for load in loads + [load_out, load_up]:
        load.start()
    place = Place(side)
    others, begin, proceed, drain = attend_body(place, layer, qkv_ref, ids_ref, row_ids_ref, load_out, res_ref, bias_ref, out_ref, bufs, sems)
    announce(others)
    drain1 = gather_body(place, layer, False, res_ref, gain1_ref, shift1_ref, w_qkv_ref, loads, None, qkv_ref, buf1, sems1, ids_in if first else None, ids_ref if first else None, lambda: meet(others), begin)
    if first:
        step = ids_ref.shape[1]

        def turn(n, carry):
            at = pl.ds(pl.multiple_of(n * step, step), step)
            row_ids_ref[:, at] = jnp.transpose(ids_ref[at, :].astype(jnp.float32))[0:1]
            return carry

        lax.fori_loop(0, ids_ref.shape[0] // step, turn, 0)
    proceed()
    drain2 = gather_body(place, layer, True, out_ref, gain2_ref, shift2_ref, w_up_ref, [load_up], b_ref, hidden_ref, buf2, sems2)
    drain1()
    drain()
    drain2()


def front(side, call_id, layer, first, residual, ids, row_ids, gain1, shift1, w_qkv, w_out, out_bias, gain2, shift2, w_up, up_bias):
    rows, width = residual.shape
    dim = w_out.shape[2]
    groups = 2 * side * side
    seq = groups * rows
    line = rows * 2 * side
    parts = 4
    cols = width // (2 * side) // parts
    block = min(QUERY_BLOCK, line)
    tail = ids.shape[1]
    vmem = pl.BlockSpec(memory_space=pltpu.VMEM)
    hbm = pl.BlockSpec(memory_space=pl.ANY)
    dma = pltpu.SemaphoreType.DMA
    gather_sems = [dma((4, groups)), dma((groups,)), dma((groups,)), dma((groups,))]
    shapes = [((rows, width), jnp.float32), ((seq, w_up.shape[2]), jnp.bfloat16)]
    if first:
        shapes += [((seq, tail), jnp.bfloat16), ((1, seq), jnp.float32)]
    return pl.pallas_call(
        functools.partial(front_kernel, side, layer, first),
        out_shape=[jax.ShapeDtypeStruct(*shape) for shape in shapes],
        in_specs=[vmem] * 5 + [hbm, hbm] + [vmem] * 3 + [hbm, vmem],
        out_specs=[vmem] * len(shapes),
        scratch_shapes=[
            pltpu.VMEM((width, w_qkv.shape[1] * dim), jnp.bfloat16),
            pltpu.VMEM((width, w_up.shape[2]), jnp.bfloat16),
            pltpu.VMEM((seq, w_qkv.shape[1] * dim), jnp.bfloat16),
            pltpu.VMEM((groups, rows, width + (tail if first else 0)), jnp.bfloat16),
            pltpu.VMEM((groups, rows, width), jnp.bfloat16),
            pltpu.VMEM((dim, width), jnp.bfloat16),
            pltpu.VMEM((parts, groups, dim, cols), jnp.bfloat16),
            pltpu.VMEM((groups, line, dim), jnp.bfloat16),
            pltpu.VMEM((seq, dim), jnp.bfloat16),
            pltpu.VMEM((block, seq), jnp.float32),
            pltpu.VMEM((parts, line, cols), jnp.float32),
            pltpu.VMEM((rows, width), jnp.float32),
            dma((w_qkv.shape[1] + 2,)),
            *gather_sems, *gather_sems,
            dma((parts, side, 2)), dma((parts, side, 2)),
            dma((parts, 6)), dma((parts, 6)),
            dma((side,)), dma((side,)),
            dma((6,)), dma((6,)),
            dma((8,)), dma((8,)),
            dma((parts, side, 2)), dma((parts, side, 2)),
        ],
        compiler_params=pltpu.CompilerParams(collective_id=call_id, has_side_effects=True, vmem_limit_bytes=VMEM_LIMIT),
        name=f"front_{call_id}",
    )(residual, ids, row_ids, gain1, shift1, w_qkv, w_out, out_bias, gain2, shift2, w_up, up_bias)


def solution(mesh):
    groups = mesh.shape["tp"]
    side = math.isqrt(groups // 2)
    assert 2 * side * side == groups and side == 4
    row_spec = P("dp", "tp", None)
    vec_spec = P()
    second = P(None, "tp")
    in_specs = (row_spec, P("dp", "tp"), vec_spec, vec_spec, P(None, None, None, "tp"), second, vec_spec, vec_spec, vec_spec, P(None, None, "tp"), second, second, vec_spec)

    def device_fn(tokens, doc_ids, norm1_gain, norm1_shift, qkv_weight, out_weight, out_bias, norm2_gain, norm2_shift, up_weight, up_bias, down_weight, down_bias):
        layers = norm1_gain.shape[0]
        id_cols = jnp.broadcast_to(doc_ids[0].astype(jnp.bfloat16)[:, None], (doc_ids.shape[1], 128))
        qkv_thirds = jnp.transpose(qkv_weight, (0, 2, 3, 1, 4))
        residual = tokens[0]
        all_ids, row_ids = id_cols, jnp.zeros((1, 128), jnp.float32)
        for layer in range(layers):
            first = layer == 0
            residual, hidden, *made = front(side, 2 * layer, layer, first, residual, all_ids, row_ids, norm1_gain, norm1_shift, qkv_thirds, out_weight, out_bias, norm2_gain, norm2_shift, up_weight, up_bias)
            if first:
                all_ids, row_ids = made
            residual = project_and_scatter(side, 2 * layer + 1, layer, hidden, down_weight, residual, down_bias)
        return residual.astype(jnp.bfloat16)[None]

    return jax.shard_map(device_fn, mesh=mesh, in_specs=in_specs, out_specs=row_spec, check_vma=False)
```

```python
import functools
import math

import jax
import jax.numpy as jnp
from jax import lax
from jax.experimental import pallas as pl
from jax.experimental.pallas import tpu as pltpu
from jax.sharding import PartitionSpec as P

COLS = 512
PIECES = 2
MESH = pl.DeviceIdType.MESH
VMEM_LIMIT = 66 * 1000 * 1000

STEPS = (2, 1, -1, 0)
OTHER_SIDE = (2, -1, 1, 0)


class Place:
    def __init__(self, side):
        self.side = side
        self.me = lax.axis_index("tp")
        self.core = self.me % 2
        chip = self.me // 2
        self.x = chip % side
        self.y = chip // side
        self.partner = chip * 2 + 1 - self.core
        self.first = {1: self.dev(1, 0), -1: self.dev(-1, 0)}
        self.second = {1: self.dev(0, 1), -1: self.dev(0, -1)}

    def dev(self, i, j, core=None):
        core = self.core if core is None else core
        dx = i * (1 - core) + j * core
        dy = j * (1 - core) + i * core
        return (((self.y + dy + self.side) % self.side) * self.side + (self.x + dx + self.side) % self.side) * 2 + core

    def neighbours(self):
        return [self.first[1], self.first[-1], self.second[1], self.second[-1], self.partner]


def announce(others):
    for other in others:
        pl.semaphore_signal(pltpu.get_barrier_semaphore(), inc=1, device_id={"tp": other}, device_id_type=MESH)


def meet(others):
    pl.semaphore_wait(pltpu.get_barrier_semaphore(), len(others))


def by_cols(width, fn, step=COLS // 2):
    step = min(step, width)

    def body(n, carry):
        fn(pl.ds(pl.multiple_of(n * step, step), step))
        return carry

    lax.fori_loop(0, width // step, body, 0)


def scatter_kernel(side, layer, act_ref, w_hbm, res_ref, bias_ref, out_ref, w_ref, own, snd, prt, stg, mid, fin, stg2, mid2, fin2, w_sem, pair_send, pair_recv, send_sem, recv_sem):
    load_w = pltpu.make_async_copy(w_hbm.at[layer, 0] if len(w_hbm.shape) == 4 else w_hbm.at[layer], w_ref, w_sem)
    load_w.start()
    place = Place(side)
    rows, width = res_ref.shape
    half = rows // 2
    announce(place.neighbours())
    load_w.wait()

    span = width // PIECES

    def piece_of(z):
        return pl.ds(z * span, span)

    def by_piece(z, fn, step=COLS // 2):
        by_cols(span, lambda at: fn(pl.ds(pl.multiple_of(z * span + at.start, 128), at.size)), step)

    def remote(src, dst, slot, z, device):
        return pltpu.make_async_remote_copy(src_ref=src.at[:, piece_of(z)], dst_ref=dst.at[:, piece_of(z)], send_sem=send_sem.at[slot, z], recv_sem=recv_sem.at[slot, z], device_id={"tp": device}, device_id_type=MESH)

    def pair_copy(g, jj, z):
        return pltpu.make_async_remote_copy(src_ref=snd.at[g % 2, jj, :, piece_of(z)], dst_ref=prt.at[g, jj, :, piece_of(z)], send_sem=pair_send.at[g, jj, z], recv_sem=pair_recv.at[g, jj, z], device_id={"tp": place.partner}, device_id_type=MESH)

    def product(core, g, z, dst):
        starts = [pl.multiple_of(place.dev(i, j, core) * rows + h * half, half) for j in STEPS for h, i in enumerate((STEPS[g], OTHER_SIDE[g]))]

        def piece(cols):
            lhs = jnp.concatenate([act_ref[pl.ds(s, half), :] for s in starts], axis=0)
            part = jnp.dot(lhs, w_ref[:, cols], preferred_element_type=jnp.float32).astype(jnp.bfloat16)
            for jj in range(side):
                dst[jj, :, cols] = part[jj * rows:(jj + 1) * rows]

        by_piece(z, piece, COLS)

    def pair_sum(g, jj, h, cols):
        at = pl.ds(h * half, half)
        return own[g, jj, at, cols].astype(jnp.float32) + prt[g, jj, at, cols].astype(jnp.float32)

    far, plus, minus, here = range(side)
    sent = []

    def send(src, dst, slot, z, device):
        copy = remote(src, dst, slot, z, device)
        copy.start()
        sent.append(copy)

    def arrived(dst, slot, z):
        remote(dst, dst, slot, z, place.me).wait_recv()

    def open_group(g, z):
        for jj in range(side):
            if g >= 2:
                pair_copy(g - 2, jj, z).wait_send()
        product(1 - place.core, g, z, snd.at[g % 2])
        if g == 0 and z == 0:
            meet(place.neighbours())
        for jj in range(side):
            pair_copy(g, jj, z).start()
        product(place.core, g, z, own.at[g])
        shared = set()
        for k, (jj, h) in enumerate(((far, 0), (far, 1), (plus, 1), (minus, 0))):
            if jj not in shared:
                shared.add(jj)
                pair_copy(g, jj, z).wait_recv()
            def stage(cols, k=k, jj=jj, h=h):
                stg[g, k, :, cols] = pair_sum(g, jj, h, cols)
            by_piece(z, stage)
            dst = mid.at[g, k] if k < 2 else fin.at[g, k]
            slot = 6 * g + (4 + k if k < 2 else k)
            send(stg.at[g, k], dst, slot, z, place.second[1 if k % 2 == 0 else -1])

    def relay(g, z):
        for k, (jj, h) in enumerate(((plus, 0), (minus, 1))):
            arrived(mid.at[g, k], 6 * g + 4 + k, z)
            def add(cols, k=k, jj=jj, h=h):
                mid[g, k, :, cols] += pair_sum(g, jj, h, cols)
            by_piece(z, add)
            send(mid.at[g, k], fin.at[g, k], 6 * g + k, z, place.second[1 if k == 0 else -1])

    base = 6 * side

    def close_group(g, z):
        pair_copy(g, here, z).wait_recv()
        for k in range(4):
            arrived(fin.at[g, k], 6 * g + k, z)

        def total(h, cols):
            return pair_sum(g, here, h, cols) + fin[g, 0 if h == 0 else 1, :, cols] + fin[g, 3 if h == 0 else 2, :, cols]

        def keep(k, h):
            def fn(cols):
                stg2[k, :, cols] = total(h, cols)
            by_piece(z, fn)

        def join(k):
            arrived(mid2.at[k], base + 4 + k, z)
            def fn(cols):
                mid2[k, :, cols] += total(k, cols)
            by_piece(z, fn)
            send(mid2.at[k], fin2.at[k], base + k, z, place.first[1 if k == 0 else -1])

        if g == far:
            keep(0, 0)
            send(stg2.at[0], mid2.at[0], base + 4, z, place.first[1])
            keep(1, 1)
            send(stg2.at[1], mid2.at[1], base + 5, z, place.first[-1])
        elif g == plus:
            join(0)
            join(1)
        elif g == minus:
            keep(2, 1)
            send(stg2.at[2], fin2.at[2], base + 2, z, place.first[1])
            keep(3, 0)
            send(stg2.at[3], fin2.at[3], base + 3, z, place.first[-1])
        else:
            for k in range(4):
                arrived(fin2.at[k], base + k, z)
            for h in range(2):
                def fn(cols, h=h):
                    at = pl.ds(h * half, half)
                    summed = total(h, cols) + fin2[0 if h == 0 else 1, :, cols] + fin2[3 if h == 0 else 2, :, cols]
                    out_ref[at, cols] = res_ref[at, cols] + (summed + bias_ref[layer:layer + 1, cols])
                by_piece(z, fn)

    for act, g in ((open_group, 0), (open_group, 1), (open_group, 2), (relay, 0), (open_group, 3), (relay, 1), (close_group, 0), (relay, 2), (close_group, 1), (relay, 3), (close_group, 2), (close_group, 3)):
        for z in range(PIECES):
            act(g, z)
    for g in (side - 2, side - 1):
        for jj in range(side):
            for z in range(PIECES):
                pair_copy(g, jj, z).wait_send()
    for copy in sent:
        copy.wait_send()


def project_and_scatter(side, call_id, layer, act, weight, residual, bias):
    rows, width = residual.shape
    depth = act.shape[1]
    half = rows // 2
    quad = (side, side, rows, width)
    part = (side, 2, half, width)
    vmem = pl.BlockSpec(memory_space=pltpu.VMEM)
    return pl.pallas_call(
        functools.partial(scatter_kernel, side, layer),
        out_shape=jax.ShapeDtypeStruct((rows, width), jnp.float32),
        in_specs=[vmem, pl.BlockSpec(memory_space=pl.ANY), vmem, vmem],
        out_specs=vmem,
        scratch_shapes=[
            pltpu.VMEM((depth, width), jnp.bfloat16),
            pltpu.VMEM(quad, jnp.bfloat16),
            pltpu.VMEM((2,) + quad[1:], jnp.bfloat16),
            pltpu.VMEM(quad, jnp.bfloat16),
            pltpu.VMEM((side, 4, half, width), jnp.float32),
            pltpu.VMEM(part, jnp.float32),
            pltpu.VMEM((side, 4, half, width), jnp.float32),
            pltpu.VMEM((4, half, width), jnp.float32),
            pltpu.VMEM((2, half, width), jnp.float32),
            pltpu.VMEM((4, half, width), jnp.float32),
            pltpu.SemaphoreType.DMA,
            pltpu.SemaphoreType.DMA((side, side, PIECES)),
            pltpu.SemaphoreType.DMA((side, side, PIECES)),
            pltpu.SemaphoreType.DMA((6 * side + 6, PIECES)),
            pltpu.SemaphoreType.DMA((6 * side + 6, PIECES)),
        ],
        compiler_params=pltpu.CompilerParams(collective_id=call_id, has_side_effects=True, vmem_limit_bytes=VMEM_LIMIT),
        name=f"scatter_{call_id}",
    )(act, weight, residual, bias)


GATHER_ORDER = sorted(((i, j) for i in STEPS for j in STEPS), key=lambda at: (2 * abs(at[0]) + 3 * abs(at[1]), at))


def gather_body(place, layer, gelu, res_ref, gain_ref, shift_ref, w_ref, loads, b_ref, out, buf, sems, tails=None, tails_out=None, ready=None, hook=None):
    send_sem, recv_sem, pair_send, pair_recv = sems
    side = place.side
    rows, width = res_ref.shape
    tail = 0 if tails is None else tails.shape[1]
    half = rows // 2
    for at in (pl.ds(0, half), pl.ds(half, half)):
        residual = res_ref[at, :].astype(jnp.float32)
        centered = residual - jnp.mean(residual, axis=-1, keepdims=True)
        variance = jnp.mean(centered * centered, axis=-1, keepdims=True)
        normed = centered * lax.rsqrt(variance + 1e-5) * gain_ref[layer:layer + 1, :] + shift_ref[layer:layer + 1, :]
        buf[place.me, at, pl.ds(0, width)] = normed.astype(jnp.bfloat16)
    if tail:
        buf[place.me, :, pl.ds(width, tail)] = tails[...]
    if ready is not None:
        ready()

    def pick(n, values):
        value = values[0]
        for k, other in enumerate(values):
            value = jnp.where(n == k, other, value)
        return value

    def view(i, j, h, core=None):
        return buf.at[place.dev(i, j, core), pl.ds(pl.multiple_of(h * half, half), half)]

    def wrap(k):
        return (k + side + 1) % side - 1

    def slot(i, j, h):
        return ((i + side) % side * side + (j + side) % side) * 2 + h

    def ring_copies(i, j, h):
        own = (j == 0) & (i == 0)
        begins = (h == 0, h == 1)
        for axis, ahead in enumerate(((j == 0, i), (True, j))):
            whole = own if axis == 0 else j == 0
            for side_of, step in enumerate((1, -1)):
                there = (wrap(i - step), j) if axis == 0 else (i, wrap(j - step))
                device = (place.first, place.second)[axis][step]
                condition = whole | (ahead[0] & (ahead[1] == -step) & begins[side_of])
                yield condition, pltpu.make_async_remote_copy(src_ref=view(i, j, h), dst_ref=view(i, j, h), send_sem=send_sem.at[axis * 2 + side_of, slot(i, j, h)], recv_sem=recv_sem.at[slot(*there, h)], device_id={"tp": device}, device_id_type=MESH)

    def pair(i, j, h, core=None):
        index = slot(i, j, h)
        ref = view(i, j, h, core)
        return pltpu.make_async_remote_copy(src_ref=ref, dst_ref=ref, send_sem=pair_send.at[index], recv_sem=pair_recv.at[index], device_id={"tp": place.partner}, device_id_type=MESH)

    def arrived(i, j, h):
        ref = view(i, j, h)
        pltpu.make_async_remote_copy(src_ref=ref, dst_ref=ref, send_sem=send_sem.at[0, 0], recv_sem=recv_sem.at[slot(i, j, h)], device_id={"tp": place.me}, device_id_type=MESH).wait_recv()

    def multiply(i, j):
        devs = [place.dev(i, j), place.dev(i, j, 1 - place.core)]
        at = [pl.ds(pl.multiple_of(d * rows, rows), rows) for d in devs]
        if tail:
            for d, where in zip(devs, at):
                tails_out[where, :] = buf[d, :, pl.ds(width, tail)]
        lhs = jnp.concatenate([buf[d, :, pl.ds(0, width)] for d in devs], axis=0)
        part = jnp.dot(lhs, w_ref[...], preferred_element_type=jnp.float32)
        if gelu:
            part = jax.nn.gelu(part + b_ref[layer:layer + 1, :], approximate=True)
        part = part.astype(jnp.bfloat16)
        for k, where in enumerate(at):
            out[where, :] = part[k * rows:(k + 1) * rows]

    firsts = [at[0] for at in GATHER_ORDER]
    seconds = [at[1] for at in GATHER_ORDER]
    leads = [int(1 in at and -1 not in at) for at in GATHER_ORDER]

    def take(n, carry):
        i, j, lead = pick(n, firsts), pick(n, seconds), pick(n, leads)
        for k in range(2):
            h = (lead + k) % 2

            @pl.when(n > 0)
            def _():
                arrived(i, j, h)

            for condition, copy in ring_copies(i, j, h):
                pl.when(condition)(copy.start)
            pair(i, j, h).start()

        @pl.when(n == 0)
        def _():
            for load in loads:
                load.wait()

        for h in range(2):
            pair(i, j, h, 1 - place.core).wait_recv()
        multiply(i, j)
        return carry

    def drain(n, carry):
        i, j = pick(n, firsts), pick(n, seconds)
        for h in range(2):
            for condition, copy in ring_copies(i, j, h):
                pl.when(condition)(copy.wait_send)
            pair(i, j, h).wait_send()
        return carry

    last = max(n for n, at in enumerate(GATHER_ORDER) if at[1] != 2) + 1
    lax.fori_loop(0, last, take, 0)
    if hook is not None:
        hook()
    lax.fori_loop(last, len(GATHER_ORDER), take, 0)
    return lambda: lax.fori_loop(0, len(GATHER_ORDER), drain, 0)


QUERY_BLOCK = 256
RING = ((-1, 0), (1, 1), (-1, 1), (1, 0), (2, 0), (2, 1))


def attend_body(place, layer, qkv_ref, ids_ref, row_ids_ref, load_w, res_ref, bias_ref, out_ref, bufs, sems):
    w_own, wbuf, obuf, o_own, scores, acc, rbuf = bufs
    ws_send, ws_recv, wg_send, wg_recv, os_send, os_recv, og_send, og_recv, op_send, op_recv, back_send, back_recv = sems
    side, me, core, x, y = place.side, place.me, place.core, place.x, place.y
    rows, width = res_ref.shape
    dim = w_own.shape[0]
    share = width // (2 * side)
    parts, _, _, cols = wbuf.shape
    line = rows * 2 * side
    steps = STEPS

    def at(dx, dy, dc):
        return (((y + dy + side) % side) * side + (x + dx + side) % side) * 2 + (core + dc) % 2

    peers = [at(dx, 0, dc) for dx in steps for dc in (1, 0) if (dx, dc) != (0, 0)]
    columns = [at(0, dy, 0) for dy in steps[:3]]
    sent = []

    def send(src, dst, send_sem, recv_sem, device):
        if device is None:
            copy = pltpu.make_async_copy(src, dst, recv_sem)
        else:
            copy = pltpu.make_async_remote_copy(src_ref=src, dst_ref=dst, send_sem=send_sem, recv_sem=recv_sem, device_id={"tp": device}, device_id_type=MESH)
            sent.append(copy)
        copy.start()

    def arrived(dst, recv_sem):
        pltpu.make_async_copy(dst, dst, recv_sem).wait()

    def target(dx, dy, dc):
        return None if (dx, dy, dc) == (0, 0, 0) else at(dx, dy, dc)

    def first_col(device, part):
        return pl.multiple_of(device % (2 * side) * share + part * cols, 128)

    def begin():
        load_w.wait()
        for part in range(parts):
            for k, dx in enumerate(steps):
                for dc in range(2):
                    src = w_own.at[:, pl.ds(first_col(at(dx, 0, dc), part), cols)]
                    send(src, wbuf.at[part, me], ws_send.at[part, k, dc], ws_recv.at[part, k, dc], target(dx, 0, dc))

    def w_slots(part, j, h):
        return wbuf.at[part, pl.ds(((y + j + side) % side) * 2 * side + h * side, side)]

    def w_ring(part, j, h):
        index = RING.index((j, h))
        return wg_send.at[part, index], wg_recv.at[part, index]

    def w_first(part):
        for k, dx in enumerate(steps):
            for dc in range(2):
                arrived(wbuf.at[part, at(-dx, 0, dc)], ws_recv.at[part, k, dc])
        for h in range(2):
            send(w_slots(part, 0, h), w_slots(part, 0, h), *w_ring(part, -1, h), at(0, 1, 0))
            send(w_slots(part, 0, 1 - h), w_slots(part, 0, 1 - h), *w_ring(part, 1, 1 - h), at(0, -1, 0))

    def w_arrived(part, j, h):
        arrived(w_slots(part, j, h), w_ring(part, j, h)[1])

    def w_relay(part):
        w_arrived(part, -1, 0)
        send(w_slots(part, -1, 0), w_slots(part, -1, 0), *w_ring(part, 2, 0), at(0, 1, 0))
        w_arrived(part, 1, 1)
        send(w_slots(part, 1, 1), w_slots(part, 1, 1), *w_ring(part, 2, 1), at(0, -1, 0))

    block = scores.shape[0]
    half = block // 2

    def attend(b):
        q_rows = pl.ds(pl.multiple_of(b * block, block), block)
        q = qkv_ref[q_rows, pl.ds(0, dim)]
        q_ids = ids_ref[q_rows, 0:1].astype(jnp.float32)
        q_pos = b * block + lax.broadcasted_iota(jnp.int32, (block, block), 0)

        def chunk(c):
            return pl.ds(pl.multiple_of(c * block, block), block)

        def score(c, top):
            s = lax.dot_general(q, qkv_ref[chunk(c), pl.ds(dim, dim)], (((1,), (1,)), ((), ())), preferred_element_type=jnp.float32) * dim ** -0.5
            k_pos = c * block + lax.broadcasted_iota(jnp.int32, (block, block), 1)
            allowed = (k_pos <= q_pos) & (row_ids_ref[0:1, chunk(c)] == q_ids)
            s = jnp.where(allowed, s, -1e30)
            scores[:, chunk(c)] = s
            return jnp.maximum(top, jnp.maximum(s[:, :half], s[:, half:]))

        top = jnp.max(lax.fori_loop(0, b + 1, score, jnp.full((block, half), -1e30, jnp.float32)), axis=-1, keepdims=True)

        def power(c, total):
            e = jnp.exp(scores[:, chunk(c)] - top)
            scores[:, chunk(c)] = e
            return total + (e[:, :half] + e[:, half:])

        total = jnp.sum(lax.fori_loop(0, b + 1, power, jnp.zeros((block, half), jnp.float32)), axis=-1, keepdims=True)
        inverse = 1.0 / total

        def mix(c, mixed):
            probs = (scores[:, chunk(c)] * inverse).astype(jnp.bfloat16)
            return mixed + jnp.dot(probs, qkv_ref[chunk(c), pl.ds(2 * dim, dim)], preferred_element_type=jnp.float32)

        o_own[q_rows, :] = lax.fori_loop(0, b + 1, mix, jnp.zeros((block, dim), jnp.float32)).astype(jnp.bfloat16)

    def o_slot(c, xx, yy):
        return (c * side + xx) * side + yy

    def attend_line(k):
        n = (y + steps[k] + side) % side

        def body(b, carry):
            attend(n * (line // block) + b)
            return carry

        lax.fori_loop(0, line // block, body, 0)
        src = o_own.at[pl.ds(pl.multiple_of(n * line, line), line)]
        send(src, obuf.at[o_slot(core, x, y)], os_send.at[k], os_recv.at[k], target(0, steps[k], 0))

    def o_view(k, i, dc=0):
        return obuf.at[o_slot((core + dc) % 2, (x + i + side) % side, (y - steps[k] + side) % side)]

    def o_half(k, i, h):
        return o_view(k, i).at[pl.ds(h * (line // 2), line // 2)]

    def o_send(k, i, h, step):
        index = RING.index(((i - step + side + 1) % side - 1, h))
        send(o_half(k, i, h), o_half(k, i, h), og_send.at[k, index], og_recv.at[k, index], at(step, 0, 0))

    def o_arrived(k, i, h):
        arrived(o_half(k, i, h), og_recv.at[k, RING.index((i, h))])

    def o_share(k, i):
        send(o_view(k, i), o_view(k, i), op_send.at[k, i % side], op_recv.at[k, i % side], at(0, 0, 1))

    def o_first(k):
        arrived(o_view(k, 0), os_recv.at[k])
        for h in range(2):
            o_send(k, 0, h, 1)
            o_send(k, 0, 1 - h, -1)
        o_share(k, 0)

    def o_relay(k):
        o_arrived(k, -1, 0)
        o_send(k, -1, 0, 1)
        o_arrived(k, 1, 1)
        o_send(k, 1, 1, -1)

    def o_rest(k):
        o_arrived(k, -1, 1)
        o_share(k, -1)
        o_arrived(k, 1, 0)
        o_share(k, 1)
        for h in range(2):
            o_arrived(k, 2, h)
        o_share(k, 2)

    strip = min(block, line)

    def heads_of(part, at_rows, j, total):
        yy = (y + j + side) % side
        for xx in range(side):
            for c in range(2):
                head = jnp.dot(obuf[o_slot(c, xx, yy), at_rows, :], wbuf[part, (yy * side + xx) * 2 + c], preferred_element_type=jnp.float32)
                total = total + head.astype(jnp.bfloat16).astype(jnp.float32)
        return total

    def project(part, last):
        def body(n, carry):
            at_rows = pl.ds(pl.multiple_of(n * strip, strip), strip)
            if last:
                total = heads_of(part, at_rows, 2, acc[part, at_rows, :])
            else:
                total = lax.fori_loop(0, 3, lambda k, t: heads_of(part, at_rows, (k + 1) % 3 - 1, t), jnp.zeros((strip, cols), jnp.float32))
            acc[part, at_rows, :] = total
            return carry

        lax.fori_loop(0, line // strip, body, 0)

    def back_rows(device):
        return pl.ds(pl.multiple_of(device % (2 * side) * rows, rows), rows)

    def finish(at_cols):
        out_ref[:, at_cols] = res_ref[:, at_cols].astype(jnp.float32) + (rbuf[:, at_cols] + bias_ref[layer:layer + 1, at_cols])

    def proceed():
        attend_line(0)
        attend_line(1)
        w_first(0)
        attend_line(2)
        o_first(0)
        w_first(1)
        attend_line(3)
        o_first(1)
        w_relay(0)
        o_first(3)
        o_first(2)
        o_relay(0)
        w_first(2)
        o_relay(1)
        w_relay(1)
        o_relay(3)
        o_relay(2)
        w_first(3)
        for k in range(side):
            o_rest(k)
        w_relay(2)
        for k in range(side):
            for i in steps:
                arrived(o_view(k, i, 1), op_recv.at[k, i % side])

        for part in range(parts):
            w_arrived(part, -1, 1)
            w_arrived(part, 1, 0)
            project(part, False)
            for h in range(2):
                w_arrived(part, 2, h)
            project(part, True)
            for k, dx in enumerate(steps):
                for dc in range(2):
                    src = acc.at[part, back_rows(at(dx, 0, dc))]
                    dst = rbuf.at[:, pl.ds(first_col(me, part), cols)]
                    send(src, dst, back_send.at[part, k, dc], back_recv.at[part, k, dc], target(dx, 0, dc))
            if part == 0:
                w_relay(3)
        for part in range(parts):
            for k, dx in enumerate(steps):
                for dc in range(2):
                    arrived(rbuf.at[:, pl.ds(first_col(at(-dx, 0, dc), part), cols)], back_recv.at[part, k, dc])
        by_cols(width, finish)

    def drain():
        for copy in sent:
            copy.wait_send()

    return peers + columns, begin, proceed, drain


def front_kernel(side, layer, first, res_ref, ids_in, row_ids_in, gain1_ref, shift1_ref, w_qkv, w_out, bias_ref, gain2_ref, shift2_ref, w_up, b_ref, *refs):
    out_ref, hidden_ref, refs = refs[0], refs[1], refs[2:]
    ids_ref, row_ids_ref = ids_in, row_ids_in
    if first:
        ids_ref, row_ids_ref, refs = refs[0], refs[1], refs[2:]
    w_qkv_ref, w_up_ref, qkv_ref, buf1, buf2, refs = *refs[:5], refs[5:]
    bufs, w_sem, refs = refs[:7], refs[7], refs[8:]
    sems1, sems2, sems = refs[:4], refs[4:8], refs[8:]
    thirds = w_qkv.shape[1]
    each = w_qkv.shape[4]
    loads = [pltpu.make_async_copy(w_qkv.at[layer, k, 0], w_qkv_ref.at[:, pl.ds(k * each, each)], w_sem.at[k]) for k in range(thirds)]
    load_out = pltpu.make_async_copy(w_out.at[layer, 0], bufs[0], w_sem.at[thirds])
    load_up = pltpu.make_async_copy(w_up.at[layer], w_up_ref, w_sem.at[thirds + 1])
    for load in loads + [load_out, load_up]:
        load.start()
    place = Place(side)
    others, begin, proceed, drain = attend_body(place, layer, qkv_ref, ids_ref, row_ids_ref, load_out, res_ref, bias_ref, out_ref, bufs, sems)
    announce(others)
    drain1 = gather_body(place, layer, False, res_ref, gain1_ref, shift1_ref, w_qkv_ref, loads, None, qkv_ref, buf1, sems1, ids_in if first else None, ids_ref if first else None, lambda: meet(others), begin)
    if first:
        step = ids_ref.shape[1]

        def turn(n, carry):
            at = pl.ds(pl.multiple_of(n * step, step), step)
            row_ids_ref[:, at] = jnp.transpose(ids_ref[at, :].astype(jnp.float32))[0:1]
            return carry

        lax.fori_loop(0, ids_ref.shape[0] // step, turn, 0)
    proceed()
    drain2 = gather_body(place, layer, True, out_ref, gain2_ref, shift2_ref, w_up_ref, [load_up], b_ref, hidden_ref, buf2, sems2)
    drain1()
    drain()
    drain2()


def front(side, call_id, layer, first, residual, ids, row_ids, gain1, shift1, w_qkv, w_out, out_bias, gain2, shift2, w_up, up_bias):
    rows, width = residual.shape
    dim = w_out.shape[2]
    groups = 2 * side * side
    seq = groups * rows
    line = rows * 2 * side
    parts = 4
    cols = width // (2 * side) // parts
    block = min(QUERY_BLOCK, line)
    tail = ids.shape[1]
    vmem = pl.BlockSpec(memory_space=pltpu.VMEM)
    hbm = pl.BlockSpec(memory_space=pl.ANY)
    dma = pltpu.SemaphoreType.DMA
    gather_sems = [dma((4, groups)), dma((groups,)), dma((groups,)), dma((groups,))]
    shapes = [((rows, width), jnp.float32), ((seq, w_up.shape[2]), jnp.bfloat16)]
    if first:
        shapes += [((seq, tail), jnp.bfloat16), ((1, seq), jnp.float32)]
    return pl.pallas_call(
        functools.partial(front_kernel, side, layer, first),
        out_shape=[jax.ShapeDtypeStruct(*shape) for shape in shapes],
        in_specs=[vmem] * 5 + [hbm, hbm] + [vmem] * 3 + [hbm, vmem],
        out_specs=[vmem] * len(shapes),
        scratch_shapes=[
            pltpu.VMEM((width, w_qkv.shape[1] * dim), jnp.bfloat16),
            pltpu.VMEM((width, w_up.shape[2]), jnp.bfloat16),
            pltpu.VMEM((seq, w_qkv.shape[1] * dim), jnp.bfloat16),
            pltpu.VMEM((groups, rows, width + (tail if first else 0)), jnp.bfloat16),
            pltpu.VMEM((groups, rows, width), jnp.bfloat16),
            pltpu.VMEM((dim, width), jnp.bfloat16),
            pltpu.VMEM((parts, groups, dim, cols), jnp.bfloat16),
            pltpu.VMEM((groups, line, dim), jnp.bfloat16),
            pltpu.VMEM((seq, dim), jnp.bfloat16),
            pltpu.VMEM((block, seq), jnp.float32),
            pltpu.VMEM((parts, line, cols), jnp.float32),
            pltpu.VMEM((rows, width), jnp.float32),
            dma((w_qkv.shape[1] + 2,)),
            *gather_sems, *gather_sems,
            dma((parts, side, 2)), dma((parts, side, 2)),
            dma((parts, 6)), dma((parts, 6)),
            dma((side,)), dma((side,)),
            dma((side, 6)), dma((side, 6)),
            dma((side, side)), dma((side, side)),
            dma((parts, side, 2)), dma((parts, side, 2)),
        ],
        compiler_params=pltpu.CompilerParams(collective_id=call_id, has_side_effects=True, vmem_limit_bytes=VMEM_LIMIT),
        name=f"front_{call_id}",
    )(residual, ids, row_ids, gain1, shift1, w_qkv, w_out, out_bias, gain2, shift2, w_up, up_bias)


def solution(mesh):
    groups = mesh.shape["tp"]
    side = math.isqrt(groups // 2)
    assert 2 * side * side == groups and side == 4
    row_spec = P("dp", "tp", None)
    vec_spec = P()
    second = P(None, "tp")
    in_specs = (row_spec, P("dp", "tp"), vec_spec, vec_spec, P(None, None, None, "tp"), second, vec_spec, vec_spec, vec_spec, P(None, None, "tp"), second, second, vec_spec)

    def device_fn(tokens, doc_ids, norm1_gain, norm1_shift, qkv_weight, out_weight, out_bias, norm2_gain, norm2_shift, up_weight, up_bias, down_weight, down_bias):
        layers = norm1_gain.shape[0]
        id_cols = jnp.broadcast_to(doc_ids[0].astype(jnp.bfloat16)[:, None], (doc_ids.shape[1], 128))
        qkv_thirds = jnp.transpose(qkv_weight, (0, 2, 3, 1, 4))
        residual = tokens[0]
        all_ids, row_ids = id_cols, jnp.zeros((1, 128), jnp.float32)
        for layer in range(layers):
            first = layer == 0
            residual, hidden, *made = front(side, 2 * layer, layer, first, residual, all_ids, row_ids, norm1_gain, norm1_shift, qkv_thirds, out_weight, out_bias, norm2_gain, norm2_shift, up_weight, up_bias)
            if first:
                all_ids, row_ids = made
            residual = project_and_scatter(side, 2 * layer + 1, layer, hidden, down_weight, residual, down_bias)
        return residual.astype(jnp.bfloat16)[None]

    return jax.shard_map(device_fn, mesh=mesh, in_specs=in_specs, out_specs=row_spec, check_vma=False)
```

```python
import functools
import math

import jax
import jax.numpy as jnp
from jax import lax
from jax.experimental import pallas as pl
from jax.experimental.pallas import tpu as pltpu
from jax.sharding import PartitionSpec as P

COLS = 512
PIECES = 2
MESH = pl.DeviceIdType.MESH
VMEM_LIMIT = 66 * 1000 * 1000

STEPS = (2, 1, -1, 0)
OTHER_SIDE = (2, -1, 1, 0)


class Place:
    def __init__(self, side):
        self.side = side
        self.me = lax.axis_index("tp")
        self.core = self.me % 2
        chip = self.me // 2
        self.x = chip % side
        self.y = chip // side
        self.partner = chip * 2 + 1 - self.core
        self.first = {1: self.dev(1, 0), -1: self.dev(-1, 0)}
        self.second = {1: self.dev(0, 1), -1: self.dev(0, -1)}

    def dev(self, i, j, core=None):
        core = self.core if core is None else core
        dx = i * (1 - core) + j * core
        dy = j * (1 - core) + i * core
        return (((self.y + dy + self.side) % self.side) * self.side + (self.x + dx + self.side) % self.side) * 2 + core

    def neighbours(self):
        return [self.first[1], self.first[-1], self.second[1], self.second[-1], self.partner]


def announce(others):
    for other in others:
        pl.semaphore_signal(pltpu.get_barrier_semaphore(), inc=1, device_id={"tp": other}, device_id_type=MESH)


def meet(others):
    pl.semaphore_wait(pltpu.get_barrier_semaphore(), len(others))


def by_cols(width, fn, step=COLS // 2):
    step = min(step, width)

    def body(n, carry):
        fn(pl.ds(pl.multiple_of(n * step, step), step))
        return carry

    lax.fori_loop(0, width // step, body, 0)


def scatter_kernel(side, layer, act_ref, w_hbm, res_ref, bias_ref, out_ref, w_ref, own, snd, prt, stg, mid, fin, stg2, mid2, fin2, w_sem, pair_send, pair_recv, send_sem, recv_sem):
    load_w = pltpu.make_async_copy(w_hbm.at[layer, 0] if len(w_hbm.shape) == 4 else w_hbm.at[layer], w_ref, w_sem)
    load_w.start()
    place = Place(side)
    rows, width = res_ref.shape
    half = rows // 2
    announce(place.neighbours())
    load_w.wait()

    span = width // PIECES

    def piece_of(z):
        return pl.ds(pl.multiple_of(z * span, 128), span)

    def by_piece(z, fn, step=COLS // 2):
        by_cols(span, lambda at: fn(pl.ds(pl.multiple_of(z * span + at.start, 128), at.size)), step)

    def block_of(place_in, z):
        ref, index = place_in
        return ref.at[(*index, slice(None), piece_of(z))]

    def remote(src, dst, slot, z, device):
        return pltpu.make_async_remote_copy(src_ref=block_of(src, z), dst_ref=block_of(dst, z), send_sem=send_sem.at[slot, z], recv_sem=recv_sem.at[slot, z], device_id={"tp": device}, device_id_type=MESH)

    def pair_copy(g, jj, z):
        return pltpu.make_async_remote_copy(src_ref=snd.at[g % 2, jj, :, piece_of(z)], dst_ref=prt.at[g, jj, :, piece_of(z)], send_sem=pair_send.at[g, jj, z], recv_sem=pair_recv.at[g, jj, z], device_id={"tp": place.partner}, device_id_type=MESH)

    def product(core, g, z, dst):
        starts = [pl.multiple_of(place.dev(i, j, core) * rows + h * half, half) for j in STEPS for h, i in enumerate((STEPS[g], OTHER_SIDE[g]))]

        def piece(cols):
            lhs = jnp.concatenate([act_ref[pl.ds(s, half), :] for s in starts], axis=0)
            part = jnp.dot(lhs, w_ref[:, cols], preferred_element_type=jnp.float32).astype(jnp.bfloat16)
            for jj in range(side):
                dst[jj, :, cols] = part[jj * rows:(jj + 1) * rows]

        by_piece(z, piece, COLS)

    def pair_sum(g, jj, h, cols):
        at = pl.ds(h * half, half)
        return own[g, jj, at, cols].astype(jnp.float32) + prt[g, jj, at, cols].astype(jnp.float32)

    far, plus, minus, here = range(side)
    sent = []

    def send(src, dst, slot, z, device):
        remote(src, dst, slot, z, device).start()
        sent.append((src, dst, slot, device))

    def arrived(dst, slot, z):
        remote(dst, dst, slot, z, place.me).wait_recv()

    def open_group(g, z):
        for jj in range(side):
            if g >= 2:
                pair_copy(g - 2, jj, z).wait_send()
        product(1 - place.core, g, z, snd.at[g % 2])
        if g == 0:
            pl.when(z == 0)(lambda: meet(place.neighbours()))
        for jj in range(side):
            pair_copy(g, jj, z).start()
        product(place.core, g, z, own.at[g])
        shared = set()
        for k, (jj, h) in enumerate(((far, 0), (far, 1), (plus, 1), (minus, 0))):
            if jj not in shared:
                shared.add(jj)
                pair_copy(g, jj, z).wait_recv()
            def stage(cols, k=k, jj=jj, h=h):
                stg[g, k, :, cols] = pair_sum(g, jj, h, cols)
            by_piece(z, stage)
            dst = (mid, (g, k)) if k < 2 else (fin, (g, k))
            slot = 6 * g + (4 + k if k < 2 else k)
            send((stg, (g, k)), dst, slot, z, place.second[1 if k % 2 == 0 else -1])

    def relay(g, z):
        for k, (jj, h) in enumerate(((plus, 0), (minus, 1))):
            arrived((mid, (g, k)), 6 * g + 4 + k, z)
            def add(cols, k=k, jj=jj, h=h):
                mid[g, k, :, cols] += pair_sum(g, jj, h, cols)
            by_piece(z, add)
            send((mid, (g, k)), (fin, (g, k)), 6 * g + k, z, place.second[1 if k == 0 else -1])

    base = 6 * side

    def close_group(g, z):
        pair_copy(g, here, z).wait_recv()
        for k in range(4):
            arrived((fin, (g, k)), 6 * g + k, z)

        def total(h, cols):
            return pair_sum(g, here, h, cols) + fin[g, 0 if h == 0 else 1, :, cols] + fin[g, 3 if h == 0 else 2, :, cols]

        def keep(k, h):
            def fn(cols):
                stg2[k, :, cols] = total(h, cols)
            by_piece(z, fn)

        def join(k):
            arrived((mid2, (k,)), base + 4 + k, z)
            def fn(cols):
                mid2[k, :, cols] += total(k, cols)
            by_piece(z, fn)
            send((mid2, (k,)), (fin2, (k,)), base + k, z, place.first[1 if k == 0 else -1])

        if g == far:
            keep(0, 0)
            send((stg2, (0,)), (mid2, (0,)), base + 4, z, place.first[1])
            keep(1, 1)
            send((stg2, (1,)), (mid2, (1,)), base + 5, z, place.first[-1])
        elif g == plus:
            join(0)
            join(1)
        elif g == minus:
            keep(2, 1)
            send((stg2, (2,)), (fin2, (2,)), base + 2, z, place.first[1])
            keep(3, 0)
            send((stg2, (3,)), (fin2, (3,)), base + 3, z, place.first[-1])
        else:
            for k in range(4):
                arrived((fin2, (k,)), base + k, z)
            for h in range(2):
                def fn(cols, h=h):
                    at = pl.ds(h * half, half)
                    summed = total(h, cols) + fin2[0 if h == 0 else 1, :, cols] + fin2[3 if h == 0 else 2, :, cols]
                    out_ref[at, cols] = res_ref[at, cols] + (summed + bias_ref[layer:layer + 1, cols])
                by_piece(z, fn)

    for act, g in ((open_group, 0), (open_group, 1), (open_group, 2), (relay, 0), (open_group, 3), (relay, 1), (close_group, 0), (relay, 2), (close_group, 1), (relay, 3), (close_group, 2), (close_group, 3)):
        lax.fori_loop(0, PIECES, lambda z, carry: (act(g, z), carry)[1], 0)

    def drain(z, carry):
        for g in (side - 2, side - 1):
            for jj in range(side):
                pair_copy(g, jj, z).wait_send()
        for src, dst, slot, device in sent:
            remote(src, dst, slot, z, device).wait_send()
        return carry

    lax.fori_loop(0, PIECES, drain, 0)


def project_and_scatter(side, call_id, layer, act, weight, residual, bias):
    rows, width = residual.shape
    depth = act.shape[1]
    half = rows // 2
    quad = (side, side, rows, width)
    part = (side, 2, half, width)
    vmem = pl.BlockSpec(memory_space=pltpu.VMEM)
    return pl.pallas_call(
        functools.partial(scatter_kernel, side, layer),
        out_shape=jax.ShapeDtypeStruct((rows, width), jnp.float32),
        in_specs=[vmem, pl.BlockSpec(memory_space=pl.ANY), vmem, vmem],
        out_specs=vmem,
        scratch_shapes=[
            pltpu.VMEM((depth, width), jnp.bfloat16),
            pltpu.VMEM(quad, jnp.bfloat16),
            pltpu.VMEM((2,) + quad[1:], jnp.bfloat16),
            pltpu.VMEM(quad, jnp.bfloat16),
            pltpu.VMEM((side, 4, half, width), jnp.float32),
            pltpu.VMEM(part, jnp.float32),
            pltpu.VMEM((side, 4, half, width), jnp.float32),
            pltpu.VMEM((4, half, width), jnp.float32),
            pltpu.VMEM((2, half, width), jnp.float32),
            pltpu.VMEM((4, half, width), jnp.float32),
            pltpu.SemaphoreType.DMA,
            pltpu.SemaphoreType.DMA((side, side, PIECES)),
            pltpu.SemaphoreType.DMA((side, side, PIECES)),
            pltpu.SemaphoreType.DMA((6 * side + 6, PIECES)),
            pltpu.SemaphoreType.DMA((6 * side + 6, PIECES)),
        ],
        compiler_params=pltpu.CompilerParams(collective_id=call_id, has_side_effects=True, vmem_limit_bytes=VMEM_LIMIT),
        name=f"scatter_{call_id}",
    )(act, weight, residual, bias)


GATHER_ORDER = sorted(((i, j) for i in STEPS for j in STEPS), key=lambda at: (2 * abs(at[0]) + 3 * abs(at[1]), at))


def gather_body(place, layer, gelu, res_ref, gain_ref, shift_ref, w_ref, loads, b_ref, out, buf, sems, tails=None, tails_out=None, ready=None, hook=None):
    send_sem, recv_sem, pair_send, pair_recv = sems
    side = place.side
    rows, width = res_ref.shape
    tail = 0 if tails is None else tails.shape[1]
    half = rows // 2
    for at in (pl.ds(0, half), pl.ds(half, half)):
        residual = res_ref[at, :].astype(jnp.float32)
        centered = residual - jnp.mean(residual, axis=-1, keepdims=True)
        variance = jnp.mean(centered * centered, axis=-1, keepdims=True)
        normed = centered * lax.rsqrt(variance + 1e-5) * gain_ref[layer:layer + 1, :] + shift_ref[layer:layer + 1, :]
        buf[place.me, at, pl.ds(0, width)] = normed.astype(jnp.bfloat16)
    if tail:
        buf[place.me, :, pl.ds(width, tail)] = tails[...]
    if ready is not None:
        ready()

    def pick(n, values):
        value = values[0]
        for k, other in enumerate(values):
            value = jnp.where(n == k, other, value)
        return value

    def view(i, j, h, core=None):
        return buf.at[place.dev(i, j, core), pl.ds(pl.multiple_of(h * half, half), half)]

    def wrap(k):
        return (k + side + 1) % side - 1

    def slot(i, j, h):
        return ((i + side) % side * side + (j + side) % side) * 2 + h

    def ring_copies(i, j, h):
        own = (j == 0) & (i == 0)
        begins = (h == 0, h == 1)
        for axis, ahead in enumerate(((j == 0, i), (True, j))):
            whole = own if axis == 0 else j == 0
            for side_of, step in enumerate((1, -1)):
                there = (wrap(i - step), j) if axis == 0 else (i, wrap(j - step))
                device = (place.first, place.second)[axis][step]
                condition = whole | (ahead[0] & (ahead[1] == -step) & begins[side_of])
                yield condition, pltpu.make_async_remote_copy(src_ref=view(i, j, h), dst_ref=view(i, j, h), send_sem=send_sem.at[axis * 2 + side_of, slot(i, j, h)], recv_sem=recv_sem.at[slot(*there, h)], device_id={"tp": device}, device_id_type=MESH)

    def pair(i, j, h, core=None):
        index = slot(i, j, h)
        ref = view(i, j, h, core)
        return pltpu.make_async_remote_copy(src_ref=ref, dst_ref=ref, send_sem=pair_send.at[index], recv_sem=pair_recv.at[index], device_id={"tp": place.partner}, device_id_type=MESH)

    def arrived(i, j, h):
        ref = view(i, j, h)
        pltpu.make_async_remote_copy(src_ref=ref, dst_ref=ref, send_sem=send_sem.at[0, 0], recv_sem=recv_sem.at[slot(i, j, h)], device_id={"tp": place.me}, device_id_type=MESH).wait_recv()

    def multiply(i, j):
        devs = [place.dev(i, j), place.dev(i, j, 1 - place.core)]
        at = [pl.ds(pl.multiple_of(d * rows, rows), rows) for d in devs]
        if tail:
            for d, where in zip(devs, at):
                tails_out[where, :] = buf[d, :, pl.ds(width, tail)]
        lhs = jnp.concatenate([buf[d, :, pl.ds(0, width)] for d in devs], axis=0)
        part = jnp.dot(lhs, w_ref[...], preferred_element_type=jnp.float32)
        if gelu:
            part = jax.nn.gelu(part + b_ref[layer:layer + 1, :], approximate=True)
        part = part.astype(jnp.bfloat16)
        for k, where in enumerate(at):
            out[where, :] = part[k * rows:(k + 1) * rows]

    firsts = [at[0] for at in GATHER_ORDER]
    seconds = [at[1] for at in GATHER_ORDER]
    leads = [int(1 in at and -1 not in at) for at in GATHER_ORDER]

    def take(n, carry):
        i, j, lead = pick(n, firsts), pick(n, seconds), pick(n, leads)
        for k in range(2):
            h = (lead + k) % 2

            @pl.when(n > 0)
            def _():
                arrived(i, j, h)

            for condition, copy in ring_copies(i, j, h):
                pl.when(condition)(copy.start)
            pair(i, j, h).start()

        @pl.when(n == 0)
        def _():
            for load in loads:
                load.wait()

        for h in range(2):
            pair(i, j, h, 1 - place.core).wait_recv()
        multiply(i, j)
        return carry

    def drain(n, carry):
        i, j = pick(n, firsts), pick(n, seconds)
        for h in range(2):
            for condition, copy in ring_copies(i, j, h):
                pl.when(condition)(copy.wait_send)
            pair(i, j, h).wait_send()
        return carry

    last = max(n for n, at in enumerate(GATHER_ORDER) if at[1] != 2) + 1
    lax.fori_loop(0, last, take, 0)
    if hook is not None:
        hook()
    lax.fori_loop(last, len(GATHER_ORDER), take, 0)
    return lambda: lax.fori_loop(0, len(GATHER_ORDER), drain, 0)


QUERY_BLOCK = 256
RING = ((-1, 0), (1, 1), (-1, 1), (1, 0), (2, 0), (2, 1))


def attend_body(place, layer, qkv_ref, ids_ref, row_ids_ref, load_w, res_ref, bias_ref, out_ref, bufs, sems):
    w_own, wbuf, obuf, o_own, scores, acc, rbuf, relay = bufs
    ws_send, ws_recv, wg_send, wg_recv, os_send, os_recv, og_send, og_recv, op_send, op_recv, back_send, back_recv, relay_send, relay_recv = sems
    side, me, core, x, y = place.side, place.me, place.core, place.x, place.y
    rows, width = res_ref.shape
    dim = w_own.shape[0]
    share = width // (2 * side)
    parts, _, _, cols = wbuf.shape
    line = rows * 2 * side
    steps = STEPS

    def at(dx=0, dy=0, dc=0):
        return (((y + dy + side) % side) * side + (x + dx + side) % side) * 2 + (core + dc) % 2

    peers = [at(dx, dc=dc) for dx in steps for dc in (1, 0) if (dx, dc) != (0, 0)]
    columns = [at(dy=dy) for dy in steps[:3]]
    sent = []

    def send(src, dst, send_sem, recv_sem, device):
        if device is None:
            copy = pltpu.make_async_copy(src, dst, recv_sem)
        else:
            copy = pltpu.make_async_remote_copy(src_ref=src, dst_ref=dst, send_sem=send_sem, recv_sem=recv_sem, device_id={"tp": device}, device_id_type=MESH)
            sent.append(copy)
        copy.start()

    def arrived(dst, recv_sem):
        pltpu.make_async_copy(dst, dst, recv_sem).wait()

    def target(dx, dy, dc):
        return None if (dx, dy, dc) == (0, 0, 0) else at(dx, dy, dc)

    def first_col(device, part):
        return pl.multiple_of(device % (2 * side) * share + part * cols, 128)

    def begin():
        load_w.wait()
        for part in range(parts):
            for k, dx in enumerate(steps):
                for dc in range(2):
                    src = w_own.at[:, pl.ds(first_col(at(dx, dc=dc), part), cols)]
                    send(src, wbuf.at[part, me], ws_send.at[part, k, dc], ws_recv.at[part, k, dc], target(dx, 0, dc))

    def w_slots(part, j, h):
        return wbuf.at[part, pl.ds(((y + j + side) % side) * 2 * side + h * side, side)]

    def w_ring(part, j, h):
        index = RING.index((j, h))
        return wg_send.at[part, index], wg_recv.at[part, index]

    def w_first(part):
        for k, dx in enumerate(steps):
            for dc in range(2):
                arrived(wbuf.at[part, at(-dx, dc=dc)], ws_recv.at[part, k, dc])
        for h in range(2):
            send(w_slots(part, 0, h), w_slots(part, 0, h), *w_ring(part, -1, h), at(dy=1))
            send(w_slots(part, 0, 1 - h), w_slots(part, 0, 1 - h), *w_ring(part, 1, 1 - h), at(dy=-1))

    def w_arrived(part, j, h):
        arrived(w_slots(part, j, h), w_ring(part, j, h)[1])

    def w_relay(part):
        w_arrived(part, -1, 0)
        send(w_slots(part, -1, 0), w_slots(part, -1, 0), *w_ring(part, 2, 0), at(dy=1))
        w_arrived(part, 1, 1)
        send(w_slots(part, 1, 1), w_slots(part, 1, 1), *w_ring(part, 2, 1), at(dy=-1))

    block = scores.shape[0]
    half = block // 2

    def attend(b):
        q_rows = pl.ds(pl.multiple_of(b * block, block), block)
        q = qkv_ref[q_rows, pl.ds(0, dim)]
        q_ids = ids_ref[q_rows, 0:1].astype(jnp.float32)
        q_pos = b * block + lax.broadcasted_iota(jnp.int32, (block, block), 0)

        def chunk(c):
            return pl.ds(pl.multiple_of(c * block, block), block)

        def score(c, top):
            s = lax.dot_general(q, qkv_ref[chunk(c), pl.ds(dim, dim)], (((1,), (1,)), ((), ())), preferred_element_type=jnp.float32) * dim ** -0.5
            k_pos = c * block + lax.broadcasted_iota(jnp.int32, (block, block), 1)
            allowed = (k_pos <= q_pos) & (row_ids_ref[0:1, chunk(c)] == q_ids)
            s = jnp.where(allowed, s, -1e30)
            scores[:, chunk(c)] = s
            return jnp.maximum(top, jnp.maximum(s[:, :half], s[:, half:]))

        top = jnp.max(lax.fori_loop(0, b + 1, score, jnp.full((block, half), -1e30, jnp.float32)), axis=-1, keepdims=True)

        def power(c, total):
            e = jnp.exp(scores[:, chunk(c)] - top)
            scores[:, chunk(c)] = e
            return total + (e[:, :half] + e[:, half:])

        total = jnp.sum(lax.fori_loop(0, b + 1, power, jnp.zeros((block, half), jnp.float32)), axis=-1, keepdims=True)
        inverse = 1.0 / total

        def mix(c, mixed):
            probs = (scores[:, chunk(c)] * inverse).astype(jnp.bfloat16)
            return mixed + jnp.dot(probs, qkv_ref[chunk(c), pl.ds(2 * dim, dim)], preferred_element_type=jnp.float32)

        o_own[q_rows, :] = lax.fori_loop(0, b + 1, mix, jnp.zeros((block, dim), jnp.float32)).astype(jnp.bfloat16)

    def o_slot(c, xx, yy):
        return (c * side + xx) * side + yy

    def attend_line(k):
        n = (y + steps[k] + side) % side

        def body(b, carry):
            attend(n * (line // block) + b)
            return carry

        lax.fori_loop(0, line // block, body, 0)
        src = o_own.at[pl.ds(pl.multiple_of(n * line, line), line)]
        send(src, obuf.at[o_slot(core, x, y)], os_send.at[k], os_recv.at[k], target(0, steps[k], 0))

    def o_view(k, i, dc=0):
        return obuf.at[o_slot((core + dc) % 2, (x + i + side) % side, (y - steps[k] + side) % side)]

    def o_half(k, i, h):
        return o_view(k, i).at[pl.ds(h * (line // 2), line // 2)]

    def o_send(k, i, h, step):
        index = RING.index(((i - step + side + 1) % side - 1, h))
        send(o_half(k, i, h), o_half(k, i, h), og_send.at[k, index], og_recv.at[k, index], at(step))

    def o_arrived(k, i, h):
        arrived(o_half(k, i, h), og_recv.at[k, RING.index((i, h))])

    def o_share(k, i):
        send(o_view(k, i), o_view(k, i), op_send.at[k, i % side], op_recv.at[k, i % side], at(dc=1))

    def o_first(k):
        arrived(o_view(k, 0), os_recv.at[k])
        for h in range(2):
            o_send(k, 0, h, 1)
            o_send(k, 0, 1 - h, -1)
        o_share(k, 0)

    def o_relay(k):
        o_arrived(k, -1, 0)
        o_send(k, -1, 0, 1)
        o_arrived(k, 1, 1)
        o_send(k, 1, 1, -1)

    def o_rest(k):
        o_arrived(k, -1, 1)
        o_share(k, -1)
        o_arrived(k, 1, 0)
        o_share(k, 1)
        for h in range(2):
            o_arrived(k, 2, h)
        o_share(k, 2)

    strip = min(block, line)

    def heads_of(part, at_rows, j, total):
        yy = (y + j + side) % side
        for xx in range(side):
            for c in range(2):
                head = jnp.dot(obuf[o_slot(c, xx, yy), at_rows, :], wbuf[part, (yy * side + xx) * 2 + c], preferred_element_type=jnp.float32)
                total = total + head.astype(jnp.bfloat16).astype(jnp.float32)
        return total

    def project(part, last):
        def body(n, carry):
            at_rows = pl.ds(pl.multiple_of(n * strip, strip), strip)
            if last:
                total = heads_of(part, at_rows, 2, acc[part, at_rows, :])
            else:
                total = lax.fori_loop(0, 3, lambda k, t: heads_of(part, at_rows, (k + 1) % 3 - 1, t), jnp.zeros((strip, cols), jnp.float32))
            acc[part, at_rows, :] = total
            return carry

        lax.fori_loop(0, line // strip, body, 0)

    def back_rows(device):
        return pl.ds(pl.multiple_of(device % (2 * side) * rows, rows), rows)

    def finish(at_cols):
        out_ref[:, at_cols] = res_ref[:, at_cols].astype(jnp.float32) + (rbuf[:, at_cols] + bias_ref[layer:layer + 1, at_cols])

    def pass_on(part):
        arrived(relay.at[part], relay_recv.at[part])
        far = steps.index(2)
        send(relay.at[part], rbuf.at[:, pl.ds(first_col(at(1), part), cols)], back_send.at[part, far, 1], back_recv.at[part, far, 1], at(-1, dc=1))

    def proceed():
        attend_line(0)
        attend_line(1)
        w_first(0)
        attend_line(2)
        o_first(0)
        w_first(1)
        attend_line(3)
        o_first(1)
        w_relay(0)
        o_first(3)
        o_first(2)
        o_relay(0)
        w_first(2)
        o_relay(1)
        w_relay(1)
        o_relay(3)
        o_relay(2)
        w_first(3)
        for k in range(side):
            o_rest(k)
        w_relay(2)
        for k in range(side):
            for i in steps:
                arrived(o_view(k, i, 1), op_recv.at[k, i % side])

        for part in range(parts):
            w_arrived(part, -1, 1)
            w_arrived(part, 1, 0)
            project(part, False)
            for h in range(2):
                w_arrived(part, 2, h)
            project(part, True)
            for k, dx in enumerate(steps):
                for dc in range(2):
                    src = acc.at[part, back_rows(at(dx, dc=dc))]
                    dst = rbuf.at[:, pl.ds(first_col(me, part), cols)]
                    if dx == 2 and dc:
                        send(src, relay.at[part], relay_send.at[part], relay_recv.at[part], at(-1))
                    else:
                        send(src, dst, back_send.at[part, k, dc], back_recv.at[part, k, dc], target(dx, 0, dc))
            if part == 0:
                w_relay(3)
            else:
                pass_on(part - 1)
        pass_on(parts - 1)
        for part in range(parts):
            for k, dx in enumerate(steps):
                for dc in range(2):
                    arrived(rbuf.at[:, pl.ds(first_col(at(-dx, dc=dc), part), cols)], back_recv.at[part, k, dc])
        by_cols(width, finish)

    def drain():
        for copy in sent:
            copy.wait_send()

    return peers + columns, begin, proceed, drain


def front_kernel(side, layer, first, res_ref, ids_in, row_ids_in, gain1_ref, shift1_ref, w_qkv, w_out, bias_ref, gain2_ref, shift2_ref, w_up, b_ref, *refs):
    out_ref, hidden_ref, refs = refs[0], refs[1], refs[2:]
    ids_ref, row_ids_ref = ids_in, row_ids_in
    if first:
        ids_ref, row_ids_ref, refs = refs[0], refs[1], refs[2:]
    w_qkv_ref, w_up_ref, qkv_ref, buf1, buf2, refs = *refs[:5], refs[5:]
    bufs, w_sem, refs = refs[:8], refs[8], refs[9:]
    sems1, sems2, sems = refs[:4], refs[4:8], refs[8:]
    thirds = w_qkv.shape[1]
    each = w_qkv.shape[4]
    loads = [pltpu.make_async_copy(w_qkv.at[layer, k, 0], w_qkv_ref.at[:, pl.ds(k * each, each)], w_sem.at[k]) for k in range(thirds)]
    load_out = pltpu.make_async_copy(w_out.at[layer, 0], bufs[0], w_sem.at[thirds])
    load_up = pltpu.make_async_copy(w_up.at[layer], w_up_ref, w_sem.at[thirds + 1])
    for load in loads + [load_out, load_up]:
        load.start()
    place = Place(side)
    others, begin, proceed, drain = attend_body(place, layer, qkv_ref, ids_ref, row_ids_ref, load_out, res_ref, bias_ref, out_ref, bufs, sems)
    announce(others)
    drain1 = gather_body(place, layer, False, res_ref, gain1_ref, shift1_ref, w_qkv_ref, loads, None, qkv_ref, buf1, sems1, ids_in if first else None, ids_ref if first else None, lambda: meet(others), begin)
    if first:
        step = ids_ref.shape[1]

        def turn(n, carry):
            at = pl.ds(pl.multiple_of(n * step, step), step)
            row_ids_ref[:, at] = jnp.transpose(ids_ref[at, :].astype(jnp.float32))[0:1]
            return carry

        lax.fori_loop(0, ids_ref.shape[0] // step, turn, 0)
    proceed()
    drain2 = gather_body(place, layer, True, out_ref, gain2_ref, shift2_ref, w_up_ref, [load_up], b_ref, hidden_ref, buf2, sems2)
    drain1()
    drain()
    drain2()


def front(side, call_id, layer, first, residual, ids, row_ids, gain1, shift1, w_qkv, w_out, out_bias, gain2, shift2, w_up, up_bias):
    rows, width = residual.shape
    dim = w_out.shape[2]
    groups = 2 * side * side
    seq = groups * rows
    line = rows * 2 * side
    parts = 4
    cols = width // (2 * side) // parts
    block = min(QUERY_BLOCK, line)
    tail = ids.shape[1]
    vmem = pl.BlockSpec(memory_space=pltpu.VMEM)
    hbm = pl.BlockSpec(memory_space=pl.ANY)
    dma = pltpu.SemaphoreType.DMA
    gather_sems = [dma((4, groups)), dma((groups,)), dma((groups,)), dma((groups,))]
    shapes = [((rows, width), jnp.float32), ((seq, w_up.shape[2]), jnp.bfloat16)]
    if first:
        shapes += [((seq, tail), jnp.bfloat16), ((1, seq), jnp.float32)]
    return pl.pallas_call(
        functools.partial(front_kernel, side, layer, first),
        out_shape=[jax.ShapeDtypeStruct(*shape) for shape in shapes],
        in_specs=[vmem] * 5 + [hbm, hbm] + [vmem] * 3 + [hbm, vmem],
        out_specs=[vmem] * len(shapes),
        scratch_shapes=[
            pltpu.VMEM((width, w_qkv.shape[1] * dim), jnp.bfloat16),
            pltpu.VMEM((width, w_up.shape[2]), jnp.bfloat16),
            pltpu.VMEM((seq, w_qkv.shape[1] * dim), jnp.bfloat16),
            pltpu.VMEM((groups, rows, width + (tail if first else 0)), jnp.bfloat16),
            pltpu.VMEM((groups, rows, width), jnp.bfloat16),
            pltpu.VMEM((dim, width), jnp.bfloat16),
            pltpu.VMEM((parts, groups, dim, cols), jnp.bfloat16),
            pltpu.VMEM((groups, line, dim), jnp.bfloat16),
            pltpu.VMEM((seq, dim), jnp.bfloat16),
            pltpu.VMEM((block, seq), jnp.float32),
            pltpu.VMEM((parts, line, cols), jnp.float32),
            pltpu.VMEM((rows, width), jnp.float32),
            pltpu.VMEM((parts, rows, cols), jnp.float32),
            dma((w_qkv.shape[1] + 2,)),
            *gather_sems, *gather_sems,
            dma((parts, side, 2)), dma((parts, side, 2)),
            dma((parts, 6)), dma((parts, 6)),
            dma((side,)), dma((side,)),
            dma((side, 6)), dma((side, 6)),
            dma((side, side)), dma((side, side)),
            dma((parts, side, 2)), dma((parts, side, 2)),
            dma((parts,)), dma((parts,)),
        ],
        compiler_params=pltpu.CompilerParams(collective_id=call_id, has_side_effects=True, vmem_limit_bytes=VMEM_LIMIT),
        name=f"front_{call_id}",
    )(residual, ids, row_ids, gain1, shift1, w_qkv, w_out, out_bias, gain2, shift2, w_up, up_bias)


def solution(mesh):
    groups = mesh.shape["tp"]
    side = math.isqrt(groups // 2)
    assert 2 * side * side == groups and side == 4
    row_spec = P("dp", "tp", None)
    vec_spec = P()
    second = P(None, "tp")
    in_specs = (row_spec, P("dp", "tp"), vec_spec, vec_spec, P(None, None, None, "tp"), second, vec_spec, vec_spec, vec_spec, P(None, None, "tp"), second, second, vec_spec)

    def device_fn(tokens, doc_ids, norm1_gain, norm1_shift, qkv_weight, out_weight, out_bias, norm2_gain, norm2_shift, up_weight, up_bias, down_weight, down_bias):
        layers = norm1_gain.shape[0]
        id_cols = jnp.broadcast_to(doc_ids[0].astype(jnp.bfloat16)[:, None], (doc_ids.shape[1], 128))
        qkv_thirds = jnp.transpose(qkv_weight, (0, 2, 3, 1, 4))
        residual = tokens[0]
        all_ids, row_ids = id_cols, jnp.zeros((1, 128), jnp.float32)
        for layer in range(layers):
            first = layer == 0
            residual, hidden, *made = front(side, 2 * layer, layer, first, residual, all_ids, row_ids, norm1_gain, norm1_shift, qkv_thirds, out_weight, out_bias, norm2_gain, norm2_shift, up_weight, up_bias)
            if first:
                all_ids, row_ids = made
            residual = project_and_scatter(side, 2 * layer + 1, layer, hidden, down_weight, residual, down_bias)
        return residual.astype(jnp.bfloat16)[None]

    return jax.shard_map(device_fn, mesh=mesh, in_specs=in_specs, out_specs=row_spec, check_vma=False)
```
